16 devices in a mesh: data: 16 (over z, y, x, core).
Axes of the slice: x: 2, y: 2, z: 2, core: 2. Of those that a mesh axis runs over, the one named last changes fastest.
Arguments:
- x_now: bfloat16 [64, 197, 192], P('data')
- x_next: bfloat16 [64, 197, 192], P('data')
- labels: int32 [64], P('data')
- w_up: float32 [32, 192, 768], replicated
- w_down: float32 [32, 768, 192], replicated
- w_head: float32 [192, 1000], replicated
- mom_up: float32 [32, 192, 768], P(None, None, 'data')
- mom_down: float32 [32, 768, 192], P(None, 'data')
- mom_head: float32 [192, 1000], P('data')
- learn_rate: float32 [], replicated
- mom_decay: float32 [], replicated
Outputs:
- output 1: float32 [64, 1000], P('data')
- output 2: float32 [32, 192, 768], replicated
- output 3: float32 [32, 768, 192], replicated
- output 4: float32 [192, 1000], replicated
- output 5: float32 [32, 192, 768], P(None, None, 'data')
- output 6: float32 [32, 768, 192], P(None, 'data')
- output 7: float32 [192, 1000], P('data')
All inputs are finite; a program needn't handle non-finite values.
Results may differ from the reference program's by a relative error of at most 0.0158812.
Values are sent between devices in bfloat16 or wider.
A program may use at most 1 GiB of HBM per device.

```python
import math
import jax
import jax.numpy as jnp
from jax import lax

BATCH_DEV = 4
TOKENS = 197
WIDTH = 192
HIDDEN = 768
CLASSES = 1000
LAYERS = 32
GROUPS = 16
LN_EPS = 1e-6


def setup_inputs(seed: int = 0) -> dict:
    keys = jax.random.split(jax.random.key(seed), 13)
    batch = GROUPS * BATCH_DEV
    mom_scale = batch ** -0.5
    img_now = jax.random.normal(keys[0], (batch, 1, WIDTH), jnp.float32)
    tok_now = jax.random.normal(keys[1], (batch, TOKENS, WIDTH), jnp.float32)
    img_next = jax.random.normal(keys[2], (batch, 1, WIDTH), jnp.float32)
    tok_next = jax.random.normal(keys[3], (batch, TOKENS, WIDTH), jnp.float32)
    down_raw = jax.random.normal(keys[6], (LAYERS, HIDDEN, WIDTH), jnp.float32) * HIDDEN ** -0.5
    mom_raw = jax.random.normal(keys[9], (LAYERS, HIDDEN, WIDTH), jnp.float32) * (HIDDEN ** -0.5 * mom_scale)
    return {
        "x_now": (0.8 * img_now + 0.6 * tok_now).astype(jnp.bfloat16),
        "x_next": (0.8 * img_next + 0.6 * tok_next).astype(jnp.bfloat16),
        "labels": jax.random.randint(keys[4], (batch,), 0, CLASSES, jnp.int32),
        "w_up": jax.random.normal(keys[5], (LAYERS, WIDTH, HIDDEN), jnp.float32) * WIDTH ** -0.5,
        "w_down": down_raw - jnp.mean(down_raw, axis=1, keepdims=True),
        "w_head": jax.random.normal(keys[7], (WIDTH, CLASSES), jnp.float32) * WIDTH ** -0.5,
        "mom_up": jax.random.normal(keys[8], (LAYERS, WIDTH, HIDDEN), jnp.float32) * (WIDTH ** -0.5 * mom_scale),
        "mom_down": mom_raw - jnp.mean(mom_raw, axis=1, keepdims=True),
        "mom_head": jax.random.normal(keys[10], (WIDTH, CLASSES), jnp.float32) * (WIDTH ** -0.5 * mom_scale),
        "learn_rate": jax.random.uniform(keys[11], (), jnp.float32, 0.3, 0.6) * math.sqrt(batch),
        "mom_decay": jax.random.uniform(keys[12], (), jnp.float32, 0.7, 0.95),
    }


def norm_rows(values):
    mean_v = jnp.mean(values, axis=-1, keepdims=True)
    centered = values - mean_v
    var_v = jnp.mean(centered * centered, axis=-1, keepdims=True)
    return centered * lax.rsqrt(var_v + LN_EPS)


def block_fwd(x_rows, w_in, w_out):
    x_wide = x_rows.astype(jnp.float32)
    u_rows = norm_rows(x_wide).astype(jnp.bfloat16)
    pre_act = jnp.dot(u_rows, w_in.astype(jnp.bfloat16), preferred_element_type=jnp.float32).astype(jnp.bfloat16)
    gelu_out = jax.nn.gelu(pre_act.astype(jnp.float32), approximate=True).astype(jnp.bfloat16)
    block_out = jnp.dot(gelu_out, w_out.astype(jnp.bfloat16), preferred_element_type=jnp.float32).astype(jnp.bfloat16)
    return (x_wide + block_out.astype(jnp.float32)).astype(jnp.bfloat16)


def group_logits(x_grp, w_up, w_down, w_head):
    n_img, n_tok, width = x_grp.shape

    def layer_step(rows, layer_w):
        return block_fwd(rows, layer_w[0], layer_w[1]), None

    rows, _ = lax.scan(layer_step, x_grp.reshape(n_img * n_tok, width), (w_up, w_down))
    pooled = jnp.mean(rows.reshape(n_img, n_tok, width), axis=1, dtype=jnp.float32)
    normed = norm_rows(pooled).astype(jnp.bfloat16)
    return jnp.dot(normed, w_head.astype(jnp.bfloat16), preferred_element_type=jnp.float32)


def cross_ent(logits, labels):
    log_norm = jax.nn.logsumexp(logits, axis=-1)
    picked = jnp.sum(logits * jax.nn.one_hot(labels, logits.shape[-1], dtype=logits.dtype), axis=-1)
    return log_norm - picked


def reference(x_now, x_next, labels, w_up, w_down, w_head, mom_up, mom_down, mom_head, learn_rate, mom_decay):
    weights = (w_up, w_down, w_head)
    batch_total = GROUPS * BATCH_DEV
    x_groups = x_now.reshape(GROUPS, BATCH_DEV, TOKENS, WIDTH)
    label_groups = labels.reshape(GROUPS, BATCH_DEV)

    def accumulate(total, group):
        x_grp, lab_grp = group

        def group_loss(params):
            logits = group_logits(x_grp, params[0], params[1], params[2])
            return jnp.sum(cross_ent(logits, lab_grp)) / batch_total

        _, loss_pull = jax.vjp(group_loss, weights)
        gradients = loss_pull(jnp.ones((), jnp.float32))[0]
        return (total[0] + gradients[0], total[1] + gradients[1], total[2] + gradients[2]), None

    zero_grads = (jnp.zeros_like(w_up), jnp.zeros_like(w_down), jnp.zeros_like(w_head))
    gradients, _ = lax.scan(accumulate, zero_grads, (x_groups, label_groups))
    new_mom_up = mom_decay * mom_up + gradients[0]
    new_mom_down = mom_decay * mom_down + gradients[1]
    new_mom_head = mom_decay * mom_head + gradients[2]
    new_w_up = w_up - learn_rate * new_mom_up
    new_w_down = w_down - learn_rate * new_mom_down
    new_w_head = w_head - learn_rate * new_mom_head
    next_groups = x_next.reshape(GROUPS, BATCH_DEV, TOKENS, WIDTH)
    logits_next = lax.map(lambda x_grp: group_logits(x_grp, new_w_up, new_w_down, new_w_head), next_groups)
    logits_next = logits_next.reshape(GROUPS * BATCH_DEV, CLASSES)
    return (logits_next, new_w_up, new_w_down, new_w_head, new_mom_up, new_mom_down, new_mom_head)
```

```python
import functools

import jax
import jax.numpy as jnp
from jax import lax
from jax.experimental import pallas as pl
from jax.experimental.pallas import tpu as pltpu
from jax.sharding import PartitionSpec as P

LN_EPS = 1e-6
GELU_C = 0.7978845608028654
GELU_A = 0.044715
F32 = jnp.float32
BF16 = jnp.bfloat16
LAST = (((1,), (1,)), ((), ()))
ROWS = (((0,), (0,)), ((), ()))
MESH_ID = pl.DeviceIdType.MESH
VMEM_LIMIT = 62 * 1024 * 1024
CHUNKS = 5
SLOTS = 4
AG_SLOTS = 8
PARTS = 3
ORDER = ((0, 1, 2), (1, 2, 0), (2, 0, 1))


def norm_parts(values):
    mean_v = jnp.mean(values, axis=-1, keepdims=True)
    centered = values - mean_v
    var_v = jnp.mean(centered * centered, axis=-1, keepdims=True)
    return centered, lax.rsqrt(var_v + LN_EPS)


def norm_pull(normed, scale, grad):
    mean_g = jnp.mean(grad, axis=-1, keepdims=True)
    mean_gn = jnp.mean(grad * normed, axis=-1, keepdims=True)
    return scale * (grad - mean_g - normed * mean_gn)


def gelu(values):
    half = 0.5 * values
    tanh_v = jnp.tanh(values * (GELU_C + (GELU_C * GELU_A) * (values * values)))
    return half + half * tanh_v


def gelu_both(values):
    half = 0.5 * values
    square = values * values
    tanh_v = jnp.tanh(values * (GELU_C + (GELU_C * GELU_A) * square))
    out = half + half * tanh_v
    slope = (0.5 + 0.5 * tanh_v) + (half * (1.0 - tanh_v * tanh_v)) * (GELU_C + (3.0 * GELU_C * GELU_A) * square)
    return out, slope


def pack_rows(x_ref, wide, rows, n_img, n_tok):
    wide[...] = jnp.zeros_like(wide)
    for img in range(n_img):
        wide[img * n_tok : (img + 1) * n_tok, :] = x_ref[img].astype(F32)
    rows[...] = wide[...].astype(BF16)


def pool_mask(shape, n_img, n_tok, row_axis):
    row = lax.broadcasted_iota(jnp.int32, shape, row_axis)
    img = lax.broadcasted_iota(jnp.int32, shape, 1 - row_axis)
    inside = (row >= img * n_tok) & (row < (img + 1) * n_tok) & (img < n_img)
    return jnp.where(inside, 1.0, 0.0).astype(BF16)


def pooled_norm(rows, n_img, n_tok):
    n_rows = rows.shape[0]
    mask = pool_mask((8, n_rows), n_img, n_tok, 1)
    pooled = jnp.dot(mask, rows[...], preferred_element_type=F32) * (1.0 / n_tok)
    centered, scale = norm_parts(pooled)
    return centered * scale, scale


def forward_kernel(n_img, n_tok, batch_total, n_cls, x_ref, lab_ref, wu_ref, wd_ref, wh_ref, xs_ref, pre_ref, grad_ref, norm_ref, gl_ref, wide, rows):
    layer = pl.program_id(0)

    @pl.when(layer == 0)
    def _():
        pack_rows(x_ref, wide, rows, n_img, n_tok)

    up_b = wu_ref[0].astype(BF16)
    down_b = wd_ref[0].astype(BF16)
    step = rows.shape[0] // CHUNKS
    for chunk in range(CHUNKS):
        sl = slice(chunk * step, (chunk + 1) * step)
        x_rows = rows[sl, :]
        xs_ref[0, sl, :] = x_rows
        x_wide = x_rows.astype(F32)
        centered, scale = norm_parts(x_wide)
        u_rows = (centered * scale).astype(BF16)
        pre = jnp.dot(u_rows, up_b, preferred_element_type=F32).astype(BF16)
        pre_ref[0, sl, :] = pre
        z_rows = gelu(pre.astype(F32)).astype(BF16)
        y_rows = jnp.dot(z_rows, down_b, preferred_element_type=F32).astype(BF16)
        rows[sl, :] = (x_wide + y_rows.astype(F32)).astype(BF16)

    @pl.when(layer == pl.num_programs(0) - 1)
    def _():
        normed, scale = pooled_norm(rows, n_img, n_tok)
        normed_b = normed.astype(BF16)
        head_b = wh_ref[...].astype(BF16)
        logits = jnp.dot(normed_b, head_b, preferred_element_type=F32)
        top = jnp.max(logits, axis=-1, keepdims=True)
        exps = jnp.exp(logits - top)
        probs = exps / jnp.sum(exps, axis=-1, keepdims=True)
        classes = lax.broadcasted_iota(jnp.int32, logits.shape, 1)
        image = lax.broadcasted_iota(jnp.int32, logits.shape, 0)
        targets = jnp.where(classes == lab_ref[...], 1.0, 0.0)
        grad_logits = jnp.where(image < n_img, (probs - targets) * (1.0 / batch_total), 0.0)
        grad_b = grad_logits.astype(BF16)
        gl_ref[...] = grad_b
        norm_ref[...] = normed_b
        grad_normed = lax.dot_general(grad_b, head_b, LAST, preferred_element_type=F32).astype(BF16)
        grad_pooled = norm_pull(normed, scale, grad_normed.astype(F32))
        per_row = (grad_pooled / n_tok).astype(BF16)
        spread = pool_mask((rows.shape[0], 8), n_img, n_tok, 0)
        grad_ref[...] = jnp.dot(spread, per_row, preferred_element_type=F32).astype(BF16)


def next_kernel(n_img, n_tok, lr_ref, x_ref, wu_ref, wd_ref, mom_ref, wh_ref, nwu_ref, nwd_ref, log_ref, wide, rows):
    layer = pl.program_id(0)

    @pl.when(layer == 0)
    def _():
        pack_rows(x_ref, wide, rows, n_img, n_tok)

    rate = lr_ref[0, 0]
    up_a = mom_ref[0, 0].T.astype(F32)
    mixed = mom_ref[0, 2]
    up_z = mixed.T.astype(F32)[64:, :]
    nwu_ref[0, :128, :] = wu_ref[0, :128, :] - rate * up_a
    nwu_ref[0, 128:, :] = wu_ref[0, 128:, :] - rate * up_z
    nwd_ref[0, :, :128] = wd_ref[0, :, :128] - rate * mom_ref[0, 1].astype(F32)
    nwd_ref[0, :, 128:] = wd_ref[0, :, 128:] - rate * mixed[:, :64].astype(F32)
    up_b = nwu_ref[0].astype(BF16)
    down_b = nwd_ref[0].astype(BF16)
    step = rows.shape[0] // CHUNKS
    for chunk in range(CHUNKS):
        sl = slice(chunk * step, (chunk + 1) * step)
        x_wide = rows[sl, :].astype(F32)
        centered, scale = norm_parts(x_wide)
        u_rows = (centered * scale).astype(BF16)
        pre = jnp.dot(u_rows, up_b, preferred_element_type=F32).astype(BF16)
        z_rows = gelu(pre.astype(F32)).astype(BF16)
        y_rows = jnp.dot(z_rows, down_b, preferred_element_type=F32).astype(BF16)
        rows[sl, :] = (x_wide + y_rows.astype(F32)).astype(BF16)

    @pl.when(layer == pl.num_programs(0) - 1)
    def _():
        normed, _ = pooled_norm(rows, n_img, n_tok)
        log_ref[...] = jnp.dot(normed.astype(BF16), wh_ref[...].astype(BF16), preferred_element_type=F32)


def backward_kernel(
    n_items, sc_ref, gh_ref, grad_ref, xs_ref, pre_ref, wu_ref, wd_ref, mom_ref, nm_ref, all_ref,
    g_rows, z_buf, da_buf, u_buf, g_buf, pair_buf, sum_buf, rcv0, rcv1, rcv2, ag_buf,
    d2d_send, d2d_recv, rs_send, rs_recv, ag_send, ag_recv, out_sem,
):
    t = pl.program_id(0)
    me = lax.axis_index("data")
    core = me % 2
    place = ((me // 8) % 2, (me // 4) % 2, (me // 2) % 2)
    peers = tuple(me + (1 - 2 * place[axis]) * w for axis, w in ((0, 8), (1, 4), (2, 2)))
    twin = me + 1 - 2 * core
    rcv = (rcv0, rcv1, rcv2)

    @pl.when(t == 0)
    def _():
        barrier = pltpu.get_barrier_semaphore()
        for peer in peers + (twin,):
            pl.semaphore_signal(barrier, inc=1, device_id=(peer,), device_id_type=MESH_ID)
        pl.semaphore_wait(barrier, 4)

    def pair_copy(item):
        return pltpu.make_async_remote_copy(
            src_ref=g_buf.at[item % SLOTS, :, :, :, :, 1 - core],
            dst_ref=pair_buf.at[item % SLOTS],
            send_sem=d2d_send.at[0, item % 2],
            recv_sem=d2d_recv.at[0, item % 2],
            device_id=(twin,),
            device_id_type=MESH_ID,
        )

    def cut(part, stage, value):
        index = [slice(None)] * 3
        for axis in ORDER[part][:stage]:
            index[axis] = place[axis]
        index[ORDER[part][stage]] = value
        return tuple(index)

    def rs_copy(item, stage, part):
        axis = ORDER[part][stage]
        return pltpu.make_async_remote_copy(
            src_ref=sum_buf.at[(item % SLOTS, part) + cut(part, stage, 1 - place[axis])],
            dst_ref=rcv[stage].at[item % SLOTS, part],
            send_sem=rs_send.at[stage, part, item % 2],
            recv_sem=rs_recv.at[stage, part, item % 2],
            device_id=(peers[axis],),
            device_id_type=MESH_ID,
        )

    def ag_copy(item, stage, part):
        index = [place[0], place[1], place[2]]
        for axis in ORDER[part][:stage]:
            index[axis] = slice(None)
        view = ag_buf.at[(item % AG_SLOTS, part) + tuple(index) + (core,)]
        return pltpu.make_async_remote_copy(
            src_ref=view,
            dst_ref=view,
            send_sem=ag_send.at[stage, part, item % 2],
            recv_sem=ag_recv.at[stage, part, item % 2],
            device_id=(peers[ORDER[part][stage]],),
            device_id_type=MESH_ID,
        )

    def twin_copy(item):
        view = ag_buf.at[item % AG_SLOTS, :, :, :, :, core]
        return pltpu.make_async_remote_copy(
            src_ref=view,
            dst_ref=view,
            send_sem=d2d_send.at[1, item % 2],
            recv_sem=d2d_recv.at[1, item % 2],
            device_id=(twin,),
            device_id_type=MESH_ID,
        )

    def out_copy(item):
        return pltpu.make_async_copy(ag_buf.at[item % AG_SLOTS], all_ref.at[n_items - 1 - item], out_sem.at[item % 2])

    def at_lag(lag):
        return (t >= lag) & (t < n_items + lag)

    @pl.when(t == 1)
    def _():
        g_rows[...] = grad_ref[...]

    @pl.when((t >= 1) & (t < n_items))
    def _():
        up_b = wu_ref[0].astype(BF16)
        down_b = wd_ref[0].astype(BF16)
        step = g_rows.shape[0] // CHUNKS
        grad_old = g_rows[...]
        for chunk in range(CHUNKS):
            sl = slice(chunk * step, (chunk + 1) * step)
            g_old = grad_old[sl, :]
            z_wide, slope = gelu_both(pre_ref[0, sl, :].astype(F32))
            z_buf[sl, :] = z_wide.astype(BF16)
            grad_z = lax.dot_general(g_old, down_b, LAST, preferred_element_type=F32).astype(BF16)
            grad_a = (grad_z.astype(F32) * slope).astype(BF16)
            da_buf[sl, :] = grad_a
            centered, scale = norm_parts(xs_ref[0, sl, :].astype(F32))
            normed = centered * scale
            u_buf[sl, :] = normed.astype(BF16)
            grad_u = lax.dot_general(grad_a, up_b, LAST, preferred_element_type=F32).astype(BF16)
            grad_x = norm_pull(normed, scale, grad_u.astype(F32))
            g_rows[sl, :] = (g_old.astype(F32) + grad_x).astype(BF16)
        down_t = lax.dot_general(grad_old, z_buf[...], ROWS, preferred_element_type=F32).astype(BF16)
        up_g = lax.dot_general(u_buf[...], da_buf[...], ROWS, preferred_element_type=F32).astype(BF16)
        z_buf[:128, :] = up_g[:128, :]
        z_buf[128:256, :] = down_t[:128, :]
        z_buf[256:320, :] = down_t[128:, :]
        z_buf[320:384, :] = up_g[128:, :]

    @pl.when(at_lag(9))
    def _():
        out_copy(t - 9).wait()

    @pl.when(at_lag(8))
    def _():
        item = t - 8
        twin_copy(item).wait()
        out_copy(item).start()

    @pl.when(at_lag(7))
    def _():
        item = t - 7
        for part in range(PARTS):
            ag_copy(item, 2, part).wait()
        twin_copy(item).start()

    for stage in (1, 0):

        @pl.when(at_lag(5 + stage))
        def _(stage=stage):
            item = t - 5 - stage
            for part in range(PARTS):
                ag_copy(item, stage, part).wait()
                ag_copy(item, stage + 1, part).start()

    @pl.when(at_lag(4))
    def _():
        item = t - 4
        for part in range(PARTS):
            rs_copy(item, 2, part).wait()
            grad = sum_buf[item % SLOTS, part, place[0], place[1], place[2]].astype(F32) + rcv[2][item % SLOTS, part].astype(F32)
            grad = grad.astype(BF16).astype(F32)
            mom = sc_ref[0, 0] * mom_ref[0, part] + grad
            nm_ref[0, part] = mom
            ag_buf[item % AG_SLOTS, part, place[0], place[1], place[2], core] = mom.astype(BF16)
            ag_copy(item, 0, part).start()

    for stage in (1, 0):

        @pl.when(at_lag(2 + stage))
        def _(stage=stage):
            item = t - 2 - stage
            for part in range(PARTS):
                rs_copy(item, stage, part).wait()
                kept = (item % SLOTS, part) + cut(part, stage, place[ORDER[part][stage]])
                both = sum_buf[kept].astype(F32) + rcv[stage][item % SLOTS, part].astype(F32)
                sum_buf[kept] = both.astype(BF16)
                rs_copy(item, stage + 1, part).start()

    @pl.when(at_lag(1))
    def _():
        item = t - 1
        pair_copy(item).wait()
        for part in range(PARTS):
            both = g_buf[item % SLOTS, part, :, :, :, core].astype(F32) + pair_buf[item % SLOTS, part].astype(F32)
            sum_buf[item % SLOTS, part] = both.astype(BF16)
            rs_copy(item, 0, part).start()

    @pl.when(t == 0)
    def _():
        g_buf[0] = gh_ref[...]
        pair_copy(0).start()

    @pl.when((t >= 1) & (t < n_items))
    def _():
        for part in range(PARTS):
            turned = z_buf[part * 128 : (part + 1) * 128, :].T
            for dev in range(16):
                block = turned[dev * 48 : (dev + 1) * 48, :]
                g_buf[t % SLOTS, part, dev // 8, (dev // 4) % 2, (dev // 2) % 2, dev % 2] = block
        pair_copy(t).start()


def whole(shape):
    return pl.BlockSpec(shape, lambda i: (0,) * len(shape))


def solution(mesh):
    n_dev = mesh.shape["data"]

    def local_step(x_now, x_next, labels, w_up, w_down, w_head, mom_up, mom_down, mom_head, learn_rate, mom_decay):
        n_img, n_tok, width = x_now.shape
        n_layers, _, hidden = w_up.shape
        n_cls = w_head.shape[1]
        n_rows = -(-n_img * n_tok // (16 * CHUNKS)) * 16 * CHUNKS
        n_items = n_layers + 1
        cols = mom_up.shape[2]
        head_rows = mom_head.shape[0]
        n_tile = -(-n_cls // 128)
        head_each = head_rows * n_tile // PARTS

        lab = jnp.pad(labels, (0, 8 - n_img)).reshape(8, 1)
        xs, pre, grad_rows, normed, grad_logits = pl.pallas_call(
            functools.partial(forward_kernel, n_img, n_tok, n_img * n_dev, n_cls),
            grid=(n_layers,),
            in_specs=[
                whole(x_now.shape),
                whole((8, 1)),
                pl.BlockSpec((1, width, hidden), lambda i: (i, 0, 0)),
                pl.BlockSpec((1, hidden, width), lambda i: (i, 0, 0)),
                whole(w_head.shape),
            ],
            out_specs=[
                pl.BlockSpec((1, n_rows, width), lambda i: (i, 0, 0)),
                pl.BlockSpec((1, n_rows, hidden), lambda i: (i, 0, 0)),
                whole((n_rows, width)),
                whole((8, width)),
                whole((8, n_cls)),
            ],
            out_shape=[
                jax.ShapeDtypeStruct((n_layers, n_rows, width), BF16),
                jax.ShapeDtypeStruct((n_layers, n_rows, hidden), BF16),
                jax.ShapeDtypeStruct((n_rows, width), BF16),
                jax.ShapeDtypeStruct((8, width), BF16),
                jax.ShapeDtypeStruct((8, n_cls), BF16),
            ],
            scratch_shapes=[pltpu.VMEM((n_rows, width), F32), pltpu.VMEM((n_rows, width), BF16)],
            compiler_params=pltpu.CompilerParams(vmem_limit_bytes=VMEM_LIMIT),
            name="step_forward",
        )(x_now, lab, w_up, w_down, w_head)

        def head_blocks(values):
            n_part = values.shape[0] // head_rows
            wide = jnp.pad(values, ((0, 0), (0, n_tile * 128 - n_cls)))
            blocks = wide.reshape(n_part, PARTS, head_each, 128)
            return jnp.pad(blocks, ((0, 0), (0, 0), (0, cols - head_each), (0, 0)))

        head_grad = lax.dot_general(normed, grad_logits, ROWS, preferred_element_type=F32).astype(BF16)
        head_g = head_blocks(head_grad).transpose(1, 0, 2, 3).reshape(PARTS, 2, 2, 2, 2, cols, 128)
        up_t = mom_up.transpose(0, 2, 1)
        mom_in = jnp.stack(
            [up_t[:, :, :128], mom_down[:, :, :128], jnp.concatenate([mom_down[:, :, 128:], up_t[:, :, 128:]], axis=2)], axis=1
        )
        mom_in = jnp.concatenate([mom_in, head_blocks(mom_head)], axis=0)

        def layer_at(t):
            return jnp.clip(n_items - 1 - t, 0, n_layers - 1)

        def update_at(t):
            return n_items - 1 - jnp.clip(t - 4, 0, n_items - 1)

        block = (SLOTS, PARTS, 2, 2, 2)
        new_mom, gathered = pl.pallas_call(
            functools.partial(backward_kernel, n_items),
            grid=(n_items + 9,),
            in_specs=[
                pl.BlockSpec(memory_space=pltpu.SMEM),
                whole((PARTS, 2, 2, 2, 2, cols, 128)),
                whole((n_rows, width)),
                pl.BlockSpec((1, n_rows, width), lambda t: (layer_at(t), 0, 0)),
                pl.BlockSpec((1, n_rows, hidden), lambda t: (layer_at(t), 0, 0)),
                pl.BlockSpec((1, width, hidden), lambda t: (layer_at(t), 0, 0)),
                pl.BlockSpec((1, hidden, width), lambda t: (layer_at(t), 0, 0)),
                pl.BlockSpec((1, PARTS, cols, 128), lambda t: (update_at(t), 0, 0, 0)),
            ],
            out_specs=[
                pl.BlockSpec((1, PARTS, cols, 128), lambda t: (update_at(t), 0, 0, 0)),
                pl.BlockSpec(memory_space=pl.ANY),
            ],
            out_shape=[
                jax.ShapeDtypeStruct((n_items, PARTS, cols, 128), F32),
                jax.ShapeDtypeStruct((n_items, PARTS, 2, 2, 2, 2, cols, 128), BF16),
            ],
            scratch_shapes=[
                pltpu.VMEM((n_rows, width), BF16),
                pltpu.VMEM((n_rows, hidden), BF16),
                pltpu.VMEM((n_rows, hidden), BF16),
                pltpu.VMEM((n_rows, width), BF16),
                pltpu.VMEM(block + (2, cols, 128), BF16),
                pltpu.VMEM(block + (cols, 128), BF16),
                pltpu.VMEM(block + (cols, 128), BF16),
                pltpu.VMEM((SLOTS, PARTS, 2, 2, cols, 128), BF16),
                pltpu.VMEM((SLOTS, PARTS, 2, cols, 128), BF16),
                pltpu.VMEM((SLOTS, PARTS, cols, 128), BF16),
                pltpu.VMEM((AG_SLOTS, PARTS, 2, 2, 2, 2, cols, 128), BF16),
                pltpu.SemaphoreType.DMA((2, 2)),
                pltpu.SemaphoreType.DMA((2, 2)),
                pltpu.SemaphoreType.DMA((3, PARTS, 2)),
                pltpu.SemaphoreType.DMA((3, PARTS, 2)),
                pltpu.SemaphoreType.DMA((3, PARTS, 2)),
                pltpu.SemaphoreType.DMA((3, PARTS, 2)),
                pltpu.SemaphoreType.DMA((2,)),
            ],
            compiler_params=pltpu.CompilerParams(vmem_limit_bytes=VMEM_LIMIT, collective_id=0, has_side_effects=True),
            name="step_backward",
        )(mom_decay.reshape(1, 1), head_g, grad_rows, xs, pre, w_up, w_down, mom_in)

        gathered = gathered.reshape(n_items, PARTS, n_dev * cols, 128)
        head_all = gathered[n_layers].reshape(PARTS, n_dev, cols, 128)[:, :, :head_each]
        head_all = head_all.transpose(1, 0, 2, 3).reshape(n_dev * head_rows, n_tile * 128)[:, :n_cls]
        new_w_head = w_head - learn_rate * head_all.astype(F32)

        new_w_up, new_w_down, logits = pl.pallas_call(
            functools.partial(next_kernel, n_img, n_tok),
            grid=(n_layers,),
            in_specs=[
                pl.BlockSpec(memory_space=pltpu.SMEM),
                whole(x_next.shape),
                pl.BlockSpec((1, width, hidden), lambda i: (i, 0, 0)),
                pl.BlockSpec((1, hidden, width), lambda i: (i, 0, 0)),
                pl.BlockSpec((1, PARTS, n_dev * cols, 128), lambda i: (i, 0, 0, 0)),
                whole(w_head.shape),
            ],
            out_specs=[
                pl.BlockSpec((1, width, hidden), lambda i: (i, 0, 0)),
                pl.BlockSpec((1, hidden, width), lambda i: (i, 0, 0)),
                whole((8, n_cls)),
            ],
            out_shape=[
                jax.ShapeDtypeStruct(w_up.shape, F32),
                jax.ShapeDtypeStruct(w_down.shape, F32),
                jax.ShapeDtypeStruct((8, n_cls), F32),
            ],
            scratch_shapes=[pltpu.VMEM((n_rows, width), F32), pltpu.VMEM((n_rows, width), BF16)],
            compiler_params=pltpu.CompilerParams(vmem_limit_bytes=VMEM_LIMIT),
            name="step_next",
        )(learn_rate.reshape(1, 1), x_next, w_up, w_down, gathered, new_w_head)

        layers = new_mom[:n_layers]
        new_mom_down = jnp.concatenate([layers[:, 1], layers[:, 2, :, :64]], axis=2)
        new_mom_up = jnp.concatenate([layers[:, 0], layers[:, 2, :, 64:]], axis=2).transpose(0, 2, 1)
        new_mom_head = new_mom[n_layers][:, :head_each].reshape(head_rows, n_tile * 128)[:, :n_cls]
        return (logits[:n_img], new_w_up, new_w_down, new_w_head, new_mom_up, new_mom_down, new_mom_head)

    spec_up = P(None, None, "data")
    spec_down = P(None, "data", None)
    spec_head = P("data", None)
    return jax.shard_map(
        local_step,
        mesh=mesh,
        in_specs=(P("data"), P("data"), P("data"), P(), P(), P(), spec_up, spec_down, spec_head, P(), P()),
        out_specs=(P("data"), P(), P(), P(), spec_up, spec_down, spec_head),
        check_vma=False,
    )
```

```python
import functools

import jax
import jax.numpy as jnp
from jax import lax
from jax.experimental import pallas as pl
from jax.experimental.pallas import tpu as pltpu
from jax.sharding import PartitionSpec as P

LN_EPS = 1e-6
GELU_C = 0.7978845608028654
GELU_A = 0.044715
F32 = jnp.float32
BF16 = jnp.bfloat16
LAST = (((1,), (1,)), ((), ()))
ROWS = (((0,), (0,)), ((), ()))
MESH_ID = pl.DeviceIdType.MESH
VMEM_LIMIT = 62 * 1024 * 1024
CHUNKS = 5
SLOTS = 4
AG_SLOTS = 8
PARTS = 3
ORDER = ((0, 1, 2), (1, 2, 0), (2, 0, 1))


def norm_parts(values):
    mean_v = jnp.mean(values, axis=-1, keepdims=True)
    centered = values - mean_v
    var_v = jnp.mean(centered * centered, axis=-1, keepdims=True)
    return centered, lax.rsqrt(var_v + LN_EPS)


def norm_pull(normed, scale, grad):
    mean_g = jnp.mean(grad, axis=-1, keepdims=True)
    mean_gn = jnp.mean(grad * normed, axis=-1, keepdims=True)
    return scale * (grad - mean_g - normed * mean_gn)


def gelu(values):
    inner = values * (GELU_C + (GELU_C * GELU_A) * (values * values))
    return values * (0.5 + 0.5 * jnp.tanh(inner))


def gelu_both(values):
    square = values * values
    share = 0.5 + 0.5 * jnp.tanh(values * (GELU_C + (GELU_C * GELU_A) * square))
    out = values * share
    slope = share + (out * (1.0 - share)) * (2.0 * GELU_C + (6.0 * GELU_C * GELU_A) * square)
    return out, slope


def pack_rows(x_ref, wide, rows, n_img, n_tok):
    wide[...] = jnp.zeros_like(wide)
    for img in range(n_img):
        wide[img * n_tok : (img + 1) * n_tok, :] = x_ref[img].astype(F32).T
    rows[...] = wide[...].astype(BF16)


def pool_mask(shape, n_img, n_tok, row_axis):
    row = lax.broadcasted_iota(jnp.int32, shape, row_axis)
    img = lax.broadcasted_iota(jnp.int32, shape, 1 - row_axis)
    inside = (row >= img * n_tok) & (row < (img + 1) * n_tok) & (img < n_img)
    return jnp.where(inside, 1.0, 0.0).astype(BF16)


def pooled_norm(rows, n_img, n_tok):
    n_rows = rows.shape[0]
    mask = pool_mask((8, n_rows), n_img, n_tok, 1)
    pooled = jnp.dot(mask, rows[...], preferred_element_type=F32) * (1.0 / n_tok)
    centered, scale = norm_parts(pooled)
    return centered * scale, scale


def forward_kernel(n_img, n_tok, batch_total, n_cls, x_ref, lab_ref, wu_ref, wd_ref, wh_ref, xs_ref, pre_ref, grad_ref, norm_ref, gl_ref, wide, rows):
    layer = pl.program_id(0)

    @pl.when(layer == 0)
    def _():
        pack_rows(x_ref, wide, rows, n_img, n_tok)

    step = rows.shape[0] // CHUNKS
    for sub in range(wu_ref.shape[0]):
        up_b = wu_ref[sub].astype(BF16)
        down_b = wd_ref[sub].astype(BF16)
        for chunk in range(CHUNKS):
            sl = slice(chunk * step, (chunk + 1) * step)
            x_rows = rows[sl, :]
            xs_ref[sub, sl, :] = x_rows
            x_wide = x_rows.astype(F32)
            centered, scale = norm_parts(x_wide)
            u_rows = (centered * scale).astype(BF16)
            pre = jnp.dot(u_rows, up_b, preferred_element_type=F32).astype(BF16)
            pre_ref[sub, sl, :] = pre
            z_rows = gelu(pre.astype(F32)).astype(BF16)
            y_rows = lax.dot_general(z_rows, down_b, LAST, preferred_element_type=F32).astype(BF16)
            rows[sl, :] = (x_wide + y_rows.astype(F32)).astype(BF16)

    @pl.when(layer == pl.num_programs(0) - 1)
    def _():
        normed, scale = pooled_norm(rows, n_img, n_tok)
        normed_b = normed.astype(BF16)
        head_b = wh_ref[...].astype(BF16)
        logits = jnp.dot(normed_b, head_b, preferred_element_type=F32)
        top = jnp.max(logits, axis=-1, keepdims=True)
        exps = jnp.exp(logits - top)
        probs = exps / jnp.sum(exps, axis=-1, keepdims=True)
        classes = lax.broadcasted_iota(jnp.int32, logits.shape, 1)
        image = lax.broadcasted_iota(jnp.int32, logits.shape, 0)
        targets = jnp.where(classes == lab_ref[...], 1.0, 0.0)
        grad_logits = jnp.where(image < n_img, (probs - targets) * (1.0 / batch_total), 0.0)
        grad_b = grad_logits.astype(BF16)
        gl_ref[...] = grad_b
        norm_ref[...] = normed_b
        grad_normed = lax.dot_general(grad_b, head_b, LAST, preferred_element_type=F32).astype(BF16)
        grad_pooled = norm_pull(normed, scale, grad_normed.astype(F32))
        per_row = (grad_pooled / n_tok).astype(BF16)
        spread = pool_mask((rows.shape[0], 8), n_img, n_tok, 0)
        grad_ref[...] = jnp.dot(spread, per_row, preferred_element_type=F32).astype(BF16)


def next_kernel(n_img, n_tok, lr_ref, x_ref, wu_ref, wd_ref, mom_ref, wh_ref, nwu_ref, nwd_ref, log_ref, wide, rows):
    layer = pl.program_id(0)

    @pl.when(layer == 0)
    def _():
        pack_rows(x_ref, wide, rows, n_img, n_tok)

    rate = lr_ref[0, 0]
    step = rows.shape[0] // CHUNKS
    for sub in range(wu_ref.shape[0]):
        mixed = mom_ref[sub, 2].T.astype(F32)
        nwu_ref[sub, :128, :] = wu_ref[sub, :128, :] - rate * mom_ref[sub, 0].T.astype(F32)
        nwu_ref[sub, 128:, :] = wu_ref[sub, 128:, :] - rate * mixed[64:, :]
        nwd_ref[sub, :128, :] = wd_ref[sub, :128, :] - rate * mom_ref[sub, 1].T.astype(F32)
        nwd_ref[sub, 128:, :] = wd_ref[sub, 128:, :] - rate * mixed[:64, :]
        up_b = nwu_ref[sub].astype(BF16)
        down_b = nwd_ref[sub].astype(BF16)
        for chunk in range(CHUNKS):
            sl = slice(chunk * step, (chunk + 1) * step)
            x_wide = rows[sl, :].astype(F32)
            centered, scale = norm_parts(x_wide)
            u_rows = (centered * scale).astype(BF16)
            pre = jnp.dot(u_rows, up_b, preferred_element_type=F32).astype(BF16)
            z_rows = gelu(pre.astype(F32)).astype(BF16)
            y_rows = lax.dot_general(z_rows, down_b, LAST, preferred_element_type=F32).astype(BF16)
            rows[sl, :] = (x_wide + y_rows.astype(F32)).astype(BF16)

    @pl.when(layer == pl.num_programs(0) - 1)
    def _():
        normed, _ = pooled_norm(rows, n_img, n_tok)
        log_ref[...] = jnp.dot(normed.astype(BF16), wh_ref[...].astype(BF16), preferred_element_type=F32)


def backward_kernel(
    n_items, sc_ref, gh_ref, grad_ref, xs_ref, pre_ref, wu_ref, wd_ref, mh_ref, mu_ref, md_ref, nmh_ref, nmu_ref, nmd_ref, all_ref,
    g_rows, z_buf, da_buf, u_buf, g_buf, pair_buf, sum_buf, rcv0, rcv1, rcv2, ag_buf,
    d2d_send, d2d_recv, rs_send, rs_recv, ag_send, ag_recv, out_sem,
):
    t = pl.program_id(0)
    me = lax.axis_index("data")
    core = me % 2
    place = ((me // 8) % 2, (me // 4) % 2, (me // 2) % 2)
    peers = tuple(me + (1 - 2 * place[axis]) * w for axis, w in ((0, 8), (1, 4), (2, 2)))
    twin = me + 1 - 2 * core
    rcv = (rcv0, rcv1, rcv2)

    @pl.when(t == 0)
    def _():
        barrier = pltpu.get_barrier_semaphore()
        for peer in peers + (twin,):
            pl.semaphore_signal(barrier, inc=1, device_id=(peer,), device_id_type=MESH_ID)
        pl.semaphore_wait(barrier, 4)

    def pair_copy(item):
        return pltpu.make_async_remote_copy(
            src_ref=g_buf.at[item % SLOTS, :, :, :, :, 1 - core],
            dst_ref=pair_buf.at[item % SLOTS],
            send_sem=d2d_send.at[0, item % 2],
            recv_sem=d2d_recv.at[0, item % 2],
            device_id=(twin,),
            device_id_type=MESH_ID,
        )

    def cut(part, stage, value):
        index = [slice(None)] * 3
        for axis in ORDER[part][:stage]:
            index[axis] = place[axis]
        index[ORDER[part][stage]] = value
        return tuple(index)

    def rs_copy(item, stage, part):
        axis = ORDER[part][stage]
        return pltpu.make_async_remote_copy(
            src_ref=sum_buf.at[(item % SLOTS, part) + cut(part, stage, 1 - place[axis])],
            dst_ref=rcv[stage].at[item % SLOTS, part],
            send_sem=rs_send.at[stage, part, item % 2],
            recv_sem=rs_recv.at[stage, part, item % 2],
            device_id=(peers[axis],),
            device_id_type=MESH_ID,
        )

    def ag_copy(item, stage, part):
        index = [place[0], place[1], place[2]]
        for axis in ORDER[part][:stage]:
            index[axis] = slice(None)
        view = ag_buf.at[(item % AG_SLOTS, part) + tuple(index) + (core,)]
        return pltpu.make_async_remote_copy(
            src_ref=view,
            dst_ref=view,
            send_sem=ag_send.at[stage, part, item % 2],
            recv_sem=ag_recv.at[stage, part, item % 2],
            device_id=(peers[ORDER[part][stage]],),
            device_id_type=MESH_ID,
        )

    def twin_copy(item):
        view = ag_buf.at[item % AG_SLOTS, :, :, :, :, core]
        return pltpu.make_async_remote_copy(
            src_ref=view,
            dst_ref=view,
            send_sem=d2d_send.at[1, item % 2],
            recv_sem=d2d_recv.at[1, item % 2],
            device_id=(twin,),
            device_id_type=MESH_ID,
        )

    def out_copy(item):
        return pltpu.make_async_copy(ag_buf.at[item % AG_SLOTS], all_ref.at[n_items - 1 - item], out_sem.at[item % 2])

    def at_lag(lag):
        return (t >= lag) & (t < n_items + lag)

    @pl.when(t == 1)
    def _():
        g_rows[...] = grad_ref[...]

    @pl.when((t >= 1) & (t < n_items))
    def _():
        up_b = wu_ref[0].astype(BF16)
        down_b = wd_ref[0].astype(BF16)
        step = g_rows.shape[0] // CHUNKS
        grad_old = g_rows[...]
        for chunk in range(CHUNKS):
            sl = slice(chunk * step, (chunk + 1) * step)
            g_old = grad_old[sl, :]
            z_wide, slope = gelu_both(pre_ref[0, sl, :].astype(F32))
            z_buf[sl, :] = z_wide.astype(BF16)
            grad_z = jnp.dot(g_old, down_b, preferred_element_type=F32).astype(BF16)
            grad_a = (grad_z.astype(F32) * slope).astype(BF16)
            da_buf[sl, :] = grad_a
            centered, scale = norm_parts(xs_ref[0, sl, :].astype(F32))
            normed = centered * scale
            u_buf[sl, :] = normed.astype(BF16)
            grad_u = lax.dot_general(grad_a, up_b, LAST, preferred_element_type=F32).astype(BF16)
            grad_x = norm_pull(normed, scale, grad_u.astype(F32))
            g_rows[sl, :] = (g_old.astype(F32) + grad_x).astype(BF16)
        down_t = lax.dot_general(grad_old, z_buf[...], ROWS, preferred_element_type=F32).astype(BF16)
        up_g = lax.dot_general(u_buf[...], da_buf[...], ROWS, preferred_element_type=F32).astype(BF16)
        for part, value in enumerate((up_g[:128, :], down_t[:128, :], jnp.concatenate([down_t[128:, :], up_g[128:, :]], axis=0))):
            turned = value.T
            for dev in range(16):
                block = turned[dev * 48 : (dev + 1) * 48, :]
                g_buf[t % SLOTS, part, dev // 8, (dev // 4) % 2, (dev // 2) % 2, dev % 2] = block

    @pl.when(at_lag(9))
    def _():
        out_copy(t - 9).wait()

    @pl.when(at_lag(8))
    def _():
        item = t - 8
        twin_copy(item).wait()
        out_copy(item).start()

    @pl.when(at_lag(7))
    def _():
        item = t - 7
        for part in range(PARTS):
            ag_copy(item, 2, part).wait()
        twin_copy(item).start()

    for stage in (1, 0):

        @pl.when(at_lag(5 + stage))
        def _(stage=stage):
            item = t - 5 - stage
            for part in range(PARTS):
                ag_copy(item, stage, part).wait()
                ag_copy(item, stage + 1, part).start()

    @pl.when(at_lag(4))
    def _():
        item = t - 4
        for part in range(PARTS):
            rs_copy(item, 2, part).wait()

        def reduced(part):
            return (sum_buf[item % SLOTS, part, place[0], place[1], place[2]] + rcv[2][item % SLOTS, part]).astype(F32)

        def hand_on(part, mom):
            ag_buf[item % AG_SLOTS, part, place[0], place[1], place[2], core] = mom.astype(BF16)
            ag_copy(item, 0, part).start()

        @pl.when(t == 4)
        def _():
            for part in range(PARTS):
                mom = sc_ref[0, 0] * mh_ref[part] + reduced(part)
                nmh_ref[part] = mom
                hand_on(part, mom)

        @pl.when(t > 4)
        def _():
            mixed = reduced(2)
            up_a = sc_ref[0, 0] * mu_ref[0, :, :128] + reduced(0)
            down_a = sc_ref[0, 0] * md_ref[0, :, :128] + reduced(1)
            up_z = sc_ref[0, 0] * mu_ref[0, :, 128:] + mixed[:, 64:]
            down_z = sc_ref[0, 0] * md_ref[0, :, 128:] + mixed[:, :64]
            nmu_ref[0, :, :128] = up_a
            nmu_ref[0, :, 128:] = up_z
            nmd_ref[0, :, :128] = down_a
            nmd_ref[0, :, 128:] = down_z
            hand_on(0, up_a)
            hand_on(1, down_a)
            hand_on(2, jnp.concatenate([down_z, up_z], axis=1))

    for stage in (1, 0):

        @pl.when(at_lag(2 + stage))
        def _(stage=stage):
            item = t - 2 - stage
            for part in range(PARTS):
                rs_copy(item, stage, part).wait()
                kept = (item % SLOTS, part) + cut(part, stage, place[ORDER[part][stage]])
                sum_buf[kept] = sum_buf[kept] + rcv[stage][item % SLOTS, part]
                rs_copy(item, stage + 1, part).start()

    @pl.when(at_lag(1))
    def _():
        item = t - 1
        pair_copy(item).wait()
        for part in range(PARTS):
            sum_buf[item % SLOTS, part] = g_buf[item % SLOTS, part, :, :, :, core] + pair_buf[item % SLOTS, part]
            rs_copy(item, 0, part).start()

    @pl.when(t == 0)
    def _():
        g_buf[0] = gh_ref[...]
        pair_copy(0).start()

    @pl.when((t >= 1) & (t < n_items))
    def _():
        pair_copy(t).start()


def whole(shape):
    return pl.BlockSpec(shape, lambda i: (0,) * len(shape))


def solution(mesh):
    n_dev = mesh.shape["data"]

    def local_step(x_now, x_next, labels, w_up, w_down, w_head, mom_up, mom_down, mom_head, learn_rate, mom_decay):
        n_img, n_tok, width = x_now.shape
        n_layers, _, hidden = w_up.shape
        n_cls = w_head.shape[1]
        n_rows = -(-n_img * n_tok // (16 * CHUNKS)) * 16 * CHUNKS
        n_items = n_layers + 1
        cols = mom_up.shape[2]
        head_rows = mom_head.shape[0]
        n_tile = -(-n_cls // 128)
        head_each = head_rows * n_tile // PARTS

        down_t = w_down.transpose(0, 2, 1)
        per = 2 if n_layers % 2 == 0 else 1
        lab = jnp.pad(labels, (0, 8 - n_img)).reshape(8, 1)
        xs, pre, grad_rows, normed, grad_logits = pl.pallas_call(
            functools.partial(forward_kernel, n_img, n_tok, n_img * n_dev, n_cls),
            grid=(n_layers // per,),
            in_specs=[
                whole((n_img, width, n_tok)),
                whole((8, 1)),
                pl.BlockSpec((per, width, hidden), lambda i: (i, 0, 0)),
                pl.BlockSpec((per, width, hidden), lambda i: (i, 0, 0)),
                whole(w_head.shape),
            ],
            out_specs=[
                pl.BlockSpec((per, n_rows, width), lambda i: (i, 0, 0)),
                pl.BlockSpec((per, n_rows, hidden), lambda i: (i, 0, 0)),
                whole((n_rows, width)),
                whole((8, width)),
                whole((8, n_cls)),
            ],
            out_shape=[
                jax.ShapeDtypeStruct((n_layers, n_rows, width), BF16),
                jax.ShapeDtypeStruct((n_layers, n_rows, hidden), BF16),
                jax.ShapeDtypeStruct((n_rows, width), BF16),
                jax.ShapeDtypeStruct((8, width), BF16),
                jax.ShapeDtypeStruct((8, n_cls), BF16),
            ],
            scratch_shapes=[pltpu.VMEM((n_rows, width), F32), pltpu.VMEM((n_rows, width), BF16)],
            compiler_params=pltpu.CompilerParams(vmem_limit_bytes=VMEM_LIMIT),
            name="step_forward",
        )(x_now.transpose(0, 2, 1), lab, w_up, down_t, w_head)

        def head_blocks(values):
            n_part = values.shape[0] // head_rows
            wide = jnp.pad(values, ((0, 0), (0, n_tile * 128 - n_cls)))
            blocks = wide.reshape(n_part, PARTS, head_each, 128)
            return jnp.pad(blocks, ((0, 0), (0, 0), (0, cols - head_each), (0, 0)))

        head_grad = lax.dot_general(normed, grad_logits, ROWS, preferred_element_type=F32).astype(BF16)
        head_g = head_blocks(head_grad).transpose(1, 0, 2, 3).reshape(PARTS, 2, 2, 2, 2, cols, 128)
        def layer_at(t):
            return jnp.clip(n_items - 1 - t, 0, n_layers - 1)

        def update_at(t):
            return n_items - 1 - jnp.clip(t - 4, 1, n_items - 1)

        block = (SLOTS, PARTS, 2, 2, 2)
        mom_head_new, mom_up_new, new_mom_down, gathered = pl.pallas_call(
            functools.partial(backward_kernel, n_items),
            grid=(n_items + 9,),
            in_specs=[
                pl.BlockSpec(memory_space=pltpu.SMEM),
                whole((PARTS, 2, 2, 2, 2, cols, 128)),
                whole((n_rows, width)),
                pl.BlockSpec((1, n_rows, width), lambda t: (layer_at(t), 0, 0)),
                pl.BlockSpec((1, n_rows, hidden), lambda t: (layer_at(t), 0, 0)),
                pl.BlockSpec((1, width, hidden), lambda t: (layer_at(t), 0, 0)),
                pl.BlockSpec((1, width, hidden), lambda t: (layer_at(t), 0, 0)),
                whole((PARTS, cols, 128)),
                pl.BlockSpec((1, cols, width), lambda t: (update_at(t), 0, 0)),
                pl.BlockSpec((1, cols, width), lambda t: (update_at(t), 0, 0)),
            ],
            out_specs=[
                whole((PARTS, cols, 128)),
                pl.BlockSpec((1, cols, width), lambda t: (update_at(t), 0, 0)),
                pl.BlockSpec((1, cols, width), lambda t: (update_at(t), 0, 0)),
                pl.BlockSpec(memory_space=pl.ANY),
            ],
            out_shape=[
                jax.ShapeDtypeStruct((PARTS, cols, 128), F32),
                jax.ShapeDtypeStruct((n_layers, cols, width), F32),
                jax.ShapeDtypeStruct((n_layers, cols, width), F32),
                jax.ShapeDtypeStruct((n_items, PARTS, 2, 2, 2, 2, cols, 128), BF16),
            ],
            scratch_shapes=[
                pltpu.VMEM((n_rows, width), BF16),
                pltpu.VMEM((n_rows, hidden), BF16),
                pltpu.VMEM((n_rows, hidden), BF16),
                pltpu.VMEM((n_rows, width), BF16),
                pltpu.VMEM(block + (2, cols, 128), BF16),
                pltpu.VMEM(block + (cols, 128), BF16),
                pltpu.VMEM(block + (cols, 128), BF16),
                pltpu.VMEM((SLOTS, PARTS, 2, 2, cols, 128), BF16),
                pltpu.VMEM((SLOTS, PARTS, 2, cols, 128), BF16),
                pltpu.VMEM((SLOTS, PARTS, cols, 128), BF16),
                pltpu.VMEM((AG_SLOTS, PARTS, 2, 2, 2, 2, cols, 128), BF16),
                pltpu.SemaphoreType.DMA((2, 2)),
                pltpu.SemaphoreType.DMA((2, 2)),
                pltpu.SemaphoreType.DMA((3, PARTS, 2)),
                pltpu.SemaphoreType.DMA((3, PARTS, 2)),
                pltpu.SemaphoreType.DMA((3, PARTS, 2)),
                pltpu.SemaphoreType.DMA((3, PARTS, 2)),
                pltpu.SemaphoreType.DMA((2,)),
            ],
            compiler_params=pltpu.CompilerParams(vmem_limit_bytes=VMEM_LIMIT, collective_id=0, has_side_effects=True),
            name="step_backward",
        )(mom_decay.reshape(1, 1), head_g, grad_rows, xs, pre, w_up, down_t, head_blocks(mom_head)[0], mom_up.transpose(0, 2, 1), mom_down)

        gathered = gathered.reshape(n_items, PARTS, n_dev * cols, 128)
        head_all = gathered[n_layers].reshape(PARTS, n_dev, cols, 128)[:, :, :head_each]
        head_all = head_all.transpose(1, 0, 2, 3).reshape(n_dev * head_rows, n_tile * 128)[:, :n_cls]
        new_w_head = w_head - learn_rate * head_all.astype(F32)

        new_w_up, new_down_t, logits = pl.pallas_call(
            functools.partial(next_kernel, n_img, n_tok),
            grid=(n_layers // per,),
            in_specs=[
                pl.BlockSpec(memory_space=pltpu.SMEM),
                whole((n_img, width, n_tok)),
                pl.BlockSpec((per, width, hidden), lambda i: (i, 0, 0)),
                pl.BlockSpec((per, width, hidden), lambda i: (i, 0, 0)),
                pl.BlockSpec((per, PARTS, n_dev * cols, 128), lambda i: (i, 0, 0, 0)),
                whole(w_head.shape),
            ],
            out_specs=[
                pl.BlockSpec((per, width, hidden), lambda i: (i, 0, 0)),
                pl.BlockSpec((per, width, hidden), lambda i: (i, 0, 0)),
                whole((8, n_cls)),
            ],
            out_shape=[
                jax.ShapeDtypeStruct(w_up.shape, F32),
                jax.ShapeDtypeStruct(w_up.shape, F32),
                jax.ShapeDtypeStruct((8, n_cls), F32),
            ],
            scratch_shapes=[pltpu.VMEM((n_rows, width), F32), pltpu.VMEM((n_rows, width), BF16)],
            compiler_params=pltpu.CompilerParams(vmem_limit_bytes=VMEM_LIMIT),
            name="step_next",
        )(learn_rate.reshape(1, 1), x_next.transpose(0, 2, 1), w_up, down_t, gathered, new_w_head)

        new_mom_head = mom_head_new[:, :head_each].reshape(head_rows, n_tile * 128)[:, :n_cls]
        return (logits[:n_img], new_w_up, new_down_t.transpose(0, 2, 1), new_w_head, mom_up_new.transpose(0, 2, 1), new_mom_down, new_mom_head)

    spec_up = P(None, None, "data")
    spec_down = P(None, "data", None)
    spec_head = P("data", None)
    return jax.shard_map(
        local_step,
        mesh=mesh,
        in_specs=(P("data"), P("data"), P("data"), P(), P(), P(), spec_up, spec_down, spec_head, P(), P()),
        out_specs=(P("data"), P(), P(), P(), spec_up, spec_down, spec_head),
        check_vma=False,
    )
```

```python
import functools

import jax
import jax.numpy as jnp
from jax import lax
from jax.experimental import pallas as pl
from jax.experimental.pallas import tpu as pltpu
from jax.sharding import PartitionSpec as P

LN_EPS = 1e-6
GELU_C = 0.7978845608028654
GELU_A = 0.044715
F32 = jnp.float32
BF16 = jnp.bfloat16
LAST = (((1,), (1,)), ((), ()))
ROWS = (((0,), (0,)), ((), ()))
MESH_ID = pl.DeviceIdType.MESH
VMEM_LIMIT = 66_000_000
CHUNKS = 5
SLOTS = 4
PARTS = 3
ORDER = ((0, 1, 2), (1, 2, 0), (2, 0, 1))


def norm_parts(values):
    mean_v = jnp.mean(values, axis=-1, keepdims=True)
    centered = values - mean_v
    var_v = jnp.mean(centered * centered, axis=-1, keepdims=True)
    return centered, lax.rsqrt(var_v + LN_EPS)


def norm_pull(normed, scale, grad):
    mean_g = jnp.mean(grad, axis=-1, keepdims=True)
    mean_gn = jnp.mean(grad * normed, axis=-1, keepdims=True)
    return scale * (grad - mean_g - normed * mean_gn)


def gelu(values):
    inner = values * (GELU_C + (GELU_C * GELU_A) * (values * values))
    return values * (0.5 + 0.5 * jnp.tanh(inner))


def gelu_both(values):
    square = values * values
    share = 0.5 + 0.5 * jnp.tanh(values * (GELU_C + (GELU_C * GELU_A) * square))
    out = values * share
    slope = share + (out * (1.0 - share)) * (2.0 * GELU_C + (6.0 * GELU_C * GELU_A) * square)
    return out, slope


def pack_rows(x_ref, wide, rows, n_img, n_tok):
    wide[...] = jnp.zeros_like(wide)
    for img in range(n_img):
        wide[img * n_tok : (img + 1) * n_tok, :] = x_ref[img].astype(F32).T
    rows[...] = wide[...].astype(BF16)


def pool_mask(shape, n_img, n_tok, row_axis):
    row = lax.broadcasted_iota(jnp.int32, shape, row_axis)
    img = lax.broadcasted_iota(jnp.int32, shape, 1 - row_axis)
    inside = (row >= img * n_tok) & (row < (img + 1) * n_tok) & (img < n_img)
    return jnp.where(inside, 1.0, 0.0).astype(BF16)


def pooled_norm(rows, n_img, n_tok):
    n_rows = rows.shape[0]
    mask = pool_mask((8, n_rows), n_img, n_tok, 1)
    pooled = jnp.dot(mask, rows[...], preferred_element_type=F32) * (1.0 / n_tok)
    centered, scale = norm_parts(pooled)
    return centered * scale, scale


def forward_kernel(n_img, n_tok, batch_total, n_cls, x_ref, lab_ref, wu_ref, wd_ref, wh_ref, xs_ref, pre_ref, grad_ref, norm_ref, gl_ref, wide, rows):
    layer = pl.program_id(0)

    @pl.when(layer == 0)
    def _():
        pack_rows(x_ref, wide, rows, n_img, n_tok)

    step = rows.shape[0] // CHUNKS
    for sub in range(wu_ref.shape[0]):
        up_b = wu_ref[sub].astype(BF16)
        down_b = wd_ref[sub].astype(BF16)
        for chunk in range(CHUNKS):
            sl = slice(chunk * step, (chunk + 1) * step)
            x_rows = rows[sl, :]
            xs_ref[sub, sl, :] = x_rows
            x_wide = x_rows.astype(F32)
            centered, scale = norm_parts(x_wide)
            u_rows = (centered * scale).astype(BF16)
            pre = jnp.dot(u_rows, up_b, preferred_element_type=F32).astype(BF16)
            pre_ref[sub, sl, :] = pre
            z_rows = gelu(pre.astype(F32)).astype(BF16)
            y_rows = lax.dot_general(z_rows, down_b, LAST, preferred_element_type=F32).astype(BF16)
            rows[sl, :] = (x_wide + y_rows.astype(F32)).astype(BF16)

    @pl.when(layer == pl.num_programs(0) - 1)
    def _():
        normed, scale = pooled_norm(rows, n_img, n_tok)
        normed_b = normed.astype(BF16)
        head_b = wh_ref[...].astype(BF16)
        logits = jnp.dot(normed_b, head_b, preferred_element_type=F32)
        top = jnp.max(logits, axis=-1, keepdims=True)
        exps = jnp.exp(logits - top)
        probs = exps / jnp.sum(exps, axis=-1, keepdims=True)
        classes = lax.broadcasted_iota(jnp.int32, logits.shape, 1)
        image = lax.broadcasted_iota(jnp.int32, logits.shape, 0)
        targets = jnp.where(classes == lab_ref[...], 1.0, 0.0)
        grad_logits = jnp.where(image < n_img, (probs - targets) * (1.0 / batch_total), 0.0)
        grad_b = grad_logits.astype(BF16)
        gl_ref[...] = grad_b
        norm_ref[...] = normed_b
        grad_normed = lax.dot_general(grad_b, head_b, LAST, preferred_element_type=F32).astype(BF16)
        grad_pooled = norm_pull(normed, scale, grad_normed.astype(F32))
        per_row = (grad_pooled / n_tok).astype(BF16)
        spread = pool_mask((rows.shape[0], 8), n_img, n_tok, 0)
        grad_ref[...] = jnp.dot(spread, per_row, preferred_element_type=F32).astype(BF16)


def update_kernel(
    n_items, n_img, n_tok, sc_ref, gh_ref, grad_ref, xs_ref, pre_ref, wu_ref, wd_ref, mh_ref, mu_ref, md_ref, x_ref,
    nmh_ref, nmu_ref, nmd_ref, nwu_ref, nwd_ref, head_ref, norm_ref,
    rows, z_buf, da_buf, u_buf, wide, g_buf, pair_buf, sum_buf, rcv0, rcv1, rcv2, all_buf,
    d2d_send, d2d_recv, twin_send, twin_recv, rs_send, rs_recv, ag_send, ag_recv,
):
    t = pl.program_id(0)
    me = lax.axis_index("data")
    core = lax.rem(me, 2)
    place = (lax.div(me, 8), lax.rem(lax.div(me, 4), 2), lax.rem(lax.div(me, 2), 2))
    peers = tuple(me + (1 - 2 * place[axis]) * w for axis, w in ((0, 8), (1, 4), (2, 2)))
    twin = me + 1 - 2 * core
    rcv = (rcv0, rcv1, rcv2)
    last_update, n_early, n_late, first_next = ticks(n_items)

    @pl.when(t == 0)
    def _():
        barrier = pltpu.get_barrier_semaphore()
        for peer in peers + (twin,):
            pl.semaphore_signal(barrier, inc=1, device_id=(peer,), device_id_type=MESH_ID)
        pl.semaphore_wait(barrier, 4)

    def pair_copy(item):
        slot = lax.rem(item, 2)
        return pltpu.make_async_remote_copy(
            src_ref=g_buf.at[slot, :, :, :, :, 1 - core],
            dst_ref=pair_buf.at[slot],
            send_sem=d2d_send.at[slot],
            recv_sem=d2d_recv.at[slot],
            device_id=(twin,),
            device_id_type=MESH_ID,
        )

    def cut(part, stage, value):
        index = [slice(None)] * 3
        for axis in ORDER[part][:stage]:
            index[axis] = place[axis]
        index[ORDER[part][stage]] = value
        return tuple(index)

    def rs_copy(item, stage, part):
        axis = ORDER[part][stage]
        slot = lax.rem(item, 2)
        return pltpu.make_async_remote_copy(
            src_ref=sum_buf.at[(lax.rem(item, SLOTS), part) + cut(part, stage, 1 - place[axis])],
            dst_ref=rcv[stage].at[slot, part],
            send_sem=rs_send.at[stage, part, slot],
            recv_sem=rs_recv.at[stage, part, slot],
            device_id=(peers[axis],),
            device_id_type=MESH_ID,
        )

    def launched(tick):
        even = lax.rem(tick, 2) == 0
        early = (tick >= 4) & (tick < 4 + 2 * n_early) & even
        late = (tick >= last_update - 1) & (tick <= last_update + n_late)
        order = jnp.where(tick == last_update - 1, n_items - 2, jnp.where(tick == last_update, n_items - 1, n_items - 2 + last_update - tick))
        return jnp.where(tick < last_update - 1, lax.div(tick - 4, 2), order), early | late

    def ag_copy(tick, item, stage, part):
        index = [place[0], place[1], place[2]]
        for axis in ORDER[part][:stage]:
            index[axis] = slice(None)
        view = all_buf.at[(item, part) + tuple(index) + (core,)]
        return pltpu.make_async_remote_copy(
            src_ref=view,
            dst_ref=view,
            send_sem=ag_send.at[stage, part, lax.rem(tick, 4)],
            recv_sem=ag_recv.at[stage, part, lax.rem(tick, 4)],
            device_id=(peers[ORDER[part][stage]],),
            device_id_type=MESH_ID,
        )

    def twin_copy(tick, item):
        view = all_buf.at[item, :, :, :, :, core]
        return pltpu.make_async_remote_copy(
            src_ref=view,
            dst_ref=view,
            send_sem=twin_send.at[lax.rem(tick, 4)],
            recv_sem=twin_recv.at[lax.rem(tick, 4)],
            device_id=(twin,),
            device_id_type=MESH_ID,
        )

    def at_lag(lag):
        return (t >= lag) & (t < n_items + lag)

    @pl.when(t == 1)
    def _():
        rows[...] = grad_ref[...]

    @pl.when((t >= 1) & (t < n_items))
    def _():
        up_b = wu_ref[0].astype(BF16)
        down_b = wd_ref[0].astype(BF16)
        step = rows.shape[0] // CHUNKS
        grad_old = rows[...]
        for chunk in range(CHUNKS):
            sl = slice(chunk * step, (chunk + 1) * step)
            g_old = grad_old[sl, :]
            z_wide, slope = gelu_both(pre_ref[0, sl, :].astype(F32))
            z_buf[sl, :] = z_wide.astype(BF16)
            grad_z = jnp.dot(g_old, down_b, preferred_element_type=F32).astype(BF16)
            grad_a = (grad_z.astype(F32) * slope).astype(BF16)
            da_buf[sl, :] = grad_a
            centered, scale = norm_parts(xs_ref[0, sl, :].astype(F32))
            normed = centered * scale
            u_buf[sl, :] = normed.astype(BF16)
            grad_u = lax.dot_general(grad_a, up_b, LAST, preferred_element_type=F32).astype(BF16)
            grad_x = norm_pull(normed, scale, grad_u.astype(F32))
            rows[sl, :] = (g_old.astype(F32) + grad_x).astype(BF16)
        down_t = lax.dot_general(grad_old, z_buf[...], ROWS, preferred_element_type=F32).astype(BF16)
        up_g = lax.dot_general(u_buf[...], da_buf[...], ROWS, preferred_element_type=F32).astype(BF16)
        for part, value in enumerate((up_g[:128, :], down_t[:128, :], jnp.concatenate([down_t[128:, :], up_g[128:, :]], axis=0))):
            turned = value.T
            for dev in range(16):
                block = turned[dev * 48 : (dev + 1) * 48, :]
                g_buf[lax.rem(t, 2), part, dev // 8, (dev // 4) % 2, (dev // 2) % 2, dev % 2] = block

    for stage in (4, 3, 2, 1):
        item, busy = launched(t - stage)

        @pl.when(busy)
        def _(stage=stage, item=item):
            tick = t - stage
            if stage == 4:
                twin_copy(tick, item).wait()
                return
            for part in range(PARTS):
                ag_copy(tick, item, stage - 1, part).wait()
                if stage < 3:
                    ag_copy(tick, item, stage, part).start()
            if stage == 3:
                twin_copy(tick, item).start()

    @pl.when(at_lag(4))
    def _():
        item = t - 4
        for part in range(PARTS):
            rs_copy(item, 2, part).wait()

        def reduced(part):
            return (sum_buf[lax.rem(item, SLOTS), part, place[0], place[1], place[2]] + rcv[2][lax.rem(item, 2), part]).astype(F32)

        def hand_on(part, mom):
            all_buf[item, part, place[0], place[1], place[2], core] = mom.astype(BF16)

        @pl.when(t == 4)
        def _():
            for part in range(PARTS):
                mom = sc_ref[0, 0] * mh_ref[part] + reduced(part)
                nmh_ref[part] = mom
                hand_on(part, mom)

        @pl.when(t > 4)
        def _():
            mixed = reduced(2)
            up_a = sc_ref[0, 0] * mu_ref[0, :, :128] + reduced(0)
            down_a = sc_ref[0, 0] * md_ref[0, :, :128] + reduced(1)
            up_z = sc_ref[0, 0] * mu_ref[0, :, 128:] + mixed[:, 64:]
            down_z = sc_ref[0, 0] * md_ref[0, :, 128:] + mixed[:, :64]
            nmu_ref[0, :, :128] = up_a
            nmu_ref[0, :, 128:] = up_z
            nmd_ref[0, :, :128] = down_a
            nmd_ref[0, :, 128:] = down_z
            hand_on(0, up_a)
            hand_on(1, down_a)
            hand_on(2, jnp.concatenate([down_z, up_z], axis=1))

    item, busy = launched(t)

    @pl.when(busy)
    def _():
        for part in range(PARTS):
            ag_copy(t, item, 0, part).start()

    for stage in (1, 0):

        @pl.when(at_lag(2 + stage))
        def _(stage=stage):
            item = t - 2 - stage
            for part in range(PARTS):
                rs_copy(item, stage, part).wait()
                kept = (lax.rem(item, SLOTS), part) + cut(part, stage, place[ORDER[part][stage]])
                sum_buf[kept] = sum_buf[kept] + rcv[stage][lax.rem(item, 2), part]
                rs_copy(item, stage + 1, part).start()

    @pl.when(at_lag(1))
    def _():
        item = t - 1
        pair_copy(item).wait()
        for part in range(PARTS):
            sum_buf[lax.rem(item, SLOTS), part] = g_buf[lax.rem(item, 2), part, :, :, :, core] + pair_buf[lax.rem(item, 2), part]
            rs_copy(item, 0, part).start()

    @pl.when(t == 0)
    def _():
        g_buf[0] = gh_ref[...]
        pair_copy(0).start()

    @pl.when((t >= 1) & (t < n_items))
    def _():
        pair_copy(t).start()

    @pl.when(t == n_items)
    def _():
        pack_rows(x_ref, wide, rows, n_img, n_tok)

    @pl.when(t >= first_next)
    def _():
        item = n_items - 1 - (t - first_next)
        rate = sc_ref[0, 1]

        def gathered(part):
            return all_buf[item, part].reshape(16 * 48, 128).T.astype(F32)

        mixed = gathered(2)
        nwu_ref[0, :128, :] = wu_ref[0, :128, :] - rate * gathered(0)
        nwu_ref[0, 128:, :] = wu_ref[0, 128:, :] - rate * mixed[64:, :]
        nwd_ref[0, :128, :] = wd_ref[0, :128, :] - rate * gathered(1)
        nwd_ref[0, 128:, :] = wd_ref[0, 128:, :] - rate * mixed[:64, :]
        up_b = nwu_ref[0].astype(BF16)
        down_b = nwd_ref[0].astype(BF16)
        step = rows.shape[0] // CHUNKS
        for chunk in range(CHUNKS):
            sl = slice(chunk * step, (chunk + 1) * step)
            x_wide = rows[sl, :].astype(F32)
            centered, scale = norm_parts(x_wide)
            u_rows = (centered * scale).astype(BF16)
            pre = jnp.dot(u_rows, up_b, preferred_element_type=F32).astype(BF16)
            z_rows = gelu(pre.astype(F32)).astype(BF16)
            y_rows = lax.dot_general(z_rows, down_b, LAST, preferred_element_type=F32).astype(BF16)
            rows[sl, :] = (x_wide + y_rows.astype(F32)).astype(BF16)

    @pl.when(t == pl.num_programs(0) - 1)
    def _():
        normed, _ = pooled_norm(rows, n_img, n_tok)
        norm_ref[...] = normed.astype(BF16)
        head_ref[...] = all_buf[0]


def ticks(n_items):
    last_update = n_items + 3
    n_early = (n_items - 3) // 2 + 1
    return last_update, n_early, n_items - 2 - n_early, last_update + 4


def whole(shape):
    return pl.BlockSpec(shape, lambda i: (0,) * len(shape))


def solution(mesh):
    n_dev = mesh.shape["data"]

    def local_step(x_now, x_next, labels, w_up, w_down, w_head, mom_up, mom_down, mom_head, learn_rate, mom_decay):
        n_img, n_tok, width = x_now.shape
        n_layers, _, hidden = w_up.shape
        n_cls = w_head.shape[1]
        n_rows = -(-n_img * n_tok // (16 * CHUNKS)) * 16 * CHUNKS
        n_items = n_layers + 1
        cols = mom_up.shape[2]
        head_rows = mom_head.shape[0]
        n_tile = -(-n_cls // 128)
        head_each = head_rows * n_tile // PARTS

        down_t = w_down.transpose(0, 2, 1)
        per = 2 if n_layers % 2 == 0 else 1
        lab = jnp.pad(labels, (0, 8 - n_img)).reshape(8, 1)
        xs, pre, grad_rows, normed, grad_logits = pl.pallas_call(
            functools.partial(forward_kernel, n_img, n_tok, n_img * n_dev, n_cls),
            grid=(n_layers // per,),
            in_specs=[
                whole((n_img, width, n_tok)),
                whole((8, 1)),
                pl.BlockSpec((per, width, hidden), lambda i: (i, 0, 0)),
                pl.BlockSpec((per, width, hidden), lambda i: (i, 0, 0)),
                whole(w_head.shape),
            ],
            out_specs=[
                pl.BlockSpec((per, n_rows, width), lambda i: (i, 0, 0)),
                pl.BlockSpec((per, n_rows, hidden), lambda i: (i, 0, 0)),
                whole((n_rows, width)),
                whole((8, width)),
                whole((8, n_cls)),
            ],
            out_shape=[
                jax.ShapeDtypeStruct((n_layers, n_rows, width), BF16),
                jax.ShapeDtypeStruct((n_layers, n_rows, hidden), BF16),
                jax.ShapeDtypeStruct((n_rows, width), BF16),
                jax.ShapeDtypeStruct((8, width), BF16),
                jax.ShapeDtypeStruct((8, n_cls), BF16),
            ],
            scratch_shapes=[pltpu.VMEM((n_rows, width), F32), pltpu.VMEM((n_rows, width), BF16)],
            compiler_params=pltpu.CompilerParams(vmem_limit_bytes=VMEM_LIMIT),
            name="step_forward",
        )(x_now.transpose(0, 2, 1), lab, w_up, down_t, w_head)

        def head_blocks(values):
            n_part = values.shape[0] // head_rows
            wide = jnp.pad(values, ((0, 0), (0, n_tile * 128 - n_cls)))
            blocks = wide.reshape(n_part, PARTS, head_each, 128)
            return jnp.pad(blocks, ((0, 0), (0, 0), (0, cols - head_each), (0, 0)))

        head_grad = lax.dot_general(normed, grad_logits, ROWS, preferred_element_type=F32).astype(BF16)
        head_g = head_blocks(head_grad).transpose(1, 0, 2, 3).reshape(PARTS, 2, 2, 2, 2, cols, 128)
        first_next = ticks(n_items)[3]

        def layer_at(t):
            return jnp.where(t < n_items, jnp.minimum(n_items - 1 - t, n_layers - 1), jnp.maximum(t - first_next, 0))

        def saved_at(t):
            return jnp.clip(n_items - 1 - t, 0, n_layers - 1)

        def update_at(t):
            return n_items - 1 - jnp.clip(t - 4, 1, n_items - 1)

        def next_at(t):
            return jnp.maximum(t - first_next, 0)

        block = (PARTS, 2, 2, 2)
        mom_head_new, mom_up_new, new_mom_down, new_w_up, new_down_t, head_all, normed = pl.pallas_call(
            functools.partial(update_kernel, n_items, n_img, n_tok),
            grid=(first_next + n_layers,),
            in_specs=[
                pl.BlockSpec(memory_space=pltpu.SMEM),
                whole((PARTS, 2, 2, 2, 2, cols, 128)),
                whole((n_rows, width)),
                pl.BlockSpec((1, n_rows, width), lambda t: (saved_at(t), 0, 0)),
                pl.BlockSpec((1, n_rows, hidden), lambda t: (saved_at(t), 0, 0)),
                pl.BlockSpec((1, width, hidden), lambda t: (layer_at(t), 0, 0)),
                pl.BlockSpec((1, width, hidden), lambda t: (layer_at(t), 0, 0)),
                whole((PARTS, cols, 128)),
                pl.BlockSpec((1, cols, width), lambda t: (update_at(t), 0, 0)),
                pl.BlockSpec((1, cols, width), lambda t: (update_at(t), 0, 0)),
                whole((n_img, width, n_tok)),
            ],
            out_specs=[
                whole((PARTS, cols, 128)),
                pl.BlockSpec((1, cols, width), lambda t: (update_at(t), 0, 0)),
                pl.BlockSpec((1, cols, width), lambda t: (update_at(t), 0, 0)),
                pl.BlockSpec((1, width, hidden), lambda t: (next_at(t), 0, 0)),
                pl.BlockSpec((1, width, hidden), lambda t: (next_at(t), 0, 0)),
                whole((PARTS, 2, 2, 2, 2, cols, 128)),
                whole((8, width)),
            ],
            out_shape=[
                jax.ShapeDtypeStruct((PARTS, cols, 128), F32),
                jax.ShapeDtypeStruct((n_layers, cols, width), F32),
                jax.ShapeDtypeStruct((n_layers, cols, width), F32),
                jax.ShapeDtypeStruct(w_up.shape, F32),
                jax.ShapeDtypeStruct(w_up.shape, F32),
                jax.ShapeDtypeStruct((PARTS, 2, 2, 2, 2, cols, 128), BF16),
                jax.ShapeDtypeStruct((8, width), BF16),
            ],
            scratch_shapes=[
                pltpu.VMEM((n_rows, width), BF16),
                pltpu.VMEM((n_rows, hidden), BF16),
                pltpu.VMEM((n_rows, hidden), BF16),
                pltpu.VMEM((n_rows, width), BF16),
                pltpu.VMEM((n_rows, width), F32),
                pltpu.VMEM((2,) + block + (2, cols, 128), BF16),
                pltpu.VMEM((2,) + block + (cols, 128), BF16),
                pltpu.VMEM((SLOTS,) + block + (cols, 128), BF16),
                pltpu.VMEM((2, PARTS, 2, 2, cols, 128), BF16),
                pltpu.VMEM((2, PARTS, 2, cols, 128), BF16),
                pltpu.VMEM((2, PARTS, cols, 128), BF16),
                pltpu.VMEM((n_items,) + block + (2, cols, 128), BF16),
                pltpu.SemaphoreType.DMA((2,)),
                pltpu.SemaphoreType.DMA((2,)),
                pltpu.SemaphoreType.DMA((4,)),
                pltpu.SemaphoreType.DMA((4,)),
                pltpu.SemaphoreType.DMA((3, PARTS, 2)),
                pltpu.SemaphoreType.DMA((3, PARTS, 2)),
                pltpu.SemaphoreType.DMA((3, PARTS, 4)),
                pltpu.SemaphoreType.DMA((3, PARTS, 4)),
            ],
            compiler_params=pltpu.CompilerParams(vmem_limit_bytes=VMEM_LIMIT, collective_id=0, has_side_effects=True),
            name="step_update",
        )(
            jnp.stack([mom_decay, learn_rate]).reshape(1, 2), head_g, grad_rows, xs, pre, w_up, down_t,
            head_blocks(mom_head)[0], mom_up.transpose(0, 2, 1), mom_down, x_next.transpose(0, 2, 1),
        )

        head_all = head_all.reshape(PARTS, n_dev, cols, 128)[:, :, :head_each]
        head_all = head_all.transpose(1, 0, 2, 3).reshape(n_dev * head_rows, n_tile * 128)[:, :n_cls]
        new_w_head = w_head - learn_rate * head_all.astype(F32)
        logits = jnp.dot(normed, new_w_head.astype(BF16), preferred_element_type=F32)
        new_mom_head = mom_head_new[:, :head_each].reshape(head_rows, n_tile * 128)[:, :n_cls]
        return (logits[:n_img], new_w_up, new_down_t.transpose(0, 2, 1), new_w_head, mom_up_new.transpose(0, 2, 1), new_mom_down, new_mom_head)

    spec_up = P(None, None, "data")
    spec_down = P(None, "data", None)
    spec_head = P("data", None)
    return jax.shard_map(
        local_step,
        mesh=mesh,
        in_specs=(P("data"), P("data"), P("data"), P(), P(), P(), spec_up, spec_down, spec_head, P(), P()),
        out_specs=(P("data"), P(), P(), P(), spec_up, spec_down, spec_head),
        check_vma=False,
    )
```

```python
import functools

import jax
import jax.numpy as jnp
from jax import lax
from jax.experimental import pallas as pl
from jax.experimental.pallas import tpu as pltpu
from jax.sharding import PartitionSpec as P

LN_EPS = 1e-6
GELU_C = 0.7978845608028654
GELU_A = 0.044715
F32 = jnp.float32
BF16 = jnp.bfloat16
LAST = (((1,), (1,)), ((), ()))
ROWS = (((0,), (0,)), ((), ()))
MESH_ID = pl.DeviceIdType.MESH
VMEM_LIMIT = 62 * 1024 * 1024
CHUNKS = 5
SLOTS = 4
AG_SLOTS = 8
PARTS = 3
POOL = 16
ORDER = ((0, 1, 2), (1, 2, 0), (2, 0, 1))


def norm_parts(values):
    mean_v = jnp.mean(values, axis=-1, keepdims=True)
    centered = values - mean_v
    var_v = jnp.mean(centered * centered, axis=-1, keepdims=True)
    return centered, lax.rsqrt(var_v + LN_EPS)


def norm_pull(normed, scale, grad):
    mean_g = jnp.mean(grad, axis=-1, keepdims=True)
    mean_gn = jnp.mean(grad * normed, axis=-1, keepdims=True)
    return scale * (grad - mean_g - normed * mean_gn)


def gelu(values):
    inner = values * (GELU_C + (GELU_C * GELU_A) * (values * values))
    return values * (0.5 + 0.5 * jnp.tanh(inner))


def gelu_both(values):
    square = values * values
    share = 0.5 + 0.5 * jnp.tanh(values * (GELU_C + (GELU_C * GELU_A) * square))
    out = values * share
    slope = share + (out * (1.0 - share)) * (2.0 * GELU_C + (6.0 * GELU_C * GELU_A) * square)
    return out, slope


def pack_rows(x_ref, wide, rows, n_img, n_tok):
    wide[...] = jnp.zeros_like(wide)
    for img in range(n_img):
        wide[img * n_tok : (img + 1) * n_tok, :] = x_ref[img].astype(F32).T
    rows[...] = wide[...].astype(BF16)


def pool_mask(shape, n_img, n_tok, row_axis):
    row = lax.broadcasted_iota(jnp.int32, shape, row_axis)
    img = lax.broadcasted_iota(jnp.int32, shape, 1 - row_axis)
    inside = (row >= img * n_tok) & (row < (img + 1) * n_tok) & (img < n_img)
    return jnp.where(inside, 1.0, 0.0).astype(BF16)


def pooled_norm(rows, n_img, n_tok):
    n_rows = rows.shape[0]
    mask = pool_mask((POOL, n_rows), n_img, n_tok, 1)
    pooled = jnp.dot(mask, rows[...], preferred_element_type=F32) * (1.0 / n_tok)
    centered, scale = norm_parts(pooled)
    return centered * scale, scale


def forward_kernel(
    n_img, n_tok, batch_total, head_rows, lab_ref, x_hbm, wu_ref, wd_ref, wh_hbm, xs_ref, pre_ref, grad_hbm, hg_hbm,
    x_ref, wh_ref, wide, rows, staged, hg_ref, sems,
):
    layer = pl.program_id(0)
    x_copy = pltpu.make_async_copy(x_hbm, x_ref, sems.at[0])
    wh_copy = pltpu.make_async_copy(wh_hbm, wh_ref, sems.at[1])

    @pl.when(layer == 0)
    def _():
        x_copy.start()
        wh_copy.start()
        x_copy.wait()
        pack_rows(x_ref, wide, rows, n_img, n_tok)

    step = rows.shape[0] // CHUNKS
    for sub in range(wu_ref.shape[0]):
        up_b = wu_ref[sub].astype(BF16)
        down_b = wd_ref[sub].astype(BF16)
        for chunk in range(CHUNKS):
            sl = slice(chunk * step, (chunk + 1) * step)
            x_rows = rows[sl, :]
            xs_ref[sub, sl, :] = x_rows
            x_wide = x_rows.astype(F32)
            centered, scale = norm_parts(x_wide)
            u_rows = (centered * scale).astype(BF16)
            pre = jnp.dot(u_rows, up_b, preferred_element_type=F32).astype(BF16)
            pre_ref[sub, sl, :] = pre
            z_rows = gelu(pre.astype(F32)).astype(BF16)
            y_rows = lax.dot_general(z_rows, down_b, LAST, preferred_element_type=F32).astype(BF16)
            rows[sl, :] = (x_wide + y_rows.astype(F32)).astype(BF16)

    @pl.when(layer == pl.num_programs(0) - 1)
    def _():
        wh_copy.wait()
        normed, scale = pooled_norm(rows, n_img, n_tok)
        normed_b = normed.astype(BF16)
        head_b = wh_ref[...].astype(BF16)
        logits = jnp.dot(normed_b, head_b, preferred_element_type=F32)
        top = jnp.max(logits, axis=-1, keepdims=True)
        exps = jnp.exp(logits - top)
        probs = exps / jnp.sum(exps, axis=-1, keepdims=True)
        classes = lax.broadcasted_iota(jnp.int32, logits.shape, 1)
        image = lax.broadcasted_iota(jnp.int32, logits.shape, 0)
        hit = jnp.zeros(logits.shape, jnp.bool_)
        for img in range(n_img):
            hit = hit | ((image == img) & (classes == lab_ref[img]))
        targets = jnp.where(hit, 1.0, 0.0)
        grad_b = jnp.where(image < n_img, (probs - targets) * (1.0 / batch_total), 0.0).astype(BF16)
        grad_normed = lax.dot_general(grad_b, head_b, LAST, preferred_element_type=F32).astype(BF16)
        grad_pooled = norm_pull(normed, scale, grad_normed.astype(F32))
        per_row = (grad_pooled / n_tok).astype(BF16)
        spread = pool_mask((rows.shape[0], POOL), n_img, n_tok, 0)
        rows[...] = jnp.dot(spread, per_row, preferred_element_type=F32).astype(BF16)
        grad_copy = pltpu.make_async_copy(rows, grad_hbm, sems.at[0])
        grad_copy.start()
        head_grad = lax.dot_general(normed_b, grad_b, ROWS, preferred_element_type=F32).astype(BF16)
        staged[...] = jnp.zeros_like(staged)
        staged[: head_grad.shape[0], : head_grad.shape[1]] = head_grad.astype(F32)
        hg_ref[...] = jnp.zeros_like(hg_ref)
        for dev in range(16):
            for tile in range(staged.shape[1] // 128):
                block = staged[dev * head_rows : dev * head_rows + 16, tile * 128 : (tile + 1) * 128]
                hg_ref[tile // 3, dev // 8, (dev // 4) % 2, (dev // 2) % 2, dev % 2, (tile % 3) * 16 : (tile % 3) * 16 + 16, :] = block.astype(BF16)
        hg_copy = pltpu.make_async_copy(hg_ref, hg_hbm, sems.at[1])
        hg_copy.start()
        grad_copy.wait()
        hg_copy.wait()


def next_kernel(
    n_img, n_tok, head_rows, lr_ref, x_hbm, wu_ref, wd_ref, mom_ref, all_hbm, wh_hbm, nwu_ref, nwd_ref, nwh_hbm, log_hbm,
    x_ref, wh_ref, mh_ref, log_ref, wide, rows, sems,
):
    layer = pl.program_id(0)
    x_copy = pltpu.make_async_copy(x_hbm, x_ref, sems.at[0])
    wh_copy = pltpu.make_async_copy(wh_hbm, wh_ref, sems.at[1])
    mh_copy = pltpu.make_async_copy(all_hbm.at[all_hbm.shape[0] - 1], mh_ref, sems.at[2])

    @pl.when(layer == 0)
    def _():
        x_copy.start()
        wh_copy.start()
        mh_copy.start()
        x_copy.wait()
        pack_rows(x_ref, wide, rows, n_img, n_tok)

    rate = lr_ref[0, 0]
    step = rows.shape[0] // CHUNKS
    for sub in range(wu_ref.shape[0]):
        mixed = mom_ref[sub, 2].T.astype(F32)
        nwu_ref[sub, :128, :] = wu_ref[sub, :128, :] - rate * mom_ref[sub, 0].T.astype(F32)
        nwu_ref[sub, 128:, :] = wu_ref[sub, 128:, :] - rate * mixed[64:, :]
        nwd_ref[sub, :128, :] = wd_ref[sub, :128, :] - rate * mom_ref[sub, 1].T.astype(F32)
        nwd_ref[sub, 128:, :] = wd_ref[sub, 128:, :] - rate * mixed[:64, :]
        up_b = nwu_ref[sub].astype(BF16)
        down_b = nwd_ref[sub].astype(BF16)
        for chunk in range(CHUNKS):
            sl = slice(chunk * step, (chunk + 1) * step)
            x_wide = rows[sl, :].astype(F32)
            centered, scale = norm_parts(x_wide)
            u_rows = (centered * scale).astype(BF16)
            pre = jnp.dot(u_rows, up_b, preferred_element_type=F32).astype(BF16)
            z_rows = gelu(pre.astype(F32)).astype(BF16)
            y_rows = lax.dot_general(z_rows, down_b, LAST, preferred_element_type=F32).astype(BF16)
            rows[sl, :] = (x_wide + y_rows.astype(F32)).astype(BF16)

    @pl.when(layer == pl.num_programs(0) - 1)
    def _():
        wh_copy.wait()
        mh_copy.wait()
        n_cls = wh_ref.shape[1]
        for dev in range(16):
            for tile in range(-(-n_cls // 128)):
                span = slice(tile * 128, min(n_cls, (tile + 1) * 128))
                block = mh_ref[tile // 3, dev * 48 + (tile % 3) * 16 : dev * 48 + (tile % 3) * 16 + 16, :].astype(F32)
                keep = slice(dev * head_rows, (dev + 1) * head_rows)
                wh_ref[keep, span] = wh_ref[keep, span] - rate * block[:head_rows, : span.stop - span.start]
        out_copy = pltpu.make_async_copy(wh_ref, nwh_hbm, sems.at[1])
        out_copy.start()
        normed, _ = pooled_norm(rows, n_img, n_tok)
        logits = jnp.dot(normed.astype(BF16), wh_ref[...].astype(BF16), preferred_element_type=F32)
        log_ref[...] = logits[:n_img]
        log_copy = pltpu.make_async_copy(log_ref, log_hbm, sems.at[0])
        log_copy.start()
        log_copy.wait()
        out_copy.wait()


def backward_kernel(
    n_items, sc_ref, gh_hbm, grad_hbm, xs_ref, pre_ref, wu_ref, wd_ref, mh_hbm, mu_hbm, md_hbm, nmh_hbm, nmu_hbm, nmd_hbm, all_ref,
    g_rows, z_buf, da_buf, u_buf, mh_ref, mu_ref, md_ref, g_buf, pair_buf, sum_buf, rcv0, rcv1, rcv2, ag_buf,
    d2d_send, d2d_recv, rs_send, rs_recv, ag_send, ag_recv, out_sem, in_sem, mom_sem,
):
    t = pl.program_id(0)
    me = lax.axis_index("data")
    core = lax.rem(me, 2)
    place = (lax.div(me, 8), lax.rem(lax.div(me, 4), 2), lax.rem(lax.div(me, 2), 2))
    peers = tuple(me + (1 - 2 * place[axis]) * w for axis, w in ((0, 8), (1, 4), (2, 2)))
    twin = me + 1 - 2 * core
    rcv = (rcv0, rcv1, rcv2)

    @pl.when(t == 0)
    def _():
        barrier = pltpu.get_barrier_semaphore()
        for peer in peers + (twin,):
            pl.semaphore_signal(barrier, inc=1, device_id=(peer,), device_id_type=MESH_ID)
        pl.semaphore_wait(barrier, 4)

    def pair_copy(item):
        return pltpu.make_async_remote_copy(
            src_ref=g_buf.at[lax.rem(item, SLOTS), :, :, :, :, 1 - core],
            dst_ref=pair_buf.at[lax.rem(item, SLOTS)],
            send_sem=d2d_send.at[0, lax.rem(item, 2)],
            recv_sem=d2d_recv.at[0, lax.rem(item, 2)],
            device_id=(twin,),
            device_id_type=MESH_ID,
        )

    def cut(part, stage, value):
        index = [slice(None)] * 3
        for axis in ORDER[part][:stage]:
            index[axis] = place[axis]
        index[ORDER[part][stage]] = value
        return tuple(index)

    def rs_copy(item, stage, part):
        axis = ORDER[part][stage]
        return pltpu.make_async_remote_copy(
            src_ref=sum_buf.at[(lax.rem(item, SLOTS), part) + cut(part, stage, 1 - place[axis])],
            dst_ref=rcv[stage].at[lax.rem(item, SLOTS), part],
            send_sem=rs_send.at[stage, part, lax.rem(item, 2)],
            recv_sem=rs_recv.at[stage, part, lax.rem(item, 2)],
            device_id=(peers[axis],),
            device_id_type=MESH_ID,
        )

    def ag_copy(item, stage, part):
        index = [place[0], place[1], place[2]]
        for axis in ORDER[part][:stage]:
            index[axis] = slice(None)
        view = ag_buf.at[(lax.rem(item, AG_SLOTS), part) + tuple(index) + (core,)]
        return pltpu.make_async_remote_copy(
            src_ref=view,
            dst_ref=view,
            send_sem=ag_send.at[stage, part, lax.rem(item, 2)],
            recv_sem=ag_recv.at[stage, part, lax.rem(item, 2)],
            device_id=(peers[ORDER[part][stage]],),
            device_id_type=MESH_ID,
        )

    def twin_copy(item):
        view = ag_buf.at[lax.rem(item, AG_SLOTS), :, :, :, :, core]
        return pltpu.make_async_remote_copy(
            src_ref=view,
            dst_ref=view,
            send_sem=d2d_send.at[1, lax.rem(item, 2)],
            recv_sem=d2d_recv.at[1, lax.rem(item, 2)],
            device_id=(twin,),
            device_id_type=MESH_ID,
        )

    def out_copy(item):
        return pltpu.make_async_copy(ag_buf.at[lax.rem(item, AG_SLOTS)], all_ref.at[n_items - 1 - item], out_sem.at[lax.rem(item, 2)])

    def at_lag(lag):
        return (t >= lag) & (t < n_items + lag)

    head_copy = pltpu.make_async_copy(gh_hbm, g_buf.at[0], in_sem.at[0])
    grad_copy = pltpu.make_async_copy(grad_hbm, g_rows, in_sem.at[1])
    moms = tuple(
        pltpu.make_async_copy(src, dst, in_sem.at[2 + i]) for i, (src, dst) in enumerate(((mh_hbm, mh_ref), (mu_hbm, mu_ref), (md_hbm, md_ref)))
    )
    moms_out = tuple(
        pltpu.make_async_copy(src, dst, mom_sem.at[i]) for i, (src, dst) in enumerate(((mh_ref, nmh_hbm), (mu_ref, nmu_hbm), (md_ref, nmd_hbm)))
    )

    @pl.when(t == 0)
    def _():
        head_copy.start()
        grad_copy.start()
        for copy in moms:
            copy.start()

    @pl.when(t == 1)
    def _():
        grad_copy.wait()

    @pl.when((t >= 1) & (t < n_items))
    def _():
        up_b = wu_ref[0].astype(BF16)
        down_b = wd_ref[0].astype(BF16)
        step = g_rows.shape[0] // CHUNKS
        grad_old = g_rows[...]
        for chunk in range(CHUNKS):
            sl = slice(chunk * step, (chunk + 1) * step)
            g_old = grad_old[sl, :]
            z_wide, slope = gelu_both(pre_ref[0, sl, :].astype(F32))
            z_buf[sl, :] = z_wide.astype(BF16)
            grad_z = jnp.dot(g_old, down_b, preferred_element_type=F32).astype(BF16)
            grad_a = (grad_z.astype(F32) * slope).astype(BF16)
            da_buf[sl, :] = grad_a
            centered, scale = norm_parts(xs_ref[0, sl, :].astype(F32))
            normed = centered * scale
            u_buf[sl, :] = normed.astype(BF16)
            grad_u = lax.dot_general(grad_a, up_b, LAST, preferred_element_type=F32).astype(BF16)
            grad_x = norm_pull(normed, scale, grad_u.astype(F32))
            g_rows[sl, :] = (g_old.astype(F32) + grad_x).astype(BF16)
        down_t = lax.dot_general(grad_old, z_buf[...], ROWS, preferred_element_type=F32).astype(BF16)
        up_g = lax.dot_general(u_buf[...], da_buf[...], ROWS, preferred_element_type=F32).astype(BF16)
        for part, value in enumerate((up_g[:128, :], down_t[:128, :], jnp.concatenate([down_t[128:, :], up_g[128:, :]], axis=0))):
            turned = value.T
            for dev in range(16):
                block = turned[dev * 48 : (dev + 1) * 48, :]
                g_buf[lax.rem(t, SLOTS), part, dev // 8, (dev // 4) % 2, (dev // 2) % 2, dev % 2] = block

    @pl.when(at_lag(9))
    def _():
        out_copy(t - 9).wait()

    @pl.when(at_lag(8))
    def _():
        item = t - 8
        twin_copy(item).wait()
        out_copy(item).start()

    @pl.when(at_lag(7))
    def _():
        item = t - 7
        for part in range(PARTS):
            ag_copy(item, 2, part).wait()
        twin_copy(item).start()

    for stage in (1, 0):

        @pl.when(at_lag(5 + stage))
        def _(stage=stage):
            item = t - 5 - stage
            for part in range(PARTS):
                ag_copy(item, stage, part).wait()
                ag_copy(item, stage + 1, part).start()

    @pl.when(at_lag(4))
    def _():
        item = t - 4
        for part in range(PARTS):
            rs_copy(item, 2, part).wait()

        def reduced(part):
            return (sum_buf[lax.rem(item, SLOTS), part, place[0], place[1], place[2]] + rcv[2][lax.rem(item, SLOTS), part]).astype(F32)

        def hand_on(part, mom):
            ag_buf[lax.rem(item, AG_SLOTS), part, place[0], place[1], place[2], core] = mom.astype(BF16)
            ag_copy(item, 0, part).start()

        @pl.when(t == 4)
        def _():
            for copy in moms:
                copy.wait()
            for part in range(PARTS):
                mom = sc_ref[0, 0] * mh_ref[part] + reduced(part)
                mh_ref[part] = mom
                hand_on(part, mom)

        @pl.when(t > 4)
        def _():
            layer = n_items - 1 - item
            mixed = reduced(2)
            up_a = sc_ref[0, 0] * mu_ref[layer, :, :128] + reduced(0)
            down_a = sc_ref[0, 0] * md_ref[layer, :, :128] + reduced(1)
            up_z = sc_ref[0, 0] * mu_ref[layer, :, 128:] + mixed[:, 64:]
            down_z = sc_ref[0, 0] * md_ref[layer, :, 128:] + mixed[:, :64]
            mu_ref[layer, :, :128] = up_a
            mu_ref[layer, :, 128:] = up_z
            md_ref[layer, :, :128] = down_a
            md_ref[layer, :, 128:] = down_z
            hand_on(0, up_a)
            hand_on(1, down_a)
            hand_on(2, jnp.concatenate([down_z, up_z], axis=1))

    for stage in (1, 0):

        @pl.when(at_lag(2 + stage))
        def _(stage=stage):
            item = t - 2 - stage
            for part in range(PARTS):
                rs_copy(item, stage, part).wait()
                kept = (lax.rem(item, SLOTS), part) + cut(part, stage, place[ORDER[part][stage]])
                sum_buf[kept] = sum_buf[kept] + rcv[stage][lax.rem(item, SLOTS), part]
                rs_copy(item, stage + 1, part).start()

    @pl.when(at_lag(1))
    def _():
        item = t - 1
        pair_copy(item).wait()
        for part in range(PARTS):
            sum_buf[lax.rem(item, SLOTS), part] = g_buf[lax.rem(item, SLOTS), part, :, :, :, core] + pair_buf[lax.rem(item, SLOTS), part]
            rs_copy(item, 0, part).start()

    @pl.when(t == 0)
    def _():
        head_copy.wait()
        pair_copy(0).start()

    @pl.when((t >= 1) & (t < n_items))
    def _():
        pair_copy(t).start()

    @pl.when(t == n_items + 4)
    def _():
        for copy in moms_out:
            copy.start()

    @pl.when(t == n_items + 6)
    def _():
        for copy in moms_out:
            copy.wait()


def solution(mesh):
    n_dev = mesh.shape["data"]

    def local_step(x_now, x_next, labels, w_up, w_down, w_head, mom_up, mom_down, mom_head, learn_rate, mom_decay):
        n_img, n_tok, width = x_now.shape
        n_layers, _, hidden = w_up.shape
        n_cls = w_head.shape[1]
        n_rows = -(-n_img * n_tok // (16 * CHUNKS)) * 16 * CHUNKS
        n_items = n_layers + 1
        cols = mom_up.shape[2]
        head_rows = mom_head.shape[0]
        n_tile = -(-n_cls // 128)

        down_t = w_down.transpose(0, 2, 1)
        per = 2 if n_layers % 2 == 0 else 1
        any_spec = pl.BlockSpec(memory_space=pl.ANY)
        blocks = (PARTS, 2, 2, 2, 2, cols, 128)
        xs, pre, grad_rows, head_g = pl.pallas_call(
            functools.partial(forward_kernel, n_img, n_tok, n_img * n_dev, head_rows),
            grid=(n_layers // per,),
            in_specs=[
                pl.BlockSpec(memory_space=pltpu.SMEM),
                any_spec,
                pl.BlockSpec((per, width, hidden), lambda i: (i, 0, 0)),
                pl.BlockSpec((per, width, hidden), lambda i: (i, 0, 0)),
                any_spec,
            ],
            out_specs=[
                pl.BlockSpec((per, n_rows, width), lambda i: (i, 0, 0)),
                pl.BlockSpec((per, n_rows, hidden), lambda i: (i, 0, 0)),
                any_spec,
                any_spec,
            ],
            out_shape=[
                jax.ShapeDtypeStruct((n_layers, n_rows, width), BF16),
                jax.ShapeDtypeStruct((n_layers, n_rows, hidden), BF16),
                jax.ShapeDtypeStruct((n_rows, width), BF16),
                jax.ShapeDtypeStruct(blocks, BF16),
            ],
            scratch_shapes=[
                pltpu.VMEM((n_img, width, n_tok), BF16),
                pltpu.VMEM(w_head.shape, F32),
                pltpu.VMEM((n_rows, width), F32),
                pltpu.VMEM((n_rows, width), BF16),
                pltpu.VMEM((n_dev * head_rows + 16, n_tile * 128), F32),
                pltpu.VMEM(blocks, BF16),
                pltpu.SemaphoreType.DMA((2,)),
            ],
            compiler_params=pltpu.CompilerParams(vmem_limit_bytes=VMEM_LIMIT),
            name="step_forward",
        )(labels, x_now.transpose(0, 2, 1), w_up, down_t, w_head)

        head_m = jnp.pad(mom_head, ((0, 16 - head_rows), (0, 9 * 128 - n_cls))).reshape(16, 9, 128)
        head_m = head_m.transpose(1, 0, 2).reshape(PARTS, cols, 128)

        def layer_at(t):
            return jnp.clip(n_items - 1 - t, 0, n_layers - 1)

        block = (SLOTS, PARTS, 2, 2, 2)
        mom_head_new, mom_up_new, new_mom_down, gathered = pl.pallas_call(
            functools.partial(backward_kernel, n_items),
            grid=(n_items + 9,),
            in_specs=[
                pl.BlockSpec(memory_space=pltpu.SMEM),
                any_spec,
                any_spec,
                pl.BlockSpec((1, n_rows, width), lambda t: (layer_at(t), 0, 0)),
                pl.BlockSpec((1, n_rows, hidden), lambda t: (layer_at(t), 0, 0)),
                pl.BlockSpec((1, width, hidden), lambda t: (layer_at(t), 0, 0)),
                pl.BlockSpec((1, width, hidden), lambda t: (layer_at(t), 0, 0)),
                any_spec,
                any_spec,
                any_spec,
            ],
            out_specs=[any_spec] * 4,
            out_shape=[
                jax.ShapeDtypeStruct((PARTS, cols, 128), F32),
                jax.ShapeDtypeStruct((n_layers, cols, width), F32),
                jax.ShapeDtypeStruct((n_layers, cols, width), F32),
                jax.ShapeDtypeStruct((n_items, PARTS, 2, 2, 2, 2, cols, 128), BF16),
            ],
            scratch_shapes=[
                pltpu.VMEM((n_rows, width), BF16),
                pltpu.VMEM((n_rows, hidden), BF16),
                pltpu.VMEM((n_rows, hidden), BF16),
                pltpu.VMEM((n_rows, width), BF16),
                pltpu.VMEM((PARTS, cols, 128), F32),
                pltpu.VMEM((n_layers, cols, width), F32),
                pltpu.VMEM((n_layers, cols, width), F32),
                pltpu.VMEM(block + (2, cols, 128), BF16),
                pltpu.VMEM(block + (cols, 128), BF16),
                pltpu.VMEM(block + (cols, 128), BF16),
                pltpu.VMEM((SLOTS, PARTS, 2, 2, cols, 128), BF16),
                pltpu.VMEM((SLOTS, PARTS, 2, cols, 128), BF16),
                pltpu.VMEM((SLOTS, PARTS, cols, 128), BF16),
                pltpu.VMEM((AG_SLOTS, PARTS, 2, 2, 2, 2, cols, 128), BF16),
                pltpu.SemaphoreType.DMA((2, 2)),
                pltpu.SemaphoreType.DMA((2, 2)),
                pltpu.SemaphoreType.DMA((3, PARTS, 2)),
                pltpu.SemaphoreType.DMA((3, PARTS, 2)),
                pltpu.SemaphoreType.DMA((3, PARTS, 2)),
                pltpu.SemaphoreType.DMA((3, PARTS, 2)),
                pltpu.SemaphoreType.DMA((2,)),
                pltpu.SemaphoreType.DMA((5,)),
                pltpu.SemaphoreType.DMA((3,)),
            ],
            compiler_params=pltpu.CompilerParams(vmem_limit_bytes=VMEM_LIMIT, collective_id=0, has_side_effects=True),
            name="step_backward",
        )(mom_decay.reshape(1, 1), head_g, grad_rows, xs, pre, w_up, down_t, head_m, mom_up.transpose(0, 2, 1), mom_down)

        gathered = gathered.reshape(n_items, PARTS, n_dev * cols, 128)
        new_w_up, new_down_t, new_w_head, logits = pl.pallas_call(
            functools.partial(next_kernel, n_img, n_tok, head_rows),
            grid=(n_layers // per,),
            in_specs=[
                pl.BlockSpec(memory_space=pltpu.SMEM),
                any_spec,
                pl.BlockSpec((per, width, hidden), lambda i: (i, 0, 0)),
                pl.BlockSpec((per, width, hidden), lambda i: (i, 0, 0)),
                pl.BlockSpec((per, PARTS, n_dev * cols, 128), lambda i: (i, 0, 0, 0)),
                any_spec,
                any_spec,
            ],
            out_specs=[
                pl.BlockSpec((per, width, hidden), lambda i: (i, 0, 0)),
                pl.BlockSpec((per, width, hidden), lambda i: (i, 0, 0)),
                any_spec,
                any_spec,
            ],
            out_shape=[
                jax.ShapeDtypeStruct(w_up.shape, F32),
                jax.ShapeDtypeStruct(w_up.shape, F32),
                jax.ShapeDtypeStruct(w_head.shape, F32),
                jax.ShapeDtypeStruct((n_img, n_cls), F32),
            ],
            scratch_shapes=[
                pltpu.VMEM((n_img, width, n_tok), BF16),
                pltpu.VMEM(w_head.shape, F32),
                pltpu.VMEM((PARTS, n_dev * cols, 128), BF16),
                pltpu.VMEM((n_img, n_cls), F32),
                pltpu.VMEM((n_rows, width), F32),
                pltpu.VMEM((n_rows, width), BF16),
                pltpu.SemaphoreType.DMA((3,)),
            ],
            compiler_params=pltpu.CompilerParams(vmem_limit_bytes=VMEM_LIMIT),
            name="step_next",
        )(learn_rate.reshape(1, 1), x_next.transpose(0, 2, 1), w_up, down_t, gathered, gathered, w_head)

        new_mom_head = mom_head_new.reshape(9, 16, 128).transpose(1, 0, 2).reshape(16, 9 * 128)[:head_rows, :n_cls]
        return (logits, new_w_up, new_down_t.transpose(0, 2, 1), new_w_head, mom_up_new.transpose(0, 2, 1), new_mom_down, new_mom_head)

    spec_up = P(None, None, "data")
    spec_down = P(None, "data", None)
    spec_head = P("data", None)
    return jax.shard_map(
        local_step,
        mesh=mesh,
        in_specs=(P("data"), P("data"), P("data"), P(), P(), P(), spec_up, spec_down, spec_head, P(), P()),
        out_specs=(P("data"), P(), P(), P(), spec_up, spec_down, spec_head),
        check_vma=False,
    )
```

```python
import functools

import jax
import jax.numpy as jnp
from jax import lax
from jax.experimental import pallas as pl
from jax.experimental.pallas import tpu as pltpu
from jax.sharding import PartitionSpec as P

LN_EPS = 1e-6
GELU_C = 0.7978845608028654
GELU_A = 0.044715
F32 = jnp.float32
BF16 = jnp.bfloat16
LAST = (((1,), (1,)), ((), ()))
ROWS = (((0,), (0,)), ((), ()))
MESH_ID = pl.DeviceIdType.MESH
VMEM_LIMIT = 62 * 1024 * 1024
CHUNKS = 5
G_SLOTS = 2
RS_SLOTS = 8
IN_SLOTS = 4
AG_SLOTS = 12
UPDATE = 7
TWIN = 13
PARTS = 3
POOL = 16
ORDER = ((0, 1, 2), (1, 2, 0), (2, 0, 1))


def norm_parts(values):
    mean_v = jnp.mean(values, axis=-1, keepdims=True)
    centered = values - mean_v
    var_v = jnp.mean(centered * centered, axis=-1, keepdims=True)
    return centered, lax.rsqrt(var_v + LN_EPS)


def norm_pull(normed, scale, grad):
    mean_g = jnp.mean(grad, axis=-1, keepdims=True)
    mean_gn = jnp.mean(grad * normed, axis=-1, keepdims=True)
    return scale * (grad - mean_g - normed * mean_gn)


def gelu(values):
    inner = values * (GELU_C + (GELU_C * GELU_A) * (values * values))
    return values * (0.5 + 0.5 * jnp.tanh(inner))


def gelu_both(values):
    square = values * values
    share = 0.5 + 0.5 * jnp.tanh(values * (GELU_C + (GELU_C * GELU_A) * square))
    out = values * share
    slope = share + (out * (1.0 - share)) * (2.0 * GELU_C + (6.0 * GELU_C * GELU_A) * square)
    return out, slope


def pack_rows(x_ref, wide, rows, n_img, n_tok):
    wide[...] = jnp.zeros_like(wide)
    for img in range(n_img):
        wide[img * n_tok : (img + 1) * n_tok, :] = x_ref[img].astype(F32).T
    rows[...] = wide[...].astype(BF16)


def pool_mask(shape, n_img, n_tok, row_axis):
    row = lax.broadcasted_iota(jnp.int32, shape, row_axis)
    img = lax.broadcasted_iota(jnp.int32, shape, 1 - row_axis)
    inside = (row >= img * n_tok) & (row < (img + 1) * n_tok) & (img < n_img)
    return jnp.where(inside, 1.0, 0.0).astype(BF16)


def pooled_norm(rows, n_img, n_tok):
    n_rows = rows.shape[0]
    mask = pool_mask((POOL, n_rows), n_img, n_tok, 1)
    pooled = jnp.dot(mask, rows[...], preferred_element_type=F32) * (1.0 / n_tok)
    centered, scale = norm_parts(pooled)
    return centered * scale, scale


def forward_kernel(
    n_img, n_tok, batch_total, head_rows, lab_ref, x_hbm, wu_ref, wd_ref, wh_hbm, xs_ref, pre_ref, grad_hbm, hg_hbm,
    x_ref, wh_ref, wide, rows, staged, hg_ref, sems,
):
    layer = pl.program_id(0)
    x_copy = pltpu.make_async_copy(x_hbm, x_ref, sems.at[0])
    wh_copy = pltpu.make_async_copy(wh_hbm, wh_ref, sems.at[1])

    @pl.when(layer == 0)
    def _():
        x_copy.start()
        wh_copy.start()
        x_copy.wait()
        pack_rows(x_ref, wide, rows, n_img, n_tok)

    step = rows.shape[0] // CHUNKS
    for sub in range(wu_ref.shape[0]):
        up_b = wu_ref[sub].astype(BF16)
        down_b = wd_ref[sub].astype(BF16)
        for chunk in range(CHUNKS):
            sl = slice(chunk * step, (chunk + 1) * step)
            x_rows = rows[sl, :]
            xs_ref[sub, sl, :] = x_rows
            x_wide = x_rows.astype(F32)
            centered, scale = norm_parts(x_wide)
            u_rows = (centered * scale).astype(BF16)
            pre = jnp.dot(u_rows, up_b, preferred_element_type=F32).astype(BF16)
            pre_ref[sub, sl, :] = pre
            z_rows = gelu(pre.astype(F32)).astype(BF16)
            y_rows = lax.dot_general(z_rows, down_b, LAST, preferred_element_type=F32).astype(BF16)
            rows[sl, :] = (x_wide + y_rows.astype(F32)).astype(BF16)

    @pl.when(layer == pl.num_programs(0) - 1)
    def _():
        wh_copy.wait()
        normed, scale = pooled_norm(rows, n_img, n_tok)
        normed_b = normed.astype(BF16)
        head_b = wh_ref[...].astype(BF16)
        logits = jnp.dot(normed_b, head_b, preferred_element_type=F32)
        top = jnp.max(logits, axis=-1, keepdims=True)
        exps = jnp.exp(logits - top)
        probs = exps / jnp.sum(exps, axis=-1, keepdims=True)
        classes = lax.broadcasted_iota(jnp.int32, logits.shape, 1)
        image = lax.broadcasted_iota(jnp.int32, logits.shape, 0)
        hit = jnp.zeros(logits.shape, jnp.bool_)
        for img in range(n_img):
            hit = hit | ((image == img) & (classes == lab_ref[img]))
        targets = jnp.where(hit, 1.0, 0.0)
        grad_b = jnp.where(image < n_img, (probs - targets) * (1.0 / batch_total), 0.0).astype(BF16)
        grad_normed = lax.dot_general(grad_b, head_b, LAST, preferred_element_type=F32).astype(BF16)
        grad_pooled = norm_pull(normed, scale, grad_normed.astype(F32))
        per_row = (grad_pooled / n_tok).astype(BF16)
        spread = pool_mask((rows.shape[0], POOL), n_img, n_tok, 0)
        rows[...] = jnp.dot(spread, per_row, preferred_element_type=F32).astype(BF16)
        grad_copy = pltpu.make_async_copy(rows, grad_hbm, sems.at[0])
        grad_copy.start()
        head_grad = lax.dot_general(normed_b, grad_b, ROWS, preferred_element_type=F32).astype(BF16)
        staged[...] = jnp.zeros_like(staged)
        staged[: head_grad.shape[0], : head_grad.shape[1]] = head_grad.astype(F32)
        hg_ref[...] = jnp.zeros_like(hg_ref)
        for dev in range(16):
            for tile in range(staged.shape[1] // 128):
                block = staged[dev * head_rows : dev * head_rows + 16, tile * 128 : (tile + 1) * 128]
                hg_ref[tile // 3, dev // 8, (dev // 4) % 2, (dev // 2) % 2, dev % 2, (tile % 3) * 16 : (tile % 3) * 16 + 16, :] = block.astype(BF16)
        hg_copy = pltpu.make_async_copy(hg_ref, hg_hbm, sems.at[1])
        hg_copy.start()
        grad_copy.wait()
        hg_copy.wait()


def next_kernel(
    n_img, n_tok, head_rows, lr_ref, x_hbm, wu_ref, wd_ref, mom_ref, all_hbm, wh_hbm, nwu_ref, nwd_ref, nwh_hbm, log_hbm,
    x_ref, wh_ref, mh_ref, log_ref, wide, rows, sems,
):
    layer = pl.program_id(0)
    x_copy = pltpu.make_async_copy(x_hbm, x_ref, sems.at[0])
    wh_copy = pltpu.make_async_copy(wh_hbm, wh_ref, sems.at[1])
    mh_copy = pltpu.make_async_copy(all_hbm.at[all_hbm.shape[0] - 1], mh_ref, sems.at[2])

    @pl.when(layer == 0)
    def _():
        x_copy.start()
        wh_copy.start()
        mh_copy.start()
        x_copy.wait()
        pack_rows(x_ref, wide, rows, n_img, n_tok)

    rate = lr_ref[0, 0]
    step = rows.shape[0] // CHUNKS
    for sub in range(wu_ref.shape[0]):
        mixed = mom_ref[sub, 2].T.astype(F32)
        nwu_ref[sub, :128, :] = wu_ref[sub, :128, :] - rate * mom_ref[sub, 0].T.astype(F32)
        nwu_ref[sub, 128:, :] = wu_ref[sub, 128:, :] - rate * mixed[64:, :]
        nwd_ref[sub, :128, :] = wd_ref[sub, :128, :] - rate * mom_ref[sub, 1].T.astype(F32)
        nwd_ref[sub, 128:, :] = wd_ref[sub, 128:, :] - rate * mixed[:64, :]
        up_b = nwu_ref[sub].astype(BF16)
        down_b = nwd_ref[sub].astype(BF16)
        for chunk in range(CHUNKS):
            sl = slice(chunk * step, (chunk + 1) * step)
            x_wide = rows[sl, :].astype(F32)
            centered, scale = norm_parts(x_wide)
            u_rows = (centered * scale).astype(BF16)
            pre = jnp.dot(u_rows, up_b, preferred_element_type=F32).astype(BF16)
            z_rows = gelu(pre.astype(F32)).astype(BF16)
            y_rows = lax.dot_general(z_rows, down_b, LAST, preferred_element_type=F32).astype(BF16)
            rows[sl, :] = (x_wide + y_rows.astype(F32)).astype(BF16)

    @pl.when(layer == pl.num_programs(0) - 1)
    def _():
        wh_copy.wait()
        mh_copy.wait()
        n_cls = wh_ref.shape[1]
        for dev in range(16):
            for tile in range(-(-n_cls // 128)):
                span = slice(tile * 128, min(n_cls, (tile + 1) * 128))
                block = mh_ref[tile // 3, dev * 48 + (tile % 3) * 16 : dev * 48 + (tile % 3) * 16 + 16, :].astype(F32)
                keep = slice(dev * head_rows, (dev + 1) * head_rows)
                wh_ref[keep, span] = wh_ref[keep, span] - rate * block[:head_rows, : span.stop - span.start]
        out_copy = pltpu.make_async_copy(wh_ref, nwh_hbm, sems.at[1])
        out_copy.start()
        normed, _ = pooled_norm(rows, n_img, n_tok)
        logits = jnp.dot(normed.astype(BF16), wh_ref[...].astype(BF16), preferred_element_type=F32)
        log_ref[...] = logits[:n_img]
        log_copy = pltpu.make_async_copy(log_ref, log_hbm, sems.at[0])
        log_copy.start()
        log_copy.wait()
        out_copy.wait()


def backward_kernel(
    n_items, sc_ref, gh_hbm, grad_hbm, xs_ref, pre_ref, wu_ref, wd_ref, mh_hbm, mu_hbm, md_hbm, nmh_hbm, nmu_hbm, nmd_hbm, all_ref,
    g_rows, z_buf, da_buf, u_buf, mh_ref, mu_ref, md_ref, g_buf, pair_buf, sum_buf, rcv0, rcv1, rcv2, ag_buf,
    d2d_send, d2d_recv, rs_send, rs_recv, ag_send, ag_recv, out_sem, in_sem, mom_sem,
):
    t = pl.program_id(0)
    me = lax.axis_index("data")
    core = lax.rem(me, 2)
    place = (lax.div(me, 8), lax.rem(lax.div(me, 4), 2), lax.rem(lax.div(me, 2), 2))
    peers = tuple(me + (1 - 2 * place[axis]) * w for axis, w in ((0, 8), (1, 4), (2, 2)))
    twin = me + 1 - 2 * core
    rcv = (rcv0, rcv1, rcv2)

    @pl.when(t == 0)
    def _():
        barrier = pltpu.get_barrier_semaphore()
        for peer in peers + (twin,):
            pl.semaphore_signal(barrier, inc=1, device_id=(peer,), device_id_type=MESH_ID)
        pl.semaphore_wait(barrier, 4)

    def pair_copy(item):
        slot = lax.rem(item, G_SLOTS)
        return pltpu.make_async_remote_copy(
            src_ref=g_buf.at[slot, :, :, :, :, 1 - core],
            dst_ref=pair_buf.at[slot],
            send_sem=d2d_send.at[0, slot],
            recv_sem=d2d_recv.at[0, slot],
            device_id=(twin,),
            device_id_type=MESH_ID,
        )

    def cut(part, stage, value):
        index = [slice(None)] * 3
        for axis in ORDER[part][:stage]:
            index[axis] = place[axis]
        index[ORDER[part][stage]] = value
        return tuple(index)

    def rs_copy(item, stage, part):
        axis = ORDER[part][stage]
        slot = lax.rem(item, IN_SLOTS)
        return pltpu.make_async_remote_copy(
            src_ref=sum_buf.at[(lax.rem(item, RS_SLOTS), part) + cut(part, stage, 1 - place[axis])],
            dst_ref=rcv[stage].at[slot, part],
            send_sem=rs_send.at[stage, part, slot],
            recv_sem=rs_recv.at[stage, part, slot],
            device_id=(peers[axis],),
            device_id_type=MESH_ID,
        )

    def ag_copy(item, stage, part):
        index = [place[0], place[1], place[2]]
        for axis in ORDER[part][:stage]:
            index[axis] = slice(None)
        view = ag_buf.at[(lax.rem(item, AG_SLOTS), part) + tuple(index) + (core,)]
        return pltpu.make_async_remote_copy(
            src_ref=view,
            dst_ref=view,
            send_sem=ag_send.at[stage, part, lax.rem(item, IN_SLOTS)],
            recv_sem=ag_recv.at[stage, part, lax.rem(item, IN_SLOTS)],
            device_id=(peers[ORDER[part][stage]],),
            device_id_type=MESH_ID,
        )

    def twin_copy(item):
        view = ag_buf.at[lax.rem(item, AG_SLOTS), :, :, :, :, core]
        return pltpu.make_async_remote_copy(
            src_ref=view,
            dst_ref=view,
            send_sem=d2d_send.at[1, lax.rem(item, 2)],
            recv_sem=d2d_recv.at[1, lax.rem(item, 2)],
            device_id=(twin,),
            device_id_type=MESH_ID,
        )

    def out_copy(item):
        return pltpu.make_async_copy(ag_buf.at[lax.rem(item, AG_SLOTS)], all_ref.at[n_items - 1 - item], out_sem.at[lax.rem(item, 2)])

    def at_lag(lag):
        return (t >= lag) & (t < n_items + lag)

    head_copy = pltpu.make_async_copy(gh_hbm, g_buf.at[0], in_sem.at[0])
    grad_copy = pltpu.make_async_copy(grad_hbm, g_rows, in_sem.at[1])
    moms = tuple(
        pltpu.make_async_copy(src, dst, in_sem.at[2 + i]) for i, (src, dst) in enumerate(((mh_hbm, mh_ref), (mu_hbm, mu_ref), (md_hbm, md_ref)))
    )
    moms_out = tuple(
        pltpu.make_async_copy(src, dst, mom_sem.at[i]) for i, (src, dst) in enumerate(((mh_ref, nmh_hbm), (mu_ref, nmu_hbm), (md_ref, nmd_hbm)))
    )

    @pl.when(t == 0)
    def _():
        head_copy.start()
        grad_copy.start()
        for copy in moms:
            copy.start()

    @pl.when(t == 1)
    def _():
        grad_copy.wait()

    @pl.when((t >= 1) & (t < n_items))
    def _():
        up_b = wu_ref[0].astype(BF16)
        down_b = wd_ref[0].astype(BF16)
        step = g_rows.shape[0] // CHUNKS
        grad_old = g_rows[...]
        for chunk in range(CHUNKS):
            sl = slice(chunk * step, (chunk + 1) * step)
            g_old = grad_old[sl, :]
            z_wide, slope = gelu_both(pre_ref[0, sl, :].astype(F32))
            z_buf[sl, :] = z_wide.astype(BF16)
            grad_z = jnp.dot(g_old, down_b, preferred_element_type=F32).astype(BF16)
            grad_a = (grad_z.astype(F32) * slope).astype(BF16)
            da_buf[sl, :] = grad_a
            centered, scale = norm_parts(xs_ref[0, sl, :].astype(F32))
            normed = centered * scale
            u_buf[sl, :] = normed.astype(BF16)
            grad_u = lax.dot_general(grad_a, up_b, LAST, preferred_element_type=F32).astype(BF16)
            grad_x = norm_pull(normed, scale, grad_u.astype(F32))
            g_rows[sl, :] = (g_old.astype(F32) + grad_x).astype(BF16)
        down_t = lax.dot_general(grad_old, z_buf[...], ROWS, preferred_element_type=F32).astype(BF16)
        up_g = lax.dot_general(u_buf[...], da_buf[...], ROWS, preferred_element_type=F32).astype(BF16)
        for part, value in enumerate((up_g[:128, :], down_t[:128, :], jnp.concatenate([down_t[128:, :], up_g[128:, :]], axis=0))):
            turned = value.T
            for dev in range(16):
                block = turned[dev * 48 : (dev + 1) * 48, :]
                g_buf[lax.rem(t, G_SLOTS), part, dev // 8, (dev // 4) % 2, (dev // 2) % 2, dev % 2] = block

    @pl.when(at_lag(UPDATE))
    def _():
        item = t - UPDATE
        for part in range(PARTS):
            rs_copy(item, 2, part).wait()

        def reduced(part):
            return (sum_buf[lax.rem(item, RS_SLOTS), part, place[0], place[1], place[2]] + rcv[2][lax.rem(item, IN_SLOTS), part]).astype(F32)

        def hand_on(part, mom):
            ag_buf[lax.rem(item, AG_SLOTS), part, place[0], place[1], place[2], core] = mom.astype(BF16)

        @pl.when(t == UPDATE)
        def _():
            for copy in moms:
                copy.wait()
            for part in range(PARTS):
                mom = sc_ref[0, 0] * mh_ref[part] + reduced(part)
                mh_ref[part] = mom
                hand_on(part, mom)

        @pl.when(t > UPDATE)
        def _():
            layer = n_items - 1 - item
            mixed = reduced(2)
            up_a = sc_ref[0, 0] * mu_ref[layer, :, :128] + reduced(0)
            down_a = sc_ref[0, 0] * md_ref[layer, :, :128] + reduced(1)
            up_z = sc_ref[0, 0] * mu_ref[layer, :, 128:] + mixed[:, 64:]
            down_z = sc_ref[0, 0] * md_ref[layer, :, 128:] + mixed[:, :64]
            mu_ref[layer, :, :128] = up_a
            mu_ref[layer, :, 128:] = up_z
            md_ref[layer, :, :128] = down_a
            md_ref[layer, :, 128:] = down_z
            hand_on(0, up_a)
            hand_on(1, down_a)
            hand_on(2, jnp.concatenate([down_z, up_z], axis=1))

    for stage in (1, 0):

        @pl.when(at_lag(3 + 2 * stage))
        def _(stage=stage):
            item = t - 3 - 2 * stage
            for part in range(PARTS):
                rs_copy(item, stage, part).wait()
                kept = (lax.rem(item, RS_SLOTS), part) + cut(part, stage, place[ORDER[part][stage]])
                sum_buf[kept] = sum_buf[kept] + rcv[stage][lax.rem(item, IN_SLOTS), part]
                rs_copy(item, stage + 1, part).start()

    @pl.when(at_lag(1))
    def _():
        item = t - 1
        pair_copy(item).wait()
        for part in range(PARTS):
            kept = g_buf[lax.rem(item, G_SLOTS), part, :, :, :, core]
            sum_buf[lax.rem(item, RS_SLOTS), part] = kept + pair_buf[lax.rem(item, G_SLOTS), part]
            rs_copy(item, 0, part).start()

    @pl.when(t == 0)
    def _():
        head_copy.wait()
        pair_copy(0).start()

    @pl.when((t >= 1) & (t < n_items))
    def _():
        pair_copy(t).start()

    @pl.when(at_lag(TWIN + 2))
    def _():
        out_copy(t - TWIN - 2).wait()

    @pl.when(at_lag(TWIN + 1))
    def _():
        item = t - TWIN - 1
        twin_copy(item).wait()
        out_copy(item).start()

    for stage in (3, 2, 1):

        @pl.when(at_lag(UPDATE + 2 * stage))
        def _(stage=stage):
            item = t - UPDATE - 2 * stage
            for part in range(PARTS):
                ag_copy(item, stage - 1, part).wait()
                if stage < 3:
                    ag_copy(item, stage, part).start()
            if stage == 3:
                twin_copy(item).start()

    @pl.when(at_lag(UPDATE))
    def _():
        for part in range(PARTS):
            ag_copy(t - UPDATE, 0, part).start()

    @pl.when(t == n_items + UPDATE)
    def _():
        for copy in moms_out:
            copy.start()

    @pl.when(t == n_items + UPDATE + 3)
    def _():
        for copy in moms_out:
            copy.wait()


def solution(mesh):
    n_dev = mesh.shape["data"]

    def local_step(x_now, x_next, labels, w_up, w_down, w_head, mom_up, mom_down, mom_head, learn_rate, mom_decay):
        n_img, n_tok, width = x_now.shape
        n_layers, _, hidden = w_up.shape
        n_cls = w_head.shape[1]
        n_rows = -(-n_img * n_tok // (16 * CHUNKS)) * 16 * CHUNKS
        n_items = n_layers + 1
        cols = mom_up.shape[2]
        head_rows = mom_head.shape[0]
        n_tile = -(-n_cls // 128)

        down_t = w_down.transpose(0, 2, 1)
        per = 2 if n_layers % 2 == 0 else 1
        any_spec = pl.BlockSpec(memory_space=pl.ANY)
        blocks = (PARTS, 2, 2, 2, 2, cols, 128)
        xs, pre, grad_rows, head_g = pl.pallas_call(
            functools.partial(forward_kernel, n_img, n_tok, n_img * n_dev, head_rows),
            grid=(n_layers // per,),
            in_specs=[
                pl.BlockSpec(memory_space=pltpu.SMEM),
                any_spec,
                pl.BlockSpec((per, width, hidden), lambda i: (i, 0, 0)),
                pl.BlockSpec((per, width, hidden), lambda i: (i, 0, 0)),
                any_spec,
            ],
            out_specs=[
                pl.BlockSpec((per, n_rows, width), lambda i: (i, 0, 0)),
                pl.BlockSpec((per, n_rows, hidden), lambda i: (i, 0, 0)),
                any_spec,
                any_spec,
            ],
            out_shape=[
                jax.ShapeDtypeStruct((n_layers, n_rows, width), BF16),
                jax.ShapeDtypeStruct((n_layers, n_rows, hidden), BF16),
                jax.ShapeDtypeStruct((n_rows, width), BF16),
                jax.ShapeDtypeStruct(blocks, BF16),
            ],
            scratch_shapes=[
                pltpu.VMEM((n_img, width, n_tok), BF16),
                pltpu.VMEM(w_head.shape, F32),
                pltpu.VMEM((n_rows, width), F32),
                pltpu.VMEM((n_rows, width), BF16),
                pltpu.VMEM((n_dev * head_rows + 16, n_tile * 128), F32),
                pltpu.VMEM(blocks, BF16),
                pltpu.SemaphoreType.DMA((2,)),
            ],
            compiler_params=pltpu.CompilerParams(vmem_limit_bytes=VMEM_LIMIT),
            name="step_forward",
        )(labels, x_now.transpose(0, 2, 1), w_up, down_t, w_head)

        head_m = jnp.pad(mom_head, ((0, 16 - head_rows), (0, 9 * 128 - n_cls))).reshape(16, 9, 128)
        head_m = head_m.transpose(1, 0, 2).reshape(PARTS, cols, 128)

        def layer_at(t):
            return jnp.clip(n_items - 1 - t, 0, n_layers - 1)

        block = (PARTS, 2, 2, 2)
        mom_head_new, mom_up_new, new_mom_down, gathered = pl.pallas_call(
            functools.partial(backward_kernel, n_items),
            grid=(n_items + TWIN + 2,),
            in_specs=[
                pl.BlockSpec(memory_space=pltpu.SMEM),
                any_spec,
                any_spec,
                pl.BlockSpec((1, n_rows, width), lambda t: (layer_at(t), 0, 0)),
                pl.BlockSpec((1, n_rows, hidden), lambda t: (layer_at(t), 0, 0)),
                pl.BlockSpec((1, width, hidden), lambda t: (layer_at(t), 0, 0)),
                pl.BlockSpec((1, width, hidden), lambda t: (layer_at(t), 0, 0)),
                any_spec,
                any_spec,
                any_spec,
            ],
            out_specs=[any_spec] * 4,
            out_shape=[
                jax.ShapeDtypeStruct((PARTS, cols, 128), F32),
                jax.ShapeDtypeStruct((n_layers, cols, width), F32),
                jax.ShapeDtypeStruct((n_layers, cols, width), F32),
                jax.ShapeDtypeStruct((n_items, PARTS, 2, 2, 2, 2, cols, 128), BF16),
            ],
            scratch_shapes=[
                pltpu.VMEM((n_rows, width), BF16),
                pltpu.VMEM((n_rows, hidden), BF16),
                pltpu.VMEM((n_rows, hidden), BF16),
                pltpu.VMEM((n_rows, width), BF16),
                pltpu.VMEM((PARTS, cols, 128), F32),
                pltpu.VMEM((n_layers, cols, width), F32),
                pltpu.VMEM((n_layers, cols, width), F32),
                pltpu.VMEM((G_SLOTS,) + block + (2, cols, 128), BF16),
                pltpu.VMEM((G_SLOTS,) + block + (cols, 128), BF16),
                pltpu.VMEM((RS_SLOTS,) + block + (cols, 128), BF16),
                pltpu.VMEM((IN_SLOTS, PARTS, 2, 2, cols, 128), BF16),
                pltpu.VMEM((IN_SLOTS, PARTS, 2, cols, 128), BF16),
                pltpu.VMEM((IN_SLOTS, PARTS, cols, 128), BF16),
                pltpu.VMEM((AG_SLOTS,) + block + (2, cols, 128), BF16),
                pltpu.SemaphoreType.DMA((2, 2)),
                pltpu.SemaphoreType.DMA((2, 2)),
                pltpu.SemaphoreType.DMA((3, PARTS, IN_SLOTS)),
                pltpu.SemaphoreType.DMA((3, PARTS, IN_SLOTS)),
                pltpu.SemaphoreType.DMA((3, PARTS, IN_SLOTS)),
                pltpu.SemaphoreType.DMA((3, PARTS, IN_SLOTS)),
                pltpu.SemaphoreType.DMA((2,)),
                pltpu.SemaphoreType.DMA((5,)),
                pltpu.SemaphoreType.DMA((3,)),
            ],
            compiler_params=pltpu.CompilerParams(vmem_limit_bytes=VMEM_LIMIT, collective_id=0, has_side_effects=True),
            name="step_backward",
        )(mom_decay.reshape(1, 1), head_g, grad_rows, xs, pre, w_up, down_t, head_m, mom_up.transpose(0, 2, 1), mom_down)

        gathered = gathered.reshape(n_items, PARTS, n_dev * cols, 128)
        new_w_up, new_down_t, new_w_head, logits = pl.pallas_call(
            functools.partial(next_kernel, n_img, n_tok, head_rows),
            grid=(n_layers // per,),
            in_specs=[
                pl.BlockSpec(memory_space=pltpu.SMEM),
                any_spec,
                pl.BlockSpec((per, width, hidden), lambda i: (i, 0, 0)),
                pl.BlockSpec((per, width, hidden), lambda i: (i, 0, 0)),
                pl.BlockSpec((per, PARTS, n_dev * cols, 128), lambda i: (i, 0, 0, 0)),
                any_spec,
                any_spec,
            ],
            out_specs=[
                pl.BlockSpec((per, width, hidden), lambda i: (i, 0, 0)),
                pl.BlockSpec((per, width, hidden), lambda i: (i, 0, 0)),
                any_spec,
                any_spec,
            ],
            out_shape=[
                jax.ShapeDtypeStruct(w_up.shape, F32),
                jax.ShapeDtypeStruct(w_up.shape, F32),
                jax.ShapeDtypeStruct(w_head.shape, F32),
                jax.ShapeDtypeStruct((n_img, n_cls), F32),
            ],
            scratch_shapes=[
                pltpu.VMEM((n_img, width, n_tok), BF16),
                pltpu.VMEM(w_head.shape, F32),
                pltpu.VMEM((PARTS, n_dev * cols, 128), BF16),
                pltpu.VMEM((n_img, n_cls), F32),
                pltpu.VMEM((n_rows, width), F32),
                pltpu.VMEM((n_rows, width), BF16),
                pltpu.SemaphoreType.DMA((3,)),
            ],
            compiler_params=pltpu.CompilerParams(vmem_limit_bytes=VMEM_LIMIT),
            name="step_next",
        )(learn_rate.reshape(1, 1), x_next.transpose(0, 2, 1), w_up, down_t, gathered, gathered, w_head)

        new_mom_head = mom_head_new.reshape(9, 16, 128).transpose(1, 0, 2).reshape(16, 9 * 128)[:head_rows, :n_cls]
        return (logits, new_w_up, new_down_t.transpose(0, 2, 1), new_w_head, mom_up_new.transpose(0, 2, 1), new_mom_down, new_mom_head)

    spec_up = P(None, None, "data")
    spec_down = P(None, "data", None)
    spec_head = P("data", None)
    return jax.shard_map(
        local_step,
        mesh=mesh,
        in_specs=(P("data"), P("data"), P("data"), P(), P(), P(), spec_up, spec_down, spec_head, P(), P()),
        out_specs=(P("data"), P(), P(), P(), spec_up, spec_down, spec_head),
        check_vma=False,
    )
```

```python
import functools

import jax
import jax.numpy as jnp
from jax import lax
from jax.experimental import pallas as pl
from jax.experimental.pallas import tpu as pltpu
from jax.sharding import PartitionSpec as P

LN_EPS = 1e-6
GELU_C = 0.7978845608028654
GELU_A = 0.044715
F32 = jnp.float32
BF16 = jnp.bfloat16
LAST = (((1,), (1,)), ((), ()))
ROWS = (((0,), (0,)), ((), ()))
MESH_ID = pl.DeviceIdType.MESH
VMEM_LIMIT = 62 * 1024 * 1024
CHUNKS = 5
G_SLOTS = 2
RS_SLOTS = 8
IN_SLOTS = 4
AG_SLOTS = 12
UPDATE = 7
TWIN = 13
PARTS = 3
POOL = 16
ORDER = ((0, 1, 2), (1, 2, 0), (2, 0, 1))


def norm_parts(values):
    mean_v = jnp.mean(values, axis=-1, keepdims=True)
    centered = values - mean_v
    var_v = jnp.mean(centered * centered, axis=-1, keepdims=True)
    return centered, lax.rsqrt(var_v + LN_EPS)


def norm_pull(normed, scale, grad):
    mean_g = jnp.mean(grad, axis=-1, keepdims=True)
    mean_gn = jnp.mean(grad * normed, axis=-1, keepdims=True)
    return scale * (grad - mean_g - normed * mean_gn)


def gelu(values):
    inner = values * (GELU_C + (GELU_C * GELU_A) * (values * values))
    return values * (0.5 + 0.5 * jnp.tanh(inner))


def gelu_half(half):
    tanh_v = jnp.tanh(half * (2.0 * GELU_C + (8.0 * GELU_C * GELU_A) * (half * half)))
    return half + half * tanh_v


def gelu_both(values):
    square = values * values
    share = 0.5 + 0.5 * jnp.tanh(values * (GELU_C + (GELU_C * GELU_A) * square))
    out = values * share
    slope = share + (out * (1.0 - share)) * (2.0 * GELU_C + (6.0 * GELU_C * GELU_A) * square)
    return out, slope


def pack_rows(x_ref, wide, rows, n_img, n_tok):
    wide[...] = jnp.zeros_like(wide)
    for img in range(n_img):
        wide[img * n_tok : (img + 1) * n_tok, :] = x_ref[img].astype(F32).T
    rows[...] = wide[...].astype(BF16)


def pool_mask(shape, n_img, n_tok, row_axis):
    row = lax.broadcasted_iota(jnp.int32, shape, row_axis)
    img = lax.broadcasted_iota(jnp.int32, shape, 1 - row_axis)
    inside = (row >= img * n_tok) & (row < (img + 1) * n_tok) & (img < n_img)
    return jnp.where(inside, 1.0, 0.0).astype(BF16)


def pooled_norm(rows, n_img, n_tok):
    n_rows = rows.shape[0]
    mask = pool_mask((POOL, n_rows), n_img, n_tok, 1)
    pooled = jnp.dot(mask, rows[...], preferred_element_type=F32) * (1.0 / n_tok)
    centered, scale = norm_parts(pooled)
    return centered * scale, scale


def forward_kernel(
    n_img, n_tok, batch_total, head_rows, lab_ref, x_hbm, wu_ref, wd_ref, wh_hbm, xs_ref, pre_ref, grad_hbm, hg_hbm,
    x_ref, wh_ref, wide, rows, staged, hg_ref, sems,
):
    layer = pl.program_id(0)
    x_copy = pltpu.make_async_copy(x_hbm, x_ref, sems.at[0])
    wh_copy = pltpu.make_async_copy(wh_hbm, wh_ref, sems.at[1])

    @pl.when(layer == 0)
    def _():
        x_copy.start()
        wh_copy.start()
        x_copy.wait()
        pack_rows(x_ref, wide, rows, n_img, n_tok)

    step = rows.shape[0] // CHUNKS
    for sub in range(wu_ref.shape[0]):
        up_b = wu_ref[sub].astype(BF16)
        down_b = wd_ref[sub].astype(BF16)
        for chunk in range(CHUNKS):
            sl = slice(chunk * step, (chunk + 1) * step)
            x_rows = rows[sl, :]
            xs_ref[sub, sl, :] = x_rows
            x_wide = x_rows.astype(F32)
            centered, scale = norm_parts(x_wide)
            u_rows = (centered * scale).astype(BF16)
            pre = jnp.dot(u_rows, up_b, preferred_element_type=F32).astype(BF16)
            pre_ref[sub, sl, :] = pre
            z_rows = gelu(pre.astype(F32)).astype(BF16)
            y_rows = lax.dot_general(z_rows, down_b, LAST, preferred_element_type=F32).astype(BF16)
            rows[sl, :] = (x_wide + y_rows.astype(F32)).astype(BF16)

    @pl.when(layer == pl.num_programs(0) - 1)
    def _():
        wh_copy.wait()
        normed, scale = pooled_norm(rows, n_img, n_tok)
        normed_b = normed.astype(BF16)
        head_b = wh_ref[...].astype(BF16)
        logits = jnp.dot(normed_b, head_b, preferred_element_type=F32)
        top = jnp.max(logits, axis=-1, keepdims=True)
        exps = jnp.exp(logits - top)
        probs = exps / jnp.sum(exps, axis=-1, keepdims=True)
        classes = lax.broadcasted_iota(jnp.int32, logits.shape, 1)
        image = lax.broadcasted_iota(jnp.int32, logits.shape, 0)
        hit = jnp.zeros(logits.shape, jnp.bool_)
        for img in range(n_img):
            hit = hit | ((image == img) & (classes == lab_ref[img]))
        targets = jnp.where(hit, 1.0, 0.0)
        grad_b = jnp.where(image < n_img, (probs - targets) * (1.0 / batch_total), 0.0).astype(BF16)
        grad_normed = lax.dot_general(grad_b, head_b, LAST, preferred_element_type=F32).astype(BF16)
        grad_pooled = norm_pull(normed, scale, grad_normed.astype(F32))
        per_row = (grad_pooled / n_tok).astype(BF16)
        spread = pool_mask((rows.shape[0], POOL), n_img, n_tok, 0)
        rows[...] = jnp.dot(spread, per_row, preferred_element_type=F32).astype(BF16)
        grad_copy = pltpu.make_async_copy(rows, grad_hbm, sems.at[0])
        grad_copy.start()
        head_grad = lax.dot_general(normed_b, grad_b, ROWS, preferred_element_type=F32).astype(BF16)
        staged[...] = jnp.zeros_like(staged)
        staged[: head_grad.shape[0], : head_grad.shape[1]] = head_grad.astype(F32)
        hg_ref[...] = jnp.zeros_like(hg_ref)
        for dev in range(16):
            for tile in range(staged.shape[1] // 128):
                block = staged[dev * head_rows : dev * head_rows + 16, tile * 128 : (tile + 1) * 128]
                hg_ref[tile // 3, dev // 8, (dev // 4) % 2, (dev // 2) % 2, dev % 2, (tile % 3) * 16 : (tile % 3) * 16 + 16, :] = block.astype(BF16)
        hg_copy = pltpu.make_async_copy(hg_ref, hg_hbm, sems.at[1])
        hg_copy.start()
        grad_copy.wait()
        hg_copy.wait()


def next_kernel(
    n_img, n_tok, head_rows, lr_ref, x_hbm, wu_ref, wd_ref, mom_ref, all_hbm, wh_hbm, mh_in, mu_in, md_in,
    nwu_ref, nwd_ref, nwh_hbm, log_hbm, mh_out, mu_out, md_out,
    x_ref, wh_ref, mh_ref, log_ref, wide, rows, keep_h, keep_u, keep_d, sems,
):
    layer = pl.program_id(0)
    x_copy = pltpu.make_async_copy(x_hbm, x_ref, sems.at[0])
    wh_copy = pltpu.make_async_copy(wh_hbm, wh_ref, sems.at[1])
    kept = ((mh_in, keep_h, mh_out), (mu_in, keep_u, mu_out), (md_in, keep_d, md_out))
    takes = tuple(pltpu.make_async_copy(src, ref, sems.at[3 + i]) for i, (src, ref, _) in enumerate(kept))
    gives = tuple(pltpu.make_async_copy(ref, dst, sems.at[3 + i]) for i, (_, ref, dst) in enumerate(kept))
    mh_copy = pltpu.make_async_copy(all_hbm.at[all_hbm.shape[0] - 1], mh_ref, sems.at[2])

    @pl.when(layer == 0)
    def _():
        x_copy.start()
        wh_copy.start()
        mh_copy.start()
        for copy in takes:
            copy.start()
        x_copy.wait()
        pack_rows(x_ref, wide, rows, n_img, n_tok)

    @pl.when(layer == pl.num_programs(0) // 2)
    def _():
        for copy in takes:
            copy.wait()
        for copy in gives:
            copy.start()

    rate = lr_ref[0, 0]
    step = rows.shape[0] // CHUNKS
    for sub in range(wu_ref.shape[0]):
        mixed = mom_ref[sub, 2].T.astype(F32)
        nwu_ref[sub, :128, :] = wu_ref[sub, :128, :] - rate * mom_ref[sub, 0].T.astype(F32)
        nwu_ref[sub, 128:, :] = wu_ref[sub, 128:, :] - rate * mixed[64:, :]
        nwd_ref[sub, :128, :] = wd_ref[sub, :128, :] - rate * mom_ref[sub, 1].T.astype(F32)
        nwd_ref[sub, 128:, :] = wd_ref[sub, 128:, :] - rate * mixed[:64, :]
        up_b = nwu_ref[sub].astype(BF16) * 0.5
        down_b = nwd_ref[sub].astype(BF16)
        for chunk in range(CHUNKS):
            sl = slice(chunk * step, (chunk + 1) * step)
            x_wide = rows[sl, :].astype(F32)
            centered, scale = norm_parts(x_wide)
            u_rows = (centered * scale).astype(BF16)
            half = jnp.dot(u_rows, up_b, preferred_element_type=F32).astype(BF16)
            z_rows = gelu_half(half.astype(F32)).astype(BF16)
            y_rows = lax.dot_general(z_rows, down_b, LAST, preferred_element_type=F32).astype(BF16)
            rows[sl, :] = (x_wide + y_rows.astype(F32)).astype(BF16)

    @pl.when(layer == pl.num_programs(0) - 1)
    def _():
        wh_copy.wait()
        mh_copy.wait()
        n_cls = wh_ref.shape[1]
        for dev in range(16):
            for tile in range(-(-n_cls // 128)):
                span = slice(tile * 128, min(n_cls, (tile + 1) * 128))
                block = mh_ref[tile // 3, dev * 48 + (tile % 3) * 16 : dev * 48 + (tile % 3) * 16 + 16, :].astype(F32)
                keep = slice(dev * head_rows, (dev + 1) * head_rows)
                wh_ref[keep, span] = wh_ref[keep, span] - rate * block[:head_rows, : span.stop - span.start]
        out_copy = pltpu.make_async_copy(wh_ref, nwh_hbm, sems.at[1])
        out_copy.start()
        normed, _ = pooled_norm(rows, n_img, n_tok)
        logits = jnp.dot(normed.astype(BF16), wh_ref[...].astype(BF16), preferred_element_type=F32)
        log_ref[...] = logits[:n_img]
        log_copy = pltpu.make_async_copy(log_ref, log_hbm, sems.at[0])
        log_copy.start()
        log_copy.wait()
        out_copy.wait()
        for copy in gives:
            copy.wait()


def backward_kernel(
    n_items, sc_ref, gh_hbm, grad_hbm, xs_ref, pre_ref, wu_ref, wd_ref, mh_hbm, mu_hbm, md_hbm, nmh_hbm, nmu_hbm, nmd_hbm, all_ref,
    g_rows, z_buf, da_buf, u_buf, mh_wide, mh_ref, mu_ref, md_ref, g_buf, pair_buf, sum_buf, rcv0, rcv1, rcv2, ag_buf,
    d2d_send, d2d_recv, rs_send, rs_recv, ag_send, ag_recv, out_sem, in_sem, mom_sem,
):
    t = pl.program_id(0)
    me = lax.axis_index("data")
    core = lax.rem(me, 2)
    place = (lax.div(me, 8), lax.rem(lax.div(me, 4), 2), lax.rem(lax.div(me, 2), 2))
    peers = tuple(me + (1 - 2 * place[axis]) * w for axis, w in ((0, 8), (1, 4), (2, 2)))
    twin = me + 1 - 2 * core
    rcv = (rcv0, rcv1, rcv2)

    @pl.when(t == 0)
    def _():
        barrier = pltpu.get_barrier_semaphore()
        for peer in peers + (twin,):
            pl.semaphore_signal(barrier, inc=1, device_id=(peer,), device_id_type=MESH_ID)
        pl.semaphore_wait(barrier, 4)

    def pair_copy(item):
        slot = lax.rem(item, G_SLOTS)
        return pltpu.make_async_remote_copy(
            src_ref=g_buf.at[slot, :, :, :, :, 1 - core],
            dst_ref=pair_buf.at[slot],
            send_sem=d2d_send.at[0, slot],
            recv_sem=d2d_recv.at[0, slot],
            device_id=(twin,),
            device_id_type=MESH_ID,
        )

    def cut(part, stage, value):
        index = [slice(None)] * 3
        for axis in ORDER[part][:stage]:
            index[axis] = place[axis]
        index[ORDER[part][stage]] = value
        return tuple(index)

    def rs_copy(item, stage, part):
        axis = ORDER[part][stage]
        slot = lax.rem(item, IN_SLOTS)
        return pltpu.make_async_remote_copy(
            src_ref=sum_buf.at[(lax.rem(item, RS_SLOTS), part) + cut(part, stage, 1 - place[axis])],
            dst_ref=rcv[stage].at[slot, part],
            send_sem=rs_send.at[stage, part, slot],
            recv_sem=rs_recv.at[stage, part, slot],
            device_id=(peers[axis],),
            device_id_type=MESH_ID,
        )

    def ag_copy(item, stage, part):
        index = [place[0], place[1], place[2]]
        for axis in ORDER[part][:stage]:
            index[axis] = slice(None)
        view = ag_buf.at[(lax.rem(item, AG_SLOTS), part) + tuple(index) + (core,)]
        return pltpu.make_async_remote_copy(
            src_ref=view,
            dst_ref=view,
            send_sem=ag_send.at[stage, part, lax.rem(item, IN_SLOTS)],
            recv_sem=ag_recv.at[stage, part, lax.rem(item, IN_SLOTS)],
            device_id=(peers[ORDER[part][stage]],),
            device_id_type=MESH_ID,
        )

    def twin_copy(item):
        view = ag_buf.at[lax.rem(item, AG_SLOTS), :, :, :, :, core]
        return pltpu.make_async_remote_copy(
            src_ref=view,
            dst_ref=view,
            send_sem=d2d_send.at[1, lax.rem(item, 2)],
            recv_sem=d2d_recv.at[1, lax.rem(item, 2)],
            device_id=(twin,),
            device_id_type=MESH_ID,
        )

    def out_copy(item):
        return pltpu.make_async_copy(ag_buf.at[lax.rem(item, AG_SLOTS)], all_ref.at[n_items - 1 - item], out_sem.at[lax.rem(item, 2)])

    def at_lag(lag):
        return (t >= lag) & (t < n_items + lag)

    head_copy = pltpu.make_async_copy(gh_hbm, g_buf.at[0], in_sem.at[0])
    grad_copy = pltpu.make_async_copy(grad_hbm, g_rows, in_sem.at[1])
    moms = tuple(
        pltpu.make_async_copy(src, dst, in_sem.at[2 + i]) for i, (src, dst) in enumerate(((mh_hbm, mh_ref), (mu_hbm, mu_ref), (md_hbm, md_ref)))
    )
    moms_out = tuple(
        pltpu.make_async_copy(src, dst, mom_sem.at[i]) for i, (src, dst) in enumerate(((mh_ref, nmh_hbm), (mu_ref, nmu_hbm), (md_ref, nmd_hbm)))
    )

    @pl.when(t == 0)
    def _():
        head_copy.start()
        grad_copy.start()
        for copy in moms:
            copy.start()

    @pl.when(t == 1)
    def _():
        grad_copy.wait()

    @pl.when((t >= 1) & (t < n_items))
    def _():
        up_b = wu_ref[0].astype(BF16)
        down_b = wd_ref[0].astype(BF16)
        step = g_rows.shape[0] // CHUNKS
        grad_old = g_rows[...]
        for chunk in range(CHUNKS):
            sl = slice(chunk * step, (chunk + 1) * step)
            g_old = grad_old[sl, :]
            z_wide, slope = gelu_both(pre_ref[0, sl, :].astype(F32))
            z_buf[sl, :] = z_wide.astype(BF16)
            grad_z = jnp.dot(g_old, down_b, preferred_element_type=F32).astype(BF16)
            grad_a = (grad_z.astype(F32) * slope).astype(BF16)
            da_buf[sl, :] = grad_a
            centered, scale = norm_parts(xs_ref[0, sl, :].astype(F32))
            normed = centered * scale
            u_buf[sl, :] = normed.astype(BF16)
            grad_u = lax.dot_general(grad_a, up_b, LAST, preferred_element_type=F32).astype(BF16)
            grad_x = norm_pull(normed, scale, grad_u.astype(F32))
            g_rows[sl, :] = (g_old.astype(F32) + grad_x).astype(BF16)
        down_t = lax.dot_general(grad_old, z_buf[...], ROWS, preferred_element_type=F32).astype(BF16)
        up_g = lax.dot_general(u_buf[...], da_buf[...], ROWS, preferred_element_type=F32).astype(BF16)
        for part, value in enumerate((up_g[:128, :], down_t[:128, :], jnp.concatenate([down_t[128:, :], up_g[128:, :]], axis=0))):
            turned = value.T
            for dev in range(16):
                block = turned[dev * 48 : (dev + 1) * 48, :]
                g_buf[lax.rem(t, G_SLOTS), part, dev // 8, (dev // 4) % 2, (dev // 2) % 2, dev % 2] = block

    @pl.when(at_lag(UPDATE))
    def _():
        item = t - UPDATE
        for part in range(PARTS):
            rs_copy(item, 2, part).wait()

        def reduced(part):
            return (sum_buf[lax.rem(item, RS_SLOTS), part, place[0], place[1], place[2]] + rcv[2][lax.rem(item, IN_SLOTS), part]).astype(F32)

        def hand_on(part, mom):
            ag_buf[lax.rem(item, AG_SLOTS), part, place[0], place[1], place[2], core] = mom.astype(BF16)

        @pl.when(t == UPDATE)
        def _():
            for copy in moms:
                copy.wait()
            head_rows, n_cls = mh_ref.shape
            mh_wide[...] = jnp.zeros_like(mh_wide)
            mh_wide[:head_rows, :n_cls] = mh_ref[...]
            for part in range(PARTS):
                lanes = [slice((3 * part + i) * 128, (3 * part + i + 1) * 128) for i in range(3)]
                mom = sc_ref[0, 0] * jnp.concatenate([mh_wide[:, one] for one in lanes], axis=0) + reduced(part)
                for i in range(3):
                    mh_wide[:, lanes[i]] = mom[i * 16 : (i + 1) * 16, :]
                hand_on(part, mom)
            mh_ref[...] = mh_wide[:head_rows, :n_cls]

        @pl.when(t > UPDATE)
        def _():
            layer = n_items - 1 - item
            mixed = reduced(2)
            up_a = sc_ref[0, 0] * mu_ref[layer, :, :128] + reduced(0)
            down_a = sc_ref[0, 0] * md_ref[layer, :, :128] + reduced(1)
            up_z = sc_ref[0, 0] * mu_ref[layer, :, 128:] + mixed[:, 64:]
            down_z = sc_ref[0, 0] * md_ref[layer, :, 128:] + mixed[:, :64]
            mu_ref[layer, :, :128] = up_a
            mu_ref[layer, :, 128:] = up_z
            md_ref[layer, :, :128] = down_a
            md_ref[layer, :, 128:] = down_z
            hand_on(0, up_a)
            hand_on(1, down_a)
            hand_on(2, jnp.concatenate([down_z, up_z], axis=1))

    for stage in (1, 0):

        @pl.when(at_lag(3 + 2 * stage))
        def _(stage=stage):
            item = t - 3 - 2 * stage
            for part in range(PARTS):
                rs_copy(item, stage, part).wait()
                kept = (lax.rem(item, RS_SLOTS), part) + cut(part, stage, place[ORDER[part][stage]])
                sum_buf[kept] = sum_buf[kept] + rcv[stage][lax.rem(item, IN_SLOTS), part]
                rs_copy(item, stage + 1, part).start()

    @pl.when(at_lag(1))
    def _():
        item = t - 1
        pair_copy(item).wait()
        for part in range(PARTS):
            kept = g_buf[lax.rem(item, G_SLOTS), part, :, :, :, core]
            sum_buf[lax.rem(item, RS_SLOTS), part] = kept + pair_buf[lax.rem(item, G_SLOTS), part]
            rs_copy(item, 0, part).start()

    @pl.when(t == 0)
    def _():
        head_copy.wait()
        pair_copy(0).start()

    @pl.when((t >= 1) & (t < n_items))
    def _():
        pair_copy(t).start()

    @pl.when(at_lag(TWIN + 2))
    def _():
        out_copy(t - TWIN - 2).wait()

    @pl.when(at_lag(TWIN + 1))
    def _():
        item = t - TWIN - 1
        twin_copy(item).wait()
        out_copy(item).start()

    for stage in (3, 2, 1):

        @pl.when(at_lag(UPDATE + 2 * stage))
        def _(stage=stage):
            item = t - UPDATE - 2 * stage
            for part in range(PARTS):
                ag_copy(item, stage - 1, part).wait()
                if stage < 3:
                    ag_copy(item, stage, part).start()
            if stage == 3:
                twin_copy(item).start()

    @pl.when(at_lag(UPDATE))
    def _():
        for part in range(PARTS):
            ag_copy(t - UPDATE, 0, part).start()

    @pl.when(t == n_items + UPDATE)
    def _():
        for copy in moms_out:
            copy.start()

    @pl.when(t == n_items + UPDATE + 3)
    def _():
        for copy in moms_out:
            copy.wait()


def solution(mesh):
    n_dev = mesh.shape["data"]

    def local_step(x_now, x_next, labels, w_up, w_down, w_head, mom_up, mom_down, mom_head, learn_rate, mom_decay):
        n_img, n_tok, width = x_now.shape
        n_layers, _, hidden = w_up.shape
        n_cls = w_head.shape[1]
        n_rows = -(-n_img * n_tok // (16 * CHUNKS)) * 16 * CHUNKS
        n_items = n_layers + 1
        cols = mom_up.shape[2]
        head_rows = mom_head.shape[0]
        n_tile = -(-n_cls // 128)

        down_t = w_down.transpose(0, 2, 1)
        per = 2 if n_layers % 2 == 0 else 1
        any_spec = pl.BlockSpec(memory_space=pl.ANY)
        blocks = (PARTS, 2, 2, 2, 2, cols, 128)
        xs, pre, grad_rows, head_g = pl.pallas_call(
            functools.partial(forward_kernel, n_img, n_tok, n_img * n_dev, head_rows),
            grid=(n_layers // per,),
            in_specs=[
                pl.BlockSpec(memory_space=pltpu.SMEM),
                any_spec,
                pl.BlockSpec((per, width, hidden), lambda i: (i, 0, 0)),
                pl.BlockSpec((per, width, hidden), lambda i: (i, 0, 0)),
                any_spec,
            ],
            out_specs=[
                pl.BlockSpec((per, n_rows, width), lambda i: (i, 0, 0)),
                pl.BlockSpec((per, n_rows, hidden), lambda i: (i, 0, 0)),
                any_spec,
                any_spec,
            ],
            out_shape=[
                jax.ShapeDtypeStruct((n_layers, n_rows, width), BF16),
                jax.ShapeDtypeStruct((n_layers, n_rows, hidden), BF16),
                jax.ShapeDtypeStruct((n_rows, width), BF16),
                jax.ShapeDtypeStruct(blocks, BF16),
            ],
            scratch_shapes=[
                pltpu.VMEM((n_img, width, n_tok), BF16),
                pltpu.VMEM(w_head.shape, F32),
                pltpu.VMEM((n_rows, width), F32),
                pltpu.VMEM((n_rows, width), BF16),
                pltpu.VMEM((n_dev * head_rows + 16, n_tile * 128), F32),
                pltpu.VMEM(blocks, BF16),
                pltpu.SemaphoreType.DMA((2,)),
            ],
            compiler_params=pltpu.CompilerParams(vmem_limit_bytes=VMEM_LIMIT),
            name="step_forward",
        )(labels, x_now.transpose(0, 2, 1), w_up, down_t, w_head)

        def layer_at(t):
            return jnp.clip(n_items - 1 - t, 0, n_layers - 1)

        block = (PARTS, 2, 2, 2)
        head_kept, up_kept, down_kept, gathered = pl.pallas_call(
            functools.partial(backward_kernel, n_items),
            grid=(n_items + TWIN + 2,),
            in_specs=[
                pl.BlockSpec(memory_space=pltpu.SMEM),
                any_spec,
                any_spec,
                pl.BlockSpec((1, n_rows, width), lambda t: (layer_at(t), 0, 0)),
                pl.BlockSpec((1, n_rows, hidden), lambda t: (layer_at(t), 0, 0)),
                pl.BlockSpec((1, width, hidden), lambda t: (layer_at(t), 0, 0)),
                pl.BlockSpec((1, width, hidden), lambda t: (layer_at(t), 0, 0)),
                any_spec,
                any_spec,
                any_spec,
            ],
            out_specs=[any_spec] * 4,
            out_shape=[
                jax.ShapeDtypeStruct(mom_head.shape, F32),
                jax.ShapeDtypeStruct((n_layers, cols, width), F32),
                jax.ShapeDtypeStruct((n_layers, cols, width), F32),
                jax.ShapeDtypeStruct((n_items, PARTS, 2, 2, 2, 2, cols, 128), BF16),
            ],
            scratch_shapes=[
                pltpu.VMEM((n_rows, width), BF16),
                pltpu.VMEM((n_rows, hidden), BF16),
                pltpu.VMEM((n_rows, hidden), BF16),
                pltpu.VMEM((n_rows, width), BF16),
                pltpu.VMEM((16, 9 * 128), F32),
                pltpu.VMEM(mom_head.shape, F32),
                pltpu.VMEM((n_layers, cols, width), F32),
                pltpu.VMEM((n_layers, cols, width), F32),
                pltpu.VMEM((G_SLOTS,) + block + (2, cols, 128), BF16),
                pltpu.VMEM((G_SLOTS,) + block + (cols, 128), BF16),
                pltpu.VMEM((RS_SLOTS,) + block + (cols, 128), BF16),
                pltpu.VMEM((IN_SLOTS, PARTS, 2, 2, cols, 128), BF16),
                pltpu.VMEM((IN_SLOTS, PARTS, 2, cols, 128), BF16),
                pltpu.VMEM((IN_SLOTS, PARTS, cols, 128), BF16),
                pltpu.VMEM((AG_SLOTS,) + block + (2, cols, 128), BF16),
                pltpu.SemaphoreType.DMA((2, 2)),
                pltpu.SemaphoreType.DMA((2, 2)),
                pltpu.SemaphoreType.DMA((3, PARTS, IN_SLOTS)),
                pltpu.SemaphoreType.DMA((3, PARTS, IN_SLOTS)),
                pltpu.SemaphoreType.DMA((3, PARTS, IN_SLOTS)),
                pltpu.SemaphoreType.DMA((3, PARTS, IN_SLOTS)),
                pltpu.SemaphoreType.DMA((2,)),
                pltpu.SemaphoreType.DMA((5,)),
                pltpu.SemaphoreType.DMA((3,)),
            ],
            compiler_params=pltpu.CompilerParams(vmem_limit_bytes=VMEM_LIMIT, collective_id=0, has_side_effects=True),
            name="step_backward",
        )(mom_decay.reshape(1, 1), head_g, grad_rows, xs, pre, w_up, down_t, mom_head, mom_up.transpose(0, 2, 1), mom_down)

        gathered = gathered.reshape(n_items, PARTS, n_dev * cols, 128)
        new_w_up, new_down_t, new_w_head, logits, new_mom_head, mom_up_new, new_mom_down = pl.pallas_call(
            functools.partial(next_kernel, n_img, n_tok, head_rows),
            grid=(n_layers // per,),
            in_specs=[
                pl.BlockSpec(memory_space=pltpu.SMEM),
                any_spec,
                pl.BlockSpec((per, width, hidden), lambda i: (i, 0, 0)),
                pl.BlockSpec((per, width, hidden), lambda i: (i, 0, 0)),
                pl.BlockSpec((per, PARTS, n_dev * cols, 128), lambda i: (i, 0, 0, 0)),
                any_spec,
                any_spec,
                any_spec,
                any_spec,
                any_spec,
            ],
            out_specs=[
                pl.BlockSpec((per, width, hidden), lambda i: (i, 0, 0)),
                pl.BlockSpec((per, width, hidden), lambda i: (i, 0, 0)),
            ]
            + [any_spec] * 5,
            out_shape=[
                jax.ShapeDtypeStruct(w_up.shape, F32),
                jax.ShapeDtypeStruct(w_up.shape, F32),
                jax.ShapeDtypeStruct(w_head.shape, F32),
                jax.ShapeDtypeStruct((n_img, n_cls), F32),
                jax.ShapeDtypeStruct(mom_head.shape, F32),
                jax.ShapeDtypeStruct((n_layers, cols, width), F32),
                jax.ShapeDtypeStruct((n_layers, cols, width), F32),
            ],
            scratch_shapes=[
                pltpu.VMEM((n_img, width, n_tok), BF16),
                pltpu.VMEM(w_head.shape, F32),
                pltpu.VMEM((PARTS, n_dev * cols, 128), BF16),
                pltpu.VMEM((n_img, n_cls), F32),
                pltpu.VMEM((n_rows, width), F32),
                pltpu.VMEM((n_rows, width), BF16),
                pltpu.VMEM(mom_head.shape, F32),
                pltpu.VMEM((n_layers, cols, width), F32),
                pltpu.VMEM((n_layers, cols, width), F32),
                pltpu.SemaphoreType.DMA((6,)),
            ],
            compiler_params=pltpu.CompilerParams(vmem_limit_bytes=VMEM_LIMIT),
            name="step_next",
        )(learn_rate.reshape(1, 1), x_next.transpose(0, 2, 1), w_up, down_t, gathered, gathered, w_head, head_kept, up_kept, down_kept)

        return (logits, new_w_up, new_down_t.transpose(0, 2, 1), new_w_head, mom_up_new.transpose(0, 2, 1), new_mom_down, new_mom_head)

    spec_up = P(None, None, "data")
    spec_down = P(None, "data", None)
    spec_head = P("data", None)
    return jax.shard_map(
        local_step,
        mesh=mesh,
        in_specs=(P("data"), P("data"), P("data"), P(), P(), P(), spec_up, spec_down, spec_head, P(), P()),
        out_specs=(P("data"), P(), P(), P(), spec_up, spec_down, spec_head),
        check_vma=False,
    )
```

```python
import functools

import jax
import jax.numpy as jnp
from jax import lax
from jax.experimental import pallas as pl
from jax.experimental.pallas import tpu as pltpu
from jax.sharding import PartitionSpec as P

LN_EPS = 1e-6
GELU_C = 0.7978845608028654
GELU_A = 0.044715
F32 = jnp.float32
BF16 = jnp.bfloat16
LAST = (((1,), (1,)), ((), ()))
ROWS = (((0,), (0,)), ((), ()))
MESH_ID = pl.DeviceIdType.MESH
VMEM_LIMIT = 62 * 1024 * 1024
CHUNKS = 1
G_SLOTS = 2
RS_SLOTS = 4
IN_SLOTS = 4
AG_SLOTS = 12
UPDATE = 4
TWIN = 10
PARTS = 3
POOL = 16
ORDER = ((0, 1, 2), (1, 2, 0), (2, 0, 1))


def norm_parts(values):
    mean_v = jnp.mean(values, axis=-1, keepdims=True)
    centered = values - mean_v
    var_v = jnp.mean(centered * centered, axis=-1, keepdims=True)
    return centered, lax.rsqrt(var_v + LN_EPS)


def norm_pull(normed, scale, grad):
    mean_g = jnp.mean(grad, axis=-1, keepdims=True)
    mean_gn = jnp.mean(grad * normed, axis=-1, keepdims=True)
    return scale * (grad - mean_g - normed * mean_gn)


def gelu(values):
    inner = values * (GELU_C + (GELU_C * GELU_A) * (values * values))
    return values * (0.5 + 0.5 * jnp.tanh(inner))


def gelu_half(half):
    tanh_v = jnp.tanh(half * (2.0 * GELU_C + (8.0 * GELU_C * GELU_A) * (half * half)))
    return half + half * tanh_v


def gelu_both(values):
    square = values * values
    share = 0.5 + 0.5 * jnp.tanh(values * (GELU_C + (GELU_C * GELU_A) * square))
    out = values * share
    slope = share + (out * (1.0 - share)) * (2.0 * GELU_C + (6.0 * GELU_C * GELU_A) * square)
    return out, slope


def pack_rows(x_ref, wide, rows, n_img, n_tok):
    wide[...] = jnp.zeros_like(wide)
    for img in range(n_img):
        wide[img * n_tok : (img + 1) * n_tok, :] = x_ref[img].astype(F32).T
    rows[...] = wide[...].astype(BF16)


def pool_mask(shape, n_img, n_tok, row_axis):
    row = lax.broadcasted_iota(jnp.int32, shape, row_axis)
    img = lax.broadcasted_iota(jnp.int32, shape, 1 - row_axis)
    inside = (row >= img * n_tok) & (row < (img + 1) * n_tok) & (img < n_img)
    return jnp.where(inside, 1.0, 0.0).astype(BF16)


def pooled_norm(rows, n_img, n_tok):
    n_rows = rows.shape[0]
    mask = pool_mask((POOL, n_rows), n_img, n_tok, 1)
    pooled = jnp.dot(mask, rows[...], preferred_element_type=F32) * (1.0 / n_tok)
    centered, scale = norm_parts(pooled)
    return centered * scale, scale


def forward_kernel(
    n_img, n_tok, batch_total, head_rows, lab_ref, x_hbm, wu_ref, wd_ref, wh_hbm, xs_ref, pre_ref, grad_hbm, hg_hbm,
    x_ref, wh_ref, wide, rows, staged, hg_ref, sems,
):
    layer = pl.program_id(0)
    x_copy = pltpu.make_async_copy(x_hbm, x_ref, sems.at[0])
    wh_copy = pltpu.make_async_copy(wh_hbm, wh_ref, sems.at[1])

    @pl.when(layer == 0)
    def _():
        x_copy.start()
        wh_copy.start()
        x_copy.wait()
        pack_rows(x_ref, wide, rows, n_img, n_tok)

    step = rows.shape[0] // CHUNKS
    for sub in range(wu_ref.shape[0]):
        up_b = wu_ref[sub].astype(BF16)
        down_b = wd_ref[sub].astype(BF16)
        for chunk in range(CHUNKS):
            sl = slice(chunk * step, (chunk + 1) * step)
            x_rows = rows[sl, :]
            xs_ref[sub, sl, :] = x_rows
            x_wide = x_rows.astype(F32)
            centered, scale = norm_parts(x_wide)
            u_rows = (centered * scale).astype(BF16)
            pre = jnp.dot(u_rows, up_b, preferred_element_type=F32).astype(BF16)
            pre_ref[sub, sl, :] = pre
            z_rows = gelu(pre.astype(F32)).astype(BF16)
            y_rows = lax.dot_general(z_rows, down_b, LAST, preferred_element_type=F32).astype(BF16)
            rows[sl, :] = (x_wide + y_rows.astype(F32)).astype(BF16)

    @pl.when(layer == pl.num_programs(0) - 1)
    def _():
        wh_copy.wait()
        normed, scale = pooled_norm(rows, n_img, n_tok)
        normed_b = normed.astype(BF16)
        head_b = wh_ref[...].astype(BF16)
        logits = jnp.dot(normed_b, head_b, preferred_element_type=F32)
        top = jnp.max(logits, axis=-1, keepdims=True)
        exps = jnp.exp(logits - top)
        probs = exps / jnp.sum(exps, axis=-1, keepdims=True)
        classes = lax.broadcasted_iota(jnp.int32, logits.shape, 1)
        image = lax.broadcasted_iota(jnp.int32, logits.shape, 0)
        hit = jnp.zeros(logits.shape, jnp.bool_)
        for img in range(n_img):
            hit = hit | ((image == img) & (classes == lab_ref[img]))
        targets = jnp.where(hit, 1.0, 0.0)
        grad_b = jnp.where(image < n_img, (probs - targets) * (1.0 / batch_total), 0.0).astype(BF16)
        grad_normed = lax.dot_general(grad_b, head_b, LAST, preferred_element_type=F32).astype(BF16)
        grad_pooled = norm_pull(normed, scale, grad_normed.astype(F32))
        per_row = (grad_pooled / n_tok).astype(BF16)
        spread = pool_mask((rows.shape[0], POOL), n_img, n_tok, 0)
        rows[...] = jnp.dot(spread, per_row, preferred_element_type=F32).astype(BF16)
        grad_copy = pltpu.make_async_copy(rows, grad_hbm, sems.at[0])
        grad_copy.start()
        head_grad = lax.dot_general(normed_b, grad_b, ROWS, preferred_element_type=F32).astype(BF16)
        staged[...] = jnp.zeros_like(staged)
        staged[: head_grad.shape[0], : head_grad.shape[1]] = head_grad.astype(F32)
        hg_ref[...] = jnp.zeros_like(hg_ref)
        for dev in range(16):
            for tile in range(staged.shape[1] // 128):
                block = staged[dev * head_rows : dev * head_rows + 16, tile * 128 : (tile + 1) * 128]
                hg_ref[tile // 3, dev // 8, (dev // 4) % 2, (dev // 2) % 2, dev % 2, (tile % 3) * 16 : (tile % 3) * 16 + 16, :] = block.astype(BF16)
        hg_copy = pltpu.make_async_copy(hg_ref, hg_hbm, sems.at[1])
        hg_copy.start()
        grad_copy.wait()
        hg_copy.wait()


def next_kernel(
    n_img, n_tok, head_rows, lr_ref, x_hbm, wu_ref, wd_ref, mom_ref, all_hbm, wh_hbm, mh_in, mu_in, md_in,
    nwu_ref, nwd_ref, nwh_hbm, log_hbm, mh_out, mu_out, md_out,
    x_ref, wh_ref, mh_ref, log_ref, wide, rows, keep_h, keep_u, keep_d, sems,
):
    layer = pl.program_id(0)
    x_copy = pltpu.make_async_copy(x_hbm, x_ref, sems.at[0])
    wh_copy = pltpu.make_async_copy(wh_hbm, wh_ref, sems.at[1])
    kept = ((mh_in, keep_h, mh_out), (mu_in, keep_u, mu_out), (md_in, keep_d, md_out))
    takes = tuple(pltpu.make_async_copy(src, ref, sems.at[3 + i]) for i, (src, ref, _) in enumerate(kept))
    gives = tuple(pltpu.make_async_copy(ref, dst, sems.at[3 + i]) for i, (_, ref, dst) in enumerate(kept))
    mh_copy = pltpu.make_async_copy(all_hbm.at[all_hbm.shape[0] - 1], mh_ref, sems.at[2])

    @pl.when(layer == 0)
    def _():
        x_copy.start()
        wh_copy.start()
        mh_copy.start()
        for copy in takes:
            copy.start()
        x_copy.wait()
        pack_rows(x_ref, wide, rows, n_img, n_tok)

    @pl.when(layer == pl.num_programs(0) // 2)
    def _():
        for copy in takes:
            copy.wait()
        for copy in gives:
            copy.start()

    rate = lr_ref[0, 0]
    step = rows.shape[0] // CHUNKS
    for sub in range(wu_ref.shape[0]):
        mixed = mom_ref[sub, 2].T.astype(F32)
        nwu_ref[sub, :128, :] = wu_ref[sub, :128, :] - rate * mom_ref[sub, 0].T.astype(F32)
        nwu_ref[sub, 128:, :] = wu_ref[sub, 128:, :] - rate * mixed[64:, :]
        nwd_ref[sub, :128, :] = wd_ref[sub, :128, :] - rate * mom_ref[sub, 1].T.astype(F32)
        nwd_ref[sub, 128:, :] = wd_ref[sub, 128:, :] - rate * mixed[:64, :]
        up_b = nwu_ref[sub].astype(BF16) * 0.5
        down_b = nwd_ref[sub].astype(BF16)
        for chunk in range(CHUNKS):
            sl = slice(chunk * step, (chunk + 1) * step)
            x_wide = rows[sl, :].astype(F32)
            centered, scale = norm_parts(x_wide)
            u_rows = (centered * scale).astype(BF16)
            half = jnp.dot(u_rows, up_b, preferred_element_type=F32).astype(BF16)
            z_rows = gelu_half(half.astype(F32)).astype(BF16)
            y_rows = lax.dot_general(z_rows, down_b, LAST, preferred_element_type=F32).astype(BF16)
            rows[sl, :] = (x_wide + y_rows.astype(F32)).astype(BF16)

    @pl.when(layer == pl.num_programs(0) - 1)
    def _():
        wh_copy.wait()
        mh_copy.wait()
        n_cls = wh_ref.shape[1]
        for dev in range(16):
            for tile in range(-(-n_cls // 128)):
                span = slice(tile * 128, min(n_cls, (tile + 1) * 128))
                block = mh_ref[tile // 3, dev * 48 + (tile % 3) * 16 : dev * 48 + (tile % 3) * 16 + 16, :].astype(F32)
                keep = slice(dev * head_rows, (dev + 1) * head_rows)
                wh_ref[keep, span] = wh_ref[keep, span] - rate * block[:head_rows, : span.stop - span.start]
        out_copy = pltpu.make_async_copy(wh_ref, nwh_hbm, sems.at[1])
        out_copy.start()
        normed, _ = pooled_norm(rows, n_img, n_tok)
        logits = jnp.dot(normed.astype(BF16), wh_ref[...].astype(BF16), preferred_element_type=F32)
        log_ref[...] = logits[:n_img]
        log_copy = pltpu.make_async_copy(log_ref, log_hbm, sems.at[0])
        log_copy.start()
        log_copy.wait()
        out_copy.wait()
        for copy in gives:
            copy.wait()


def backward_kernel(
    n_items, sc_ref, gh_hbm, grad_hbm, xs_ref, pre_ref, wu_ref, wd_ref, mh_hbm, mu_hbm, md_hbm, nmh_hbm, nmu_hbm, nmd_hbm, all_ref,
    g_rows, z_buf, da_buf, u_buf, mh_wide, mh_ref, mu_ref, md_ref, g_buf, pair_buf, sum_buf, rcv0, rcv1, rcv2, ag_buf,
    d2d_send, d2d_recv, rs_send, rs_recv, ag_send, ag_recv, out_sem, in_sem, mom_sem,
):
    t = pl.program_id(0)
    me = lax.axis_index("data")
    core = lax.rem(me, 2)
    place = (lax.div(me, 8), lax.rem(lax.div(me, 4), 2), lax.rem(lax.div(me, 2), 2))
    peers = tuple(me + (1 - 2 * place[axis]) * w for axis, w in ((0, 8), (1, 4), (2, 2)))
    twin = me + 1 - 2 * core
    rcv = (rcv0, rcv1, rcv2)

    @pl.when(t == 0)
    def _():
        barrier = pltpu.get_barrier_semaphore()
        for peer in peers + (twin,):
            pl.semaphore_signal(barrier, inc=1, device_id=(peer,), device_id_type=MESH_ID)
        pl.semaphore_wait(barrier, 4)

    def pair_copy(item):
        slot = lax.rem(item, G_SLOTS)
        return pltpu.make_async_remote_copy(
            src_ref=g_buf.at[slot, :, :, :, :, 1 - core],
            dst_ref=pair_buf.at[slot],
            send_sem=d2d_send.at[0, slot],
            recv_sem=d2d_recv.at[0, slot],
            device_id=(twin,),
            device_id_type=MESH_ID,
        )

    def cut(part, stage, value):
        index = [slice(None)] * 3
        for axis in ORDER[part][:stage]:
            index[axis] = place[axis]
        index[ORDER[part][stage]] = value
        return tuple(index)

    def rs_copy(item, stage, part):
        axis = ORDER[part][stage]
        slot = lax.rem(item, IN_SLOTS)
        return pltpu.make_async_remote_copy(
            src_ref=sum_buf.at[(lax.rem(item, RS_SLOTS), part) + cut(part, stage, 1 - place[axis])],
            dst_ref=rcv[stage].at[slot, part],
            send_sem=rs_send.at[stage, part, slot],
            recv_sem=rs_recv.at[stage, part, slot],
            device_id=(peers[axis],),
            device_id_type=MESH_ID,
        )

    def ag_copy(item, stage, part):
        index = [place[0], place[1], place[2]]
        for axis in ORDER[part][:stage]:
            index[axis] = slice(None)
        view = ag_buf.at[(lax.rem(item, AG_SLOTS), part) + tuple(index) + (core,)]
        return pltpu.make_async_remote_copy(
            src_ref=view,
            dst_ref=view,
            send_sem=ag_send.at[stage, part, lax.rem(item, IN_SLOTS)],
            recv_sem=ag_recv.at[stage, part, lax.rem(item, IN_SLOTS)],
            device_id=(peers[ORDER[part][stage]],),
            device_id_type=MESH_ID,
        )

    def twin_copy(item):
        view = ag_buf.at[lax.rem(item, AG_SLOTS), :, :, :, :, core]
        return pltpu.make_async_remote_copy(
            src_ref=view,
            dst_ref=view,
            send_sem=d2d_send.at[1, lax.rem(item, 2)],
            recv_sem=d2d_recv.at[1, lax.rem(item, 2)],
            device_id=(twin,),
            device_id_type=MESH_ID,
        )

    def out_copy(item):
        return pltpu.make_async_copy(ag_buf.at[lax.rem(item, AG_SLOTS)], all_ref.at[n_items - 1 - item], out_sem.at[lax.rem(item, 2)])

    def at_lag(lag):
        return (t >= lag) & (t < n_items + lag)

    head_copy = pltpu.make_async_copy(gh_hbm, g_buf.at[0], in_sem.at[0])
    grad_copy = pltpu.make_async_copy(grad_hbm, g_rows, in_sem.at[1])
    moms = tuple(
        pltpu.make_async_copy(src, dst, in_sem.at[2 + i]) for i, (src, dst) in enumerate(((mh_hbm, mh_ref), (mu_hbm, mu_ref), (md_hbm, md_ref)))
    )
    moms_out = tuple(
        pltpu.make_async_copy(src, dst, mom_sem.at[i]) for i, (src, dst) in enumerate(((mh_ref, nmh_hbm), (mu_ref, nmu_hbm), (md_ref, nmd_hbm)))
    )

    @pl.when(t == 0)
    def _():
        head_copy.start()
        grad_copy.start()
        for copy in moms:
            copy.start()

    @pl.when(t == 1)
    def _():
        grad_copy.wait()

    @pl.when((t >= 1) & (t < n_items))
    def _():
        up_b = wu_ref[0].astype(BF16)
        down_b = wd_ref[0].astype(BF16)
        step = g_rows.shape[0] // CHUNKS
        grad_old = g_rows[...]
        for chunk in range(CHUNKS):
            sl = slice(chunk * step, (chunk + 1) * step)
            g_old = grad_old[sl, :]
            z_wide, slope = gelu_both(pre_ref[0, sl, :].astype(F32))
            z_buf[sl, :] = z_wide.astype(BF16)
            grad_z = jnp.dot(g_old, down_b, preferred_element_type=F32).astype(BF16)
            grad_a = (grad_z.astype(F32) * slope).astype(BF16)
            da_buf[sl, :] = grad_a
            centered, scale = norm_parts(xs_ref[0, sl, :].astype(F32))
            normed = centered * scale
            u_buf[sl, :] = normed.astype(BF16)
            grad_u = lax.dot_general(grad_a, up_b, LAST, preferred_element_type=F32).astype(BF16)
            grad_x = norm_pull(normed, scale, grad_u.astype(F32))
            g_rows[sl, :] = (g_old.astype(F32) + grad_x).astype(BF16)
        down_t = lax.dot_general(grad_old, z_buf[...], ROWS, preferred_element_type=F32).astype(BF16)
        up_g = lax.dot_general(u_buf[...], da_buf[...], ROWS, preferred_element_type=F32).astype(BF16)
        for part, value in enumerate((up_g[:128, :], down_t[:128, :], jnp.concatenate([down_t[128:, :], up_g[128:, :]], axis=0))):
            turned = value.T
            for dev in range(16):
                block = turned[dev * 48 : (dev + 1) * 48, :]
                g_buf[lax.rem(t, G_SLOTS), part, dev // 8, (dev // 4) % 2, (dev // 2) % 2, dev % 2] = block

    @pl.when(at_lag(UPDATE))
    def _():
        item = t - UPDATE
        for part in range(PARTS):
            rs_copy(item, 2, part).wait()

        def reduced(part):
            return (sum_buf[lax.rem(item, RS_SLOTS), part, place[0], place[1], place[2]] + rcv[2][lax.rem(item, IN_SLOTS), part]).astype(F32)

        def hand_on(part, mom):
            ag_buf[lax.rem(item, AG_SLOTS), part, place[0], place[1], place[2], core] = mom.astype(BF16)

        @pl.when(t == UPDATE)
        def _():
            for copy in moms:
                copy.wait()
            head_rows, n_cls = mh_ref.shape
            mh_wide[...] = jnp.zeros_like(mh_wide)
            mh_wide[:head_rows, :n_cls] = mh_ref[...]
            for part in range(PARTS):
                lanes = [slice((3 * part + i) * 128, (3 * part + i + 1) * 128) for i in range(3)]
                mom = sc_ref[0, 0] * jnp.concatenate([mh_wide[:, one] for one in lanes], axis=0) + reduced(part)
                for i in range(3):
                    mh_wide[:, lanes[i]] = mom[i * 16 : (i + 1) * 16, :]
                hand_on(part, mom)
            mh_ref[...] = mh_wide[:head_rows, :n_cls]

        @pl.when(t > UPDATE)
        def _():
            layer = n_items - 1 - item
            mixed = reduced(2)
            up_a = sc_ref[0, 0] * mu_ref[layer, :, :128] + reduced(0)
            down_a = sc_ref[0, 0] * md_ref[layer, :, :128] + reduced(1)
            up_z = sc_ref[0, 0] * mu_ref[layer, :, 128:] + mixed[:, 64:]
            down_z = sc_ref[0, 0] * md_ref[layer, :, 128:] + mixed[:, :64]
            mu_ref[layer, :, :128] = up_a
            mu_ref[layer, :, 128:] = up_z
            md_ref[layer, :, :128] = down_a
            md_ref[layer, :, 128:] = down_z
            hand_on(0, up_a)
            hand_on(1, down_a)
            hand_on(2, jnp.concatenate([down_z, up_z], axis=1))

    for stage in (1, 0):

        @pl.when(at_lag(2 + stage))
        def _(stage=stage):
            item = t - 2 - stage
            for part in range(PARTS):
                rs_copy(item, stage, part).wait()
                kept = (lax.rem(item, RS_SLOTS), part) + cut(part, stage, place[ORDER[part][stage]])
                sum_buf[kept] = sum_buf[kept] + rcv[stage][lax.rem(item, IN_SLOTS), part]
                rs_copy(item, stage + 1, part).start()

    @pl.when(at_lag(1))
    def _():
        item = t - 1
        pair_copy(item).wait()
        for part in range(PARTS):
            kept = g_buf[lax.rem(item, G_SLOTS), part, :, :, :, core]
            sum_buf[lax.rem(item, RS_SLOTS), part] = kept + pair_buf[lax.rem(item, G_SLOTS), part]
            rs_copy(item, 0, part).start()

    @pl.when(t == 0)
    def _():
        head_copy.wait()
        pair_copy(0).start()

    @pl.when((t >= 1) & (t < n_items))
    def _():
        pair_copy(t).start()

    @pl.when(at_lag(TWIN + 2))
    def _():
        out_copy(t - TWIN - 2).wait()

    @pl.when(at_lag(TWIN + 1))
    def _():
        item = t - TWIN - 1
        twin_copy(item).wait()
        out_copy(item).start()

    for stage in (3, 2, 1):

        @pl.when(at_lag(UPDATE + 2 * stage))
        def _(stage=stage):
            item = t - UPDATE - 2 * stage
            for part in range(PARTS):
                ag_copy(item, stage - 1, part).wait()
                if stage < 3:
                    ag_copy(item, stage, part).start()
            if stage == 3:
                twin_copy(item).start()

    @pl.when(at_lag(UPDATE))
    def _():
        for part in range(PARTS):
            ag_copy(t - UPDATE, 0, part).start()

    @pl.when(t == n_items + UPDATE)
    def _():
        for copy in moms_out:
            copy.start()

    @pl.when(t == n_items + UPDATE + 3)
    def _():
        for copy in moms_out:
            copy.wait()


def solution(mesh):
    n_dev = mesh.shape["data"]

    def local_step(x_now, x_next, labels, w_up, w_down, w_head, mom_up, mom_down, mom_head, learn_rate, mom_decay):
        n_img, n_tok, width = x_now.shape
        n_layers, _, hidden = w_up.shape
        n_cls = w_head.shape[1]
        n_rows = -(-n_img * n_tok // (16 * CHUNKS)) * 16 * CHUNKS
        n_items = n_layers + 1
        cols = mom_up.shape[2]
        head_rows = mom_head.shape[0]
        n_tile = -(-n_cls // 128)

        down_t = w_down.transpose(0, 2, 1)
        per = 2 if n_layers % 2 == 0 else 1
        any_spec = pl.BlockSpec(memory_space=pl.ANY)
        blocks = (PARTS, 2, 2, 2, 2, cols, 128)
        xs, pre, grad_rows, head_g = pl.pallas_call(
            functools.partial(forward_kernel, n_img, n_tok, n_img * n_dev, head_rows),
            grid=(n_layers // per,),
            in_specs=[
                pl.BlockSpec(memory_space=pltpu.SMEM),
                any_spec,
                pl.BlockSpec((per, width, hidden), lambda i: (i, 0, 0)),
                pl.BlockSpec((per, width, hidden), lambda i: (i, 0, 0)),
                any_spec,
            ],
            out_specs=[
                pl.BlockSpec((per, n_rows, width), lambda i: (i, 0, 0)),
                pl.BlockSpec((per, n_rows, hidden), lambda i: (i, 0, 0)),
                any_spec,
                any_spec,
            ],
            out_shape=[
                jax.ShapeDtypeStruct((n_layers, n_rows, width), BF16),
                jax.ShapeDtypeStruct((n_layers, n_rows, hidden), BF16),
                jax.ShapeDtypeStruct((n_rows, width), BF16),
                jax.ShapeDtypeStruct(blocks, BF16),
            ],
            scratch_shapes=[
                pltpu.VMEM((n_img, width, n_tok), BF16),
                pltpu.VMEM(w_head.shape, F32),
                pltpu.VMEM((n_rows, width), F32),
                pltpu.VMEM((n_rows, width), BF16),
                pltpu.VMEM((n_dev * head_rows + 16, n_tile * 128), F32),
                pltpu.VMEM(blocks, BF16),
                pltpu.SemaphoreType.DMA((2,)),
            ],
            compiler_params=pltpu.CompilerParams(vmem_limit_bytes=VMEM_LIMIT),
            name="step_forward",
        )(labels, x_now.transpose(0, 2, 1), w_up, down_t, w_head)

        def layer_at(t):
            return jnp.clip(n_items - 1 - t, 0, n_layers - 1)

        block = (PARTS, 2, 2, 2)
        head_kept, up_kept, down_kept, gathered = pl.pallas_call(
            functools.partial(backward_kernel, n_items),
            grid=(n_items + TWIN + 2,),
            in_specs=[
                pl.BlockSpec(memory_space=pltpu.SMEM),
                any_spec,
                any_spec,
                pl.BlockSpec((1, n_rows, width), lambda t: (layer_at(t), 0, 0)),
                pl.BlockSpec((1, n_rows, hidden), lambda t: (layer_at(t), 0, 0)),
                pl.BlockSpec((1, width, hidden), lambda t: (layer_at(t), 0, 0)),
                pl.BlockSpec((1, width, hidden), lambda t: (layer_at(t), 0, 0)),
                any_spec,
                any_spec,
                any_spec,
            ],
            out_specs=[any_spec] * 4,
            out_shape=[
                jax.ShapeDtypeStruct(mom_head.shape, F32),
                jax.ShapeDtypeStruct((n_layers, cols, width), F32),
                jax.ShapeDtypeStruct((n_layers, cols, width), F32),
                jax.ShapeDtypeStruct((n_items, PARTS, 2, 2, 2, 2, cols, 128), BF16),
            ],
            scratch_shapes=[
                pltpu.VMEM((n_rows, width), BF16),
                pltpu.VMEM((n_rows, hidden), BF16),
                pltpu.VMEM((n_rows, hidden), BF16),
                pltpu.VMEM((n_rows, width), BF16),
                pltpu.VMEM((16, 9 * 128), F32),
                pltpu.VMEM(mom_head.shape, F32),
                pltpu.VMEM((n_layers, cols, width), F32),
                pltpu.VMEM((n_layers, cols, width), F32),
                pltpu.VMEM((G_SLOTS,) + block + (2, cols, 128), BF16),
                pltpu.VMEM((G_SLOTS,) + block + (cols, 128), BF16),
                pltpu.VMEM((RS_SLOTS,) + block + (cols, 128), BF16),
                pltpu.VMEM((IN_SLOTS, PARTS, 2, 2, cols, 128), BF16),
                pltpu.VMEM((IN_SLOTS, PARTS, 2, cols, 128), BF16),
                pltpu.VMEM((IN_SLOTS, PARTS, cols, 128), BF16),
                pltpu.VMEM((AG_SLOTS,) + block + (2, cols, 128), BF16),
                pltpu.SemaphoreType.DMA((2, 2)),
                pltpu.SemaphoreType.DMA((2, 2)),
                pltpu.SemaphoreType.DMA((3, PARTS, IN_SLOTS)),
                pltpu.SemaphoreType.DMA((3, PARTS, IN_SLOTS)),
                pltpu.SemaphoreType.DMA((3, PARTS, IN_SLOTS)),
                pltpu.SemaphoreType.DMA((3, PARTS, IN_SLOTS)),
                pltpu.SemaphoreType.DMA((2,)),
                pltpu.SemaphoreType.DMA((5,)),
                pltpu.SemaphoreType.DMA((3,)),
            ],
            compiler_params=pltpu.CompilerParams(vmem_limit_bytes=VMEM_LIMIT, collective_id=0, has_side_effects=True),
            name="step_backward",
        )(mom_decay.reshape(1, 1), head_g, grad_rows, xs, pre, w_up, down_t, mom_head, mom_up.transpose(0, 2, 1), mom_down)

        gathered = gathered.reshape(n_items, PARTS, n_dev * cols, 128)
        new_w_up, new_down_t, new_w_head, logits, new_mom_head, mom_up_new, new_mom_down = pl.pallas_call(
            functools.partial(next_kernel, n_img, n_tok, head_rows),
            grid=(n_layers // per,),
            in_specs=[
                pl.BlockSpec(memory_space=pltpu.SMEM),
                any_spec,
                pl.BlockSpec((per, width, hidden), lambda i: (i, 0, 0)),
                pl.BlockSpec((per, width, hidden), lambda i: (i, 0, 0)),
                pl.BlockSpec((per, PARTS, n_dev * cols, 128), lambda i: (i, 0, 0, 0)),
                any_spec,
                any_spec,
                any_spec,
                any_spec,
                any_spec,
            ],
            out_specs=[
                pl.BlockSpec((per, width, hidden), lambda i: (i, 0, 0)),
                pl.BlockSpec((per, width, hidden), lambda i: (i, 0, 0)),
            ]
            + [any_spec] * 5,
            out_shape=[
                jax.ShapeDtypeStruct(w_up.shape, F32),
                jax.ShapeDtypeStruct(w_up.shape, F32),
                jax.ShapeDtypeStruct(w_head.shape, F32),
                jax.ShapeDtypeStruct((n_img, n_cls), F32),
                jax.ShapeDtypeStruct(mom_head.shape, F32),
                jax.ShapeDtypeStruct((n_layers, cols, width), F32),
                jax.ShapeDtypeStruct((n_layers, cols, width), F32),
            ],
            scratch_shapes=[
                pltpu.VMEM((n_img, width, n_tok), BF16),
                pltpu.VMEM(w_head.shape, F32),
                pltpu.VMEM((PARTS, n_dev * cols, 128), BF16),
                pltpu.VMEM((n_img, n_cls), F32),
                pltpu.VMEM((n_rows, width), F32),
                pltpu.VMEM((n_rows, width), BF16),
                pltpu.VMEM(mom_head.shape, F32),
                pltpu.VMEM((n_layers, cols, width), F32),
                pltpu.VMEM((n_layers, cols, width), F32),
                pltpu.SemaphoreType.DMA((6,)),
            ],
            compiler_params=pltpu.CompilerParams(vmem_limit_bytes=VMEM_LIMIT),
            name="step_next",
        )(learn_rate.reshape(1, 1), x_next.transpose(0, 2, 1), w_up, down_t, gathered, gathered, w_head, head_kept, up_kept, down_kept)

        return (logits, new_w_up, new_down_t.transpose(0, 2, 1), new_w_head, mom_up_new.transpose(0, 2, 1), new_mom_down, new_mom_head)

    spec_up = P(None, None, "data")
    spec_down = P(None, "data", None)
    spec_head = P("data", None)
    return jax.shard_map(
        local_step,
        mesh=mesh,
        in_specs=(P("data"), P("data"), P("data"), P(), P(), P(), spec_up, spec_down, spec_head, P(), P()),
        out_specs=(P("data"), P(), P(), P(), spec_up, spec_down, spec_head),
        check_vma=False,
    )
```

```python
import functools

import jax
import jax.numpy as jnp
from jax import lax
from jax.experimental import pallas as pl
from jax.experimental.pallas import tpu as pltpu
from jax.sharding import PartitionSpec as P

LN_EPS = 1e-6
GELU_C = 0.7978845608028654
GELU_A = 0.044715
F32 = jnp.float32
BF16 = jnp.bfloat16
LAST = (((1,), (1,)), ((), ()))
ROWS = (((0,), (0,)), ((), ()))
MESH_ID = pl.DeviceIdType.MESH
VMEM_LIMIT = 62 * 1024 * 1024
CHUNKS = 1
G_SLOTS = 2
RS_SLOTS = 8
IN_SLOTS = 4
AG_SLOTS = 12
UPDATE = 7
TWIN = 13
PARTS = 3
POOL = 16
ORDER = ((0, 1, 2), (1, 2, 0), (2, 0, 1))


def norm_parts(values):
    mean_v = jnp.mean(values, axis=-1, keepdims=True)
    centered = values - mean_v
    var_v = jnp.mean(centered * centered, axis=-1, keepdims=True)
    return centered, lax.rsqrt(var_v + LN_EPS)


def norm_pull(normed, scale, grad):
    mean_g = jnp.mean(grad, axis=-1, keepdims=True)
    mean_gn = jnp.mean(grad * normed, axis=-1, keepdims=True)
    return scale * (grad - mean_g - normed * mean_gn)


def gelu(values):
    inner = values * (GELU_C + (GELU_C * GELU_A) * (values * values))
    return values * (0.5 + 0.5 * jnp.tanh(inner))


def gelu_half(half):
    tanh_v = jnp.tanh(half * (2.0 * GELU_C + (8.0 * GELU_C * GELU_A) * (half * half)))
    return half + half * tanh_v


def gelu_both(values):
    square = values * values
    share = 0.5 + 0.5 * jnp.tanh(values * (GELU_C + (GELU_C * GELU_A) * square))
    out = values * share
    slope = share + (out * (1.0 - share)) * (2.0 * GELU_C + (6.0 * GELU_C * GELU_A) * square)
    return out, slope


def pack_rows(x_ref, wide, rows, n_img, n_tok):
    wide[...] = jnp.zeros_like(wide)
    for img in range(n_img):
        wide[img * n_tok : (img + 1) * n_tok, :] = x_ref[img].astype(F32).T
    rows[...] = wide[...].astype(BF16)


def pool_mask(shape, n_img, n_tok, row_axis):
    row = lax.broadcasted_iota(jnp.int32, shape, row_axis)
    img = lax.broadcasted_iota(jnp.int32, shape, 1 - row_axis)
    inside = (row >= img * n_tok) & (row < (img + 1) * n_tok) & (img < n_img)
    return jnp.where(inside, 1.0, 0.0).astype(BF16)


def pooled_norm(rows, n_img, n_tok):
    n_rows = rows.shape[0]
    mask = pool_mask((POOL, n_rows), n_img, n_tok, 1)
    pooled = jnp.dot(mask, rows[...], preferred_element_type=F32) * (1.0 / n_tok)
    centered, scale = norm_parts(pooled)
    return centered * scale, scale


def forward_kernel(
    n_img, n_tok, batch_total, head_rows, lab_ref, x_hbm, wu_ref, wd_ref, wh_hbm, xs_ref, pre_ref, grad_hbm, hg_hbm,
    x_ref, wh_ref, wide, rows, staged, hg_ref, sems,
):
    layer = pl.program_id(0)
    x_copy = pltpu.make_async_copy(x_hbm, x_ref, sems.at[0])
    wh_copy = pltpu.make_async_copy(wh_hbm, wh_ref, sems.at[1])

    @pl.when(layer == 0)
    def _():
        x_copy.start()
        wh_copy.start()
        x_copy.wait()
        pack_rows(x_ref, wide, rows, n_img, n_tok)

    step = rows.shape[0] // CHUNKS
    for sub in range(wu_ref.shape[0]):
        up_b = wu_ref[sub].astype(BF16)
        down_b = wd_ref[sub].astype(BF16)
        for chunk in range(CHUNKS):
            sl = slice(chunk * step, (chunk + 1) * step)
            x_rows = rows[sl, :]
            xs_ref[sub, sl, :] = x_rows
            x_wide = x_rows.astype(F32)
            centered, scale = norm_parts(x_wide)
            u_rows = (centered * scale).astype(BF16)
            pre = jnp.dot(u_rows, up_b, preferred_element_type=F32).astype(BF16)
            pre_ref[sub, sl, :] = pre
            z_rows = gelu(pre.astype(F32)).astype(BF16)
            y_rows = lax.dot_general(z_rows, down_b, LAST, preferred_element_type=F32).astype(BF16)
            rows[sl, :] = (x_wide + y_rows.astype(F32)).astype(BF16)

    @pl.when(layer == pl.num_programs(0) - 1)
    def _():
        wh_copy.wait()
        normed, scale = pooled_norm(rows, n_img, n_tok)
        normed_b = normed.astype(BF16)
        head_b = wh_ref[...].astype(BF16)
        logits = jnp.dot(normed_b, head_b, preferred_element_type=F32)
        top = jnp.max(logits, axis=-1, keepdims=True)
        exps = jnp.exp(logits - top)
        probs = exps / jnp.sum(exps, axis=-1, keepdims=True)
        classes = lax.broadcasted_iota(jnp.int32, logits.shape, 1)
        image = lax.broadcasted_iota(jnp.int32, logits.shape, 0)
        hit = jnp.zeros(logits.shape, jnp.bool_)
        for img in range(n_img):
            hit = hit | ((image == img) & (classes == lab_ref[img]))
        targets = jnp.where(hit, 1.0, 0.0)
        grad_b = jnp.where(image < n_img, (probs - targets) * (1.0 / batch_total), 0.0).astype(BF16)
        grad_normed = lax.dot_general(grad_b, head_b, LAST, preferred_element_type=F32).astype(BF16)
        grad_pooled = norm_pull(normed, scale, grad_normed.astype(F32))
        per_row = (grad_pooled / n_tok).astype(BF16)
        spread = pool_mask((rows.shape[0], POOL), n_img, n_tok, 0)
        rows[...] = jnp.dot(spread, per_row, preferred_element_type=F32).astype(BF16)
        grad_copy = pltpu.make_async_copy(rows, grad_hbm, sems.at[0])
        grad_copy.start()
        head_grad = lax.dot_general(normed_b, grad_b, ROWS, preferred_element_type=F32).astype(BF16)
        staged[...] = jnp.zeros_like(staged)
        staged[: head_grad.shape[0], : head_grad.shape[1]] = head_grad.astype(F32)
        hg_ref[...] = jnp.zeros_like(hg_ref)
        for dev in range(16):
            for tile in range(staged.shape[1] // 128):
                block = staged[dev * head_rows : dev * head_rows + 16, tile * 128 : (tile + 1) * 128]
                hg_ref[tile // 3, dev // 8, (dev // 4) % 2, (dev // 2) % 2, dev % 2, (tile % 3) * 16 : (tile % 3) * 16 + 16, :] = block.astype(BF16)
        hg_copy = pltpu.make_async_copy(hg_ref, hg_hbm, sems.at[1])
        hg_copy.start()
        grad_copy.wait()
        hg_copy.wait()


def next_kernel(
    n_img, n_tok, head_rows, lr_ref, x_hbm, wu_ref, wd_ref, mom_ref, all_hbm, wh_hbm, mh_in, mu_in, md_in,
    nwu_ref, nwd_ref, nwh_hbm, log_hbm, mh_out, mu_out, md_out,
    x_ref, wh_ref, mh_ref, log_ref, wide, rows, keep_h, keep_u, keep_d, sems,
):
    layer = pl.program_id(0)
    x_copy = pltpu.make_async_copy(x_hbm, x_ref, sems.at[0])
    wh_copy = pltpu.make_async_copy(wh_hbm, wh_ref, sems.at[1])
    kept = ((mh_in, keep_h, mh_out), (mu_in, keep_u, mu_out), (md_in, keep_d, md_out))
    takes = tuple(pltpu.make_async_copy(src, ref, sems.at[3 + i]) for i, (src, ref, _) in enumerate(kept))
    gives = tuple(pltpu.make_async_copy(ref, dst, sems.at[3 + i]) for i, (_, ref, dst) in enumerate(kept))
    mh_copy = pltpu.make_async_copy(all_hbm.at[all_hbm.shape[0] - 1], mh_ref, sems.at[2])

    @pl.when(layer == 0)
    def _():
        x_copy.start()
        wh_copy.start()
        mh_copy.start()
        for copy in takes:
            copy.start()
        x_copy.wait()
        pack_rows(x_ref, wide, rows, n_img, n_tok)

    @pl.when(layer == pl.num_programs(0) // 2)
    def _():
        for copy in takes:
            copy.wait()
        for copy in gives:
            copy.start()

    rate = lr_ref[0, 0]
    step = rows.shape[0] // CHUNKS
    for sub in range(wu_ref.shape[0]):
        mixed = mom_ref[sub, 2].T.astype(F32)
        nwu_ref[sub, :128, :] = wu_ref[sub, :128, :] - rate * mom_ref[sub, 0].T.astype(F32)
        nwu_ref[sub, 128:, :] = wu_ref[sub, 128:, :] - rate * mixed[64:, :]
        nwd_ref[sub, :128, :] = wd_ref[sub, :128, :] - rate * mom_ref[sub, 1].T.astype(F32)
        nwd_ref[sub, 128:, :] = wd_ref[sub, 128:, :] - rate * mixed[:64, :]
        up_b = nwu_ref[sub].astype(BF16) * 0.5
        down_b = nwd_ref[sub].astype(BF16)
        for chunk in range(CHUNKS):
            sl = slice(chunk * step, (chunk + 1) * step)
            x_wide = rows[sl, :].astype(F32)
            centered, scale = norm_parts(x_wide)
            u_rows = (centered * scale).astype(BF16)
            half = jnp.dot(u_rows, up_b, preferred_element_type=F32).astype(BF16)
            z_rows = gelu_half(half.astype(F32)).astype(BF16)
            y_rows = lax.dot_general(z_rows, down_b, LAST, preferred_element_type=F32).astype(BF16)
            rows[sl, :] = (x_wide + y_rows.astype(F32)).astype(BF16)

    @pl.when(layer == pl.num_programs(0) - 1)
    def _():
        wh_copy.wait()
        mh_copy.wait()
        n_cls = wh_ref.shape[1]
        for dev in range(16):
            for tile in range(-(-n_cls // 128)):
                span = slice(tile * 128, min(n_cls, (tile + 1) * 128))
                block = mh_ref[tile // 3, dev * 48 + (tile % 3) * 16 : dev * 48 + (tile % 3) * 16 + 16, :].astype(F32)
                keep = slice(dev * head_rows, (dev + 1) * head_rows)
                wh_ref[keep, span] = wh_ref[keep, span] - rate * block[:head_rows, : span.stop - span.start]
        out_copy = pltpu.make_async_copy(wh_ref, nwh_hbm, sems.at[1])
        out_copy.start()
        normed, _ = pooled_norm(rows, n_img, n_tok)
        logits = jnp.dot(normed.astype(BF16), wh_ref[...].astype(BF16), preferred_element_type=F32)
        log_ref[...] = logits[:n_img]
        log_copy = pltpu.make_async_copy(log_ref, log_hbm, sems.at[0])
        log_copy.start()
        log_copy.wait()
        out_copy.wait()
        for copy in gives:
            copy.wait()


def backward_kernel(
    n_items, sc_ref, gh_hbm, grad_hbm, xs_ref, pre_ref, wu_ref, wd_ref, mh_hbm, mu_hbm, md_hbm, nmh_hbm, nmu_hbm, nmd_hbm, all_ref,
    g_rows, z_buf, da_buf, u_buf, mh_wide, mh_ref, mu_ref, md_ref, g_buf, pair_buf, sum_buf, rcv0, rcv1, rcv2, ag_buf,
    d2d_send, d2d_recv, rs_send, rs_recv, ag_send, ag_recv, out_sem, in_sem, mom_sem,
):
    t = pl.program_id(0)
    me = lax.axis_index("data")
    core = lax.rem(me, 2)
    place = (lax.div(me, 8), lax.rem(lax.div(me, 4), 2), lax.rem(lax.div(me, 2), 2))
    peers = tuple(me + (1 - 2 * place[axis]) * w for axis, w in ((0, 8), (1, 4), (2, 2)))
    twin = me + 1 - 2 * core
    rcv = (rcv0, rcv1, rcv2)

    @pl.when(t == 0)
    def _():
        barrier = pltpu.get_barrier_semaphore()
        for peer in peers + (twin,):
            pl.semaphore_signal(barrier, inc=1, device_id=(peer,), device_id_type=MESH_ID)
        pl.semaphore_wait(barrier, 4)

    def pair_copy(item):
        slot = lax.rem(item, G_SLOTS)
        return pltpu.make_async_remote_copy(
            src_ref=g_buf.at[slot, :, :, :, :, 1 - core],
            dst_ref=pair_buf.at[slot],
            send_sem=d2d_send.at[0, slot],
            recv_sem=d2d_recv.at[0, slot],
            device_id=(twin,),
            device_id_type=MESH_ID,
        )

    def cut(part, stage, value):
        index = [slice(None)] * 3
        for axis in ORDER[part][:stage]:
            index[axis] = place[axis]
        index[ORDER[part][stage]] = value
        return tuple(index)

    def rs_copy(item, stage, part):
        axis = ORDER[part][stage]
        slot = lax.rem(item, IN_SLOTS)
        return pltpu.make_async_remote_copy(
            src_ref=sum_buf.at[(lax.rem(item, RS_SLOTS), part) + cut(part, stage, 1 - place[axis])],
            dst_ref=rcv[stage].at[slot, part],
            send_sem=rs_send.at[stage, part, slot],
            recv_sem=rs_recv.at[stage, part, slot],
            device_id=(peers[axis],),
            device_id_type=MESH_ID,
        )

    def ag_copy(item, stage, part):
        index = [place[0], place[1], place[2]]
        for axis in ORDER[part][:stage]:
            index[axis] = slice(None)
        view = ag_buf.at[(lax.rem(item, AG_SLOTS), part) + tuple(index) + (core,)]
        return pltpu.make_async_remote_copy(
            src_ref=view,
            dst_ref=view,
            send_sem=ag_send.at[stage, part, lax.rem(item, IN_SLOTS)],
            recv_sem=ag_recv.at[stage, part, lax.rem(item, IN_SLOTS)],
            device_id=(peers[ORDER[part][stage]],),
            device_id_type=MESH_ID,
        )

    def twin_copy(item):
        view = ag_buf.at[lax.rem(item, AG_SLOTS), :, :, :, :, core]
        return pltpu.make_async_remote_copy(
            src_ref=view,
            dst_ref=view,
            send_sem=d2d_send.at[1, lax.rem(item, 2)],
            recv_sem=d2d_recv.at[1, lax.rem(item, 2)],
            device_id=(twin,),
            device_id_type=MESH_ID,
        )

    def out_copy(item):
        return pltpu.make_async_copy(ag_buf.at[lax.rem(item, AG_SLOTS)], all_ref.at[n_items - 1 - item], out_sem.at[lax.rem(item, 2)])

    def at_lag(lag):
        return (t >= lag) & (t < n_items + lag)

    head_copy = pltpu.make_async_copy(gh_hbm, g_buf.at[0], in_sem.at[0])
    grad_copy = pltpu.make_async_copy(grad_hbm, g_rows, in_sem.at[1])
    moms = tuple(
        pltpu.make_async_copy(src, dst, in_sem.at[2 + i]) for i, (src, dst) in enumerate(((mh_hbm, mh_ref), (mu_hbm, mu_ref), (md_hbm, md_ref)))
    )
    moms_out = tuple(
        pltpu.make_async_copy(src, dst, mom_sem.at[i]) for i, (src, dst) in enumerate(((mh_ref, nmh_hbm), (mu_ref, nmu_hbm), (md_ref, nmd_hbm)))
    )

    @pl.when(t == 0)
    def _():
        head_copy.start()
        grad_copy.start()
        for copy in moms:
            copy.start()

    @pl.when(t == 1)
    def _():
        grad_copy.wait()

    @pl.when((t >= 1) & (t < n_items))
    def _():
        up_b = wu_ref[0].astype(BF16)
        down_b = wd_ref[0].astype(BF16)
        step = g_rows.shape[0] // CHUNKS
        grad_old = g_rows[...]
        for chunk in range(CHUNKS):
            sl = slice(chunk * step, (chunk + 1) * step)
            g_old = grad_old[sl, :]
            z_wide, slope = gelu_both(pre_ref[0, sl, :].astype(F32))
            z_buf[sl, :] = z_wide.astype(BF16)
            grad_z = jnp.dot(g_old, down_b, preferred_element_type=F32).astype(BF16)
            grad_a = (grad_z.astype(F32) * slope).astype(BF16)
            da_buf[sl, :] = grad_a
            centered, scale = norm_parts(xs_ref[0, sl, :].astype(F32))
            normed = centered * scale
            u_buf[sl, :] = normed.astype(BF16)
            grad_u = lax.dot_general(grad_a, up_b, LAST, preferred_element_type=F32).astype(BF16)
            grad_x = norm_pull(normed, scale, grad_u.astype(F32))
            g_rows[sl, :] = (g_old.astype(F32) + grad_x).astype(BF16)
        down_t = lax.dot_general(grad_old, z_buf[...], ROWS, preferred_element_type=F32).astype(BF16)
        up_g = lax.dot_general(u_buf[...], da_buf[...], ROWS, preferred_element_type=F32).astype(BF16)
        for part, value in enumerate((up_g[:128, :], down_t[:128, :], jnp.concatenate([down_t[128:, :], up_g[128:, :]], axis=0))):
            turned = value.T
            for dev in range(16):
                block = turned[dev * 48 : (dev + 1) * 48, :]
                g_buf[lax.rem(t, G_SLOTS), part, dev // 8, (dev // 4) % 2, (dev // 2) % 2, dev % 2] = block

    @pl.when(at_lag(UPDATE))
    def _():
        item = t - UPDATE
        for part in range(PARTS):
            rs_copy(item, 2, part).wait()

        def reduced(part):
            return (sum_buf[lax.rem(item, RS_SLOTS), part, place[0], place[1], place[2]] + rcv[2][lax.rem(item, IN_SLOTS), part]).astype(F32)

        def hand_on(part, mom):
            ag_buf[lax.rem(item, AG_SLOTS), part, place[0], place[1], place[2], core] = mom.astype(BF16)

        @pl.when(t == UPDATE)
        def _():
            for copy in moms:
                copy.wait()
            head_rows, n_cls = mh_ref.shape
            mh_wide[...] = jnp.zeros_like(mh_wide)
            mh_wide[:head_rows, :n_cls] = mh_ref[...]
            for part in range(PARTS):
                lanes = [slice((3 * part + i) * 128, (3 * part + i + 1) * 128) for i in range(3)]
                mom = sc_ref[0, 0] * jnp.concatenate([mh_wide[:, one] for one in lanes], axis=0) + reduced(part)
                for i in range(3):
                    mh_wide[:, lanes[i]] = mom[i * 16 : (i + 1) * 16, :]
                hand_on(part, mom)
            mh_ref[...] = mh_wide[:head_rows, :n_cls]

        @pl.when(t > UPDATE)
        def _():
            layer = n_items - 1 - item
            mixed = reduced(2)
            up_a = sc_ref[0, 0] * mu_ref[layer, :, :128] + reduced(0)
            down_a = sc_ref[0, 0] * md_ref[layer, :, :128] + reduced(1)
            up_z = sc_ref[0, 0] * mu_ref[layer, :, 128:] + mixed[:, 64:]
            down_z = sc_ref[0, 0] * md_ref[layer, :, 128:] + mixed[:, :64]
            mu_ref[layer, :, :128] = up_a
            mu_ref[layer, :, 128:] = up_z
            md_ref[layer, :, :128] = down_a
            md_ref[layer, :, 128:] = down_z
            hand_on(0, up_a)
            hand_on(1, down_a)
            hand_on(2, jnp.concatenate([down_z, up_z], axis=1))

    for stage in (1, 0):

        @pl.when(at_lag(3 + 2 * stage))
        def _(stage=stage):
            item = t - 3 - 2 * stage
            for part in range(PARTS):
                rs_copy(item, stage, part).wait()
                kept = (lax.rem(item, RS_SLOTS), part) + cut(part, stage, place[ORDER[part][stage]])
                sum_buf[kept] = sum_buf[kept] + rcv[stage][lax.rem(item, IN_SLOTS), part]
                rs_copy(item, stage + 1, part).start()

    @pl.when(at_lag(1))
    def _():
        item = t - 1
        pair_copy(item).wait()
        for part in range(PARTS):
            kept = g_buf[lax.rem(item, G_SLOTS), part, :, :, :, core]
            sum_buf[lax.rem(item, RS_SLOTS), part] = kept + pair_buf[lax.rem(item, G_SLOTS), part]
            rs_copy(item, 0, part).start()

    @pl.when(t == 0)
    def _():
        head_copy.wait()
        pair_copy(0).start()

    @pl.when((t >= 1) & (t < n_items))
    def _():
        pair_copy(t).start()

    @pl.when(at_lag(TWIN + 2))
    def _():
        out_copy(t - TWIN - 2).wait()

    @pl.when(at_lag(TWIN + 1))
    def _():
        item = t - TWIN - 1
        twin_copy(item).wait()
        out_copy(item).start()

    for stage in (3, 2, 1):

        @pl.when(at_lag(UPDATE + 2 * stage))
        def _(stage=stage):
            item = t - UPDATE - 2 * stage
            for part in range(PARTS):
                ag_copy(item, stage - 1, part).wait()
                if stage < 3:
                    ag_copy(item, stage, part).start()
            if stage == 3:
                twin_copy(item).start()

    @pl.when(at_lag(UPDATE))
    def _():
        for part in range(PARTS):
            ag_copy(t - UPDATE, 0, part).start()

    @pl.when(t == n_items + UPDATE)
    def _():
        for copy in moms_out:
            copy.start()

    @pl.when(t == n_items + UPDATE + 3)
    def _():
        for copy in moms_out:
            copy.wait()


def solution(mesh):
    n_dev = mesh.shape["data"]

    def local_step(x_now, x_next, labels, w_up, w_down, w_head, mom_up, mom_down, mom_head, learn_rate, mom_decay):
        n_img, n_tok, width = x_now.shape
        n_layers, _, hidden = w_up.shape
        n_cls = w_head.shape[1]
        n_rows = -(-n_img * n_tok // (16 * CHUNKS)) * 16 * CHUNKS
        n_items = n_layers + 1
        cols = mom_up.shape[2]
        head_rows = mom_head.shape[0]
        n_tile = -(-n_cls // 128)

        down_t = w_down.transpose(0, 2, 1)
        per = 2 if n_layers % 2 == 0 else 1
        any_spec = pl.BlockSpec(memory_space=pl.ANY)
        blocks = (PARTS, 2, 2, 2, 2, cols, 128)
        xs, pre, grad_rows, head_g = pl.pallas_call(
            functools.partial(forward_kernel, n_img, n_tok, n_img * n_dev, head_rows),
            grid=(n_layers // per,),
            in_specs=[
                pl.BlockSpec(memory_space=pltpu.SMEM),
                any_spec,
                pl.BlockSpec((per, width, hidden), lambda i: (i, 0, 0)),
                pl.BlockSpec((per, width, hidden), lambda i: (i, 0, 0)),
                any_spec,
            ],
            out_specs=[
                pl.BlockSpec((per, n_rows, width), lambda i: (i, 0, 0)),
                pl.BlockSpec((per, n_rows, hidden), lambda i: (i, 0, 0)),
                any_spec,
                any_spec,
            ],
            out_shape=[
                jax.ShapeDtypeStruct((n_layers, n_rows, width), BF16),
                jax.ShapeDtypeStruct((n_layers, n_rows, hidden), BF16),
                jax.ShapeDtypeStruct((n_rows, width), BF16),
                jax.ShapeDtypeStruct(blocks, BF16),
            ],
            scratch_shapes=[
                pltpu.VMEM((n_img, width, n_tok), BF16),
                pltpu.VMEM(w_head.shape, F32),
                pltpu.VMEM((n_rows, width), F32),
                pltpu.VMEM((n_rows, width), BF16),
                pltpu.VMEM((n_dev * head_rows + 16, n_tile * 128), F32),
                pltpu.VMEM(blocks, BF16),
                pltpu.SemaphoreType.DMA((2,)),
            ],
            compiler_params=pltpu.CompilerParams(vmem_limit_bytes=VMEM_LIMIT),
            name="step_forward",
        )(labels, x_now.transpose(0, 2, 1), w_up, down_t, w_head)

        def layer_at(t):
            return jnp.clip(n_items - 1 - t, 0, n_layers - 1)

        block = (PARTS, 2, 2, 2)
        head_kept, up_kept, down_kept, gathered = pl.pallas_call(
            functools.partial(backward_kernel, n_items),
            grid=(n_items + TWIN + 2,),
            in_specs=[
                pl.BlockSpec(memory_space=pltpu.SMEM),
                any_spec,
                any_spec,
                pl.BlockSpec((1, n_rows, width), lambda t: (layer_at(t), 0, 0)),
                pl.BlockSpec((1, n_rows, hidden), lambda t: (layer_at(t), 0, 0)),
                pl.BlockSpec((1, width, hidden), lambda t: (layer_at(t), 0, 0)),
                pl.BlockSpec((1, width, hidden), lambda t: (layer_at(t), 0, 0)),
                any_spec,
                any_spec,
                any_spec,
            ],
            out_specs=[any_spec] * 4,
            out_shape=[
                jax.ShapeDtypeStruct(mom_head.shape, F32),
                jax.ShapeDtypeStruct((n_layers, cols, width), F32),
                jax.ShapeDtypeStruct((n_layers, cols, width), F32),
                jax.ShapeDtypeStruct((n_items, PARTS, 2, 2, 2, 2, cols, 128), BF16),
            ],
            scratch_shapes=[
                pltpu.VMEM((n_rows, width), BF16),
                pltpu.VMEM((n_rows, hidden), BF16),
                pltpu.VMEM((n_rows, hidden), BF16),
                pltpu.VMEM((n_rows, width), BF16),
                pltpu.VMEM((16, 9 * 128), F32),
                pltpu.VMEM(mom_head.shape, F32),
                pltpu.VMEM((n_layers, cols, width), F32),
                pltpu.VMEM((n_layers, cols, width), F32),
                pltpu.VMEM((G_SLOTS,) + block + (2, cols, 128), BF16),
                pltpu.VMEM((G_SLOTS,) + block + (cols, 128), BF16),
                pltpu.VMEM((RS_SLOTS,) + block + (cols, 128), BF16),
                pltpu.VMEM((IN_SLOTS, PARTS, 2, 2, cols, 128), BF16),
                pltpu.VMEM((IN_SLOTS, PARTS, 2, cols, 128), BF16),
                pltpu.VMEM((IN_SLOTS, PARTS, cols, 128), BF16),
                pltpu.VMEM((AG_SLOTS,) + block + (2, cols, 128), BF16),
                pltpu.SemaphoreType.DMA((2, 2)),
                pltpu.SemaphoreType.DMA((2, 2)),
                pltpu.SemaphoreType.DMA((3, PARTS, IN_SLOTS)),
                pltpu.SemaphoreType.DMA((3, PARTS, IN_SLOTS)),
                pltpu.SemaphoreType.DMA((3, PARTS, IN_SLOTS)),
                pltpu.SemaphoreType.DMA((3, PARTS, IN_SLOTS)),
                pltpu.SemaphoreType.DMA((2,)),
                pltpu.SemaphoreType.DMA((5,)),
                pltpu.SemaphoreType.DMA((3,)),
            ],
            compiler_params=pltpu.CompilerParams(vmem_limit_bytes=VMEM_LIMIT, collective_id=0, has_side_effects=True),
            name="step_backward",
        )(mom_decay.reshape(1, 1), head_g, grad_rows, xs, pre, w_up, down_t, mom_head, mom_up.transpose(0, 2, 1), mom_down)

        gathered = gathered.reshape(n_items, PARTS, n_dev * cols, 128)
        new_w_up, new_down_t, new_w_head, logits, new_mom_head, mom_up_new, new_mom_down = pl.pallas_call(
            functools.partial(next_kernel, n_img, n_tok, head_rows),
            grid=(n_layers // per,),
            in_specs=[
                pl.BlockSpec(memory_space=pltpu.SMEM),
                any_spec,
                pl.BlockSpec((per, width, hidden), lambda i: (i, 0, 0)),
                pl.BlockSpec((per, width, hidden), lambda i: (i, 0, 0)),
                pl.BlockSpec((per, PARTS, n_dev * cols, 128), lambda i: (i, 0, 0, 0)),
                any_spec,
                any_spec,
                any_spec,
                any_spec,
                any_spec,
            ],
            out_specs=[
                pl.BlockSpec((per, width, hidden), lambda i: (i, 0, 0)),
                pl.BlockSpec((per, width, hidden), lambda i: (i, 0, 0)),
            ]
            + [any_spec] * 5,
            out_shape=[
                jax.ShapeDtypeStruct(w_up.shape, F32),
                jax.ShapeDtypeStruct(w_up.shape, F32),
                jax.ShapeDtypeStruct(w_head.shape, F32),
                jax.ShapeDtypeStruct((n_img, n_cls), F32),
                jax.ShapeDtypeStruct(mom_head.shape, F32),
                jax.ShapeDtypeStruct((n_layers, cols, width), F32),
                jax.ShapeDtypeStruct((n_layers, cols, width), F32),
            ],
            scratch_shapes=[
                pltpu.VMEM((n_img, width, n_tok), BF16),
                pltpu.VMEM(w_head.shape, F32),
                pltpu.VMEM((PARTS, n_dev * cols, 128), BF16),
                pltpu.VMEM((n_img, n_cls), F32),
                pltpu.VMEM((n_rows, width), F32),
                pltpu.VMEM((n_rows, width), BF16),
                pltpu.VMEM(mom_head.shape, F32),
                pltpu.VMEM((n_layers, cols, width), F32),
                pltpu.VMEM((n_layers, cols, width), F32),
                pltpu.SemaphoreType.DMA((6,)),
            ],
            compiler_params=pltpu.CompilerParams(vmem_limit_bytes=VMEM_LIMIT),
            name="step_next",
        )(learn_rate.reshape(1, 1), x_next.transpose(0, 2, 1), w_up, down_t, gathered, gathered, w_head, head_kept, up_kept, down_kept)

        return (logits, new_w_up, new_down_t.transpose(0, 2, 1), new_w_head, mom_up_new.transpose(0, 2, 1), new_mom_down, new_mom_head)

    spec_up = P(None, None, "data")
    spec_down = P(None, "data", None)
    spec_head = P("data", None)
    return jax.shard_map(
        local_step,
        mesh=mesh,
        in_specs=(P("data"), P("data"), P("data"), P(), P(), P(), spec_up, spec_down, spec_head, P(), P()),
        out_specs=(P("data"), P(), P(), P(), spec_up, spec_down, spec_head),
        check_vma=False,
    )
```
